32 devices in a mesh: ctx: 16 (over z, x, core), head: 2 (over y).
Axes of the slice: x: 2, y: 2, z: 4, core: 2. Of those that a mesh axis runs over, the one named last changes fastest.
Arguments:
- queries: bfloat16 [8192, 16, 128], P('ctx', 'head'), may hold values from -160 to 160, as said below
- keys: bfloat16 [8192, 2, 128], P('ctx', 'head'), may hold values from -4 to 4
- values: bfloat16 [8192, 2, 128], P('ctx', 'head'), may hold values from -6 to 6
- doc_lengths: int32 [32], replicated, may hold values from 1 to 4096, 8192 in all
Outputs:
- attended: bfloat16 [8192, 2048], P(('ctx', 'head'))
The draws below stay inside these ranges and needn't reach their ends.
Inputs may be any that keep to these rules, and one draw needn't show every extreme that they name: `queries`: queries of several heads for a few tokens may be large multiples of sums of earlier keys of the same key head. `doc_lengths`: the lengths sum to 8192; the largest is exactly 4096.
All inputs are finite; a program needn't handle non-finite values.
Results may differ from the reference program's by a relative error of at most 0.0033.
Values may be sent and summed in bfloat16 or wider, within the bound.
A program may use at most 64 MiB of HBM per device.

```python
import math
import jax
import jax.numpy as jnp
import numpy as np
from jax import lax

HD = 128
TOK_DEV = 512
SPAN = 8
KV_HEADS = 2
QH = 16
TOKENS = 8192
DOCS = 32
DOC_MOST = 4096


def make_pair(key):
    key_keys = jax.random.fold_in(key, 11)
    key_queries = jax.random.fold_in(key, 23)
    key_vectors = jnp.clip(jax.random.normal(key_keys, (TOKENS, KV_HEADS, HD), jnp.float32), -4.0, 4.0)
    query_vectors = jnp.clip(jax.random.normal(key_queries, (TOKENS, QH, HD), jnp.float32), -6.0, 6.0)
    return (query_vectors, key_vectors)


def draw_queries(key, part):
    return make_pair(key)[0].astype(jnp.bfloat16)


def draw_keys(key, part):
    return make_pair(key)[1].astype(jnp.bfloat16)


def shard_levels(key, extent, shards, least, high):
    def one(dim, parts):
        heights = jax.random.uniform(jax.random.fold_in(jax.random.fold_in(key, 6), dim), (parts,), jnp.float32, least / len(shards), high / len(shards))
        return jnp.repeat(jnp.exp(heights), extent[dim] // parts).reshape((-1,) + (1,) * (len(extent) - dim - 1))

    gain = one(*shards[0])
    for cut in shards[1:]:
        gain = gain * one(*cut)
    return gain


def split_up(number_of, total, bound, lean):
    portions = [(1 << 20) // math.isqrt(grade ** lean) + 1 for grade in range(2, number_of + 1)]
    rest, counts = total - bound - (number_of - 1), [1] * (number_of - 1)
    while rest > 0:
        candidates = [i for i in range(number_of - 1) if counts[i] < bound]
        pool, left = sum([portions[i] for i in candidates]), rest
        for i in candidates:
            extra = min(bound - counts[i], max(1, left * portions[i] // pool), rest)
            counts[i] = counts[i] + extra
            rest = rest - extra
    return np.array([bound] + counts)


def ragged_sizes(rng, amount, total, limit, slope):
    if amount == 2:
        one = jax.random.randint(rng, (), max(1, total - limit), min(limit, total - 1) + 1)
        return jnp.stack([one, total - one])
    tallies = jnp.asarray(split_up(amount, total, limit, slope), jnp.int32)
    pairs = (amount - 1) // 2
    source_of, receiver = tallies[1:1 + 2 * pairs:2], tallies[2:2 + 2 * pairs:2]
    slack = jnp.minimum(source_of - 1, limit - receiver)
    passed = jax.random.randint(jax.random.fold_in(rng, 1), (pairs,), 0, 1 << 20) % (slack + 1)
    tallies = tallies.at[1:1 + 2 * pairs:2].set(source_of - passed).at[2:2 + 2 * pairs:2].set(receiver + passed)
    return tallies[jax.random.permutation(jax.random.fold_in(rng, 2), amount)]


def noise(key, extent, width, most, shards=(), kind=jnp.bfloat16):
    level = shard_levels(key, extent, shards, -0.22, 0.18) if shards else 1.0
    values = jax.random.normal(key, extent, jnp.float32) * width * level
    return jnp.minimum(jnp.maximum(values, -most), most).astype(kind)


def setup_inputs(seed: int = 0) -> dict:
    arg_keys = jax.random.split(jax.random.key(seed), 5)
    queries = draw_queries(jax.random.fold_in(arg_keys[4], 71), 0)
    keys = draw_keys(jax.random.fold_in(arg_keys[4], 71), 0)
    values = noise(arg_keys[2], (TOKENS, KV_HEADS, HD), 1.0, 6.0, ((0, 16), (1, 2)))
    doc_lengths = ragged_sizes(arg_keys[3], DOCS, TOKENS, DOC_MOST, 2).astype(jnp.int32)
    return {"queries": queries, "keys": keys, "values": values, "doc_lengths": doc_lengths}


def doc_index(positions, ends):
    return jnp.sum((ends[None, :] <= positions[:, None]).astype(jnp.int32), axis=1).astype(jnp.int32)


def reference(queries, keys, values, doc_lengths):
    tokens, qheads, hdim = queries.shape
    kvheads = keys.shape[1]
    group = qheads // kvheads
    block = TOK_DEV
    scale = 1.0 / (hdim ** 0.5)
    ends = jnp.cumsum(doc_lengths).astype(jnp.int32)
    docs = doc_index(jnp.arange(tokens, dtype=jnp.int32), ends)
    front = jnp.zeros((SPAN * block, kvheads, hdim), keys.dtype)
    key_pad = jnp.concatenate([front, keys], axis=0)
    value_pad = jnp.concatenate([front, values], axis=0)
    grouped = queries.reshape(tokens, kvheads, group, hdim)

    def one_block(index):
        start = (index * block).astype(jnp.int32)
        query_block = lax.dynamic_slice_in_dim(grouped, start, block, 0).astype(jnp.float32)
        qpos = start + jnp.arange(block, dtype=jnp.int32)
        qdoc = lax.dynamic_slice_in_dim(docs, start, block, 0)

        def update(state, back):
            first = (start - back * block).astype(jnp.int32)
            key_block = lax.dynamic_slice_in_dim(key_pad, first + SPAN * block, block, 0).astype(jnp.float32)
            value_block = lax.dynamic_slice_in_dim(value_pad, first + SPAN * block, block, 0).astype(jnp.float32)
            kpos = first + jnp.arange(block, dtype=jnp.int32)
            kdoc = doc_index(jnp.maximum(kpos, 0), ends)
            mask = (kdoc[None, :] == qdoc[:, None]) & (kpos[None, :] <= qpos[:, None]) & (kpos[None, :] >= 0)
            highest, total, acc = state
            score = jnp.einsum("qhgd,khd->hgqk", query_block, key_block) * scale
            score = jnp.where(mask[None, None], score, -1e30)
            newmax = jnp.maximum(highest, jnp.max(score, axis=-1))
            factor = jnp.exp(highest - newmax)
            expo = jnp.exp(score - newmax[..., None])
            total = total * factor + jnp.sum(expo, axis=-1)
            rounded = lax.optimization_barrier(expo.astype(jnp.bfloat16)).astype(jnp.float32)
            acc = acc * factor[..., None] + jnp.einsum("hgqk,khd->hgqd", rounded, value_block)
            return newmax, total, acc

        def step(back, state):
            first = (start - back * block).astype(jnp.int32)
            last = first + block - 1
            need = (back == 0) | ((last >= 0) & (doc_index(jnp.maximum(last, 0)[None], ends)[0] == qdoc[0]))
            return lax.cond(need, lambda s: update(s, back), lambda s: s, state)

        init = (jnp.full((kvheads, group, block), -1e30, jnp.float32),
                jnp.zeros((kvheads, group, block), jnp.float32),
                jnp.zeros((kvheads, group, block, hdim), jnp.float32))
        highest, total, acc = lax.fori_loop(0, SPAN + 1, step, init)
        result = acc / total[..., None]
        return jnp.transpose(result, (2, 0, 1, 3)).reshape(block, qheads * hdim).astype(jnp.bfloat16)

    outs = lax.map(one_block, jnp.arange(tokens // block, dtype=jnp.int32))
    return outs.reshape(tokens, qheads * hdim)
```

```python
import functools
import math

import jax
import jax.numpy as jnp
from jax import lax
from jax.experimental import pallas as pl
from jax.experimental.pallas import tpu as pltpu
from jax.sharding import PartitionSpec as P

MESH = pl.DeviceIdType.MESH
BIG = 1e30
MOST = 1024


def kernel(n, heads, tile, lens_ref, q_ref, k_ref, v_ref, out_ref,
           kbuf, vbuf, kdoc, qaug, acc, top, norm, stage,
           send_sem, recv_sem, osend_sem, orecv_sem):
    rows, hdim = k_ref.shape
    total_rows = q_ref.shape[0]
    group = total_rows // rows
    me = lax.axis_index("ctx")
    mine = lax.axis_index("head")
    pos = me % 4
    core = pos % 2
    col = pos // 2
    mate = me + 1 - 2 * core
    across = me + 2 - 4 * col
    pos_m = pos + 1 - 2 * core
    pos_x = pos + 2 - 4 * col
    pos_d = pos_x + pos_m - pos
    has1 = me >= 4
    has2 = me >= 8
    feeds = me + 4 < n
    right = col == 1
    leftc = col == 0

    barrier = pltpu.get_barrier_semaphore()
    for peer in (mate, across):
        pl.semaphore_signal(barrier, inc=1, device_id={"ctx": peer}, device_id_type=MESH)

    @pl.when(has1)
    def _():
        pl.semaphore_signal(barrier, inc=1, device_id={"ctx": me - 4}, device_id_type=MESH)

    @pl.when(feeds)
    def _():
        pl.semaphore_signal(barrier, inc=1, device_id={"ctx": me + 4}, device_id_type=MESH)

    for d in range(1, heads):
        pl.semaphore_signal(barrier, inc=1, device_id={"head": (mine + d) % heads}, device_id_type=MESH)
    pl.semaphore_wait(barrier, 1 + heads + has1.astype(jnp.int32) + feeds.astype(jnp.int32))

    def copies(lane, slot, to_slot, target):
        made = []
        for w, buf, own in ((0, kbuf, k_ref), (1, vbuf, v_ref)):
            made.append(pltpu.make_async_remote_copy(
                src_ref=own if slot is None else buf.at[slot],
                dst_ref=buf.at[to_slot],
                send_sem=send_sem.at[lane, w],
                recv_sem=recv_sem.at[to_slot, w],
                device_id={"ctx": target},
                device_id_type=MESH,
            ))
        return made

    moves = {
        "D0": (copies(0, None, 8 + pos, mate), None),
        "X0": (copies(1, None, 8 + pos, across), leftc),
        "Z0": (copies(2, None, 4 + pos, me + 4), feeds),
        "D0x": (copies(3, 8 + pos_x, 8 + pos_x, mate), right),
        "D1": (copies(4, 4 + pos, 4 + pos, mate), has1),
        "X1": (copies(5, 4 + pos, 4 + pos, across), has1),
        "Z1": (copies(6, 4 + pos, pos, me + 4), has1 & feeds),
        "D1x": (copies(7, 4 + pos_x, 4 + pos_x, mate), has1),
        "D2": (copies(8, pos, pos, mate), has2),
        "X2": (copies(9, pos, pos, across), has2 & right),
        "D2x": (copies(10, pos_x, pos_x, mate), has2 & leftc),
    }

    def when(cond, fn):
        if cond is None:
            fn()
        else:
            pl.when(cond)(fn)

    def start(name):
        made, cond = moves[name]

        def go():
            for copy in made:
                copy.start()

        when(cond, go)

    def sent(name):
        made, cond = moves[name]

        def go():
            for copy in made:
                copy.wait_send()

        when(cond, go)

    def landed(slot, cond):
        def go():
            for w, buf in ((0, kbuf), (1, vbuf)):
                pltpu.make_async_copy(buf.at[slot], buf.at[slot], recv_sem.at[slot, w]).wait()

        when(cond, go)

    start("Z0")
    start("X0")
    start("D0")

    lane = lax.broadcasted_iota(jnp.int32, (8, 128), 1)
    firsts = jnp.full((8, 128), 2**30, jnp.int32)
    ends = jnp.full((8, 128), 2**30, jnp.int32)
    run = jnp.int32(0)
    for d in range(lens_ref.shape[0]):
        firsts = jnp.where(lane == d, run, firsts)
        run = run + lens_ref[d]
        ends = jnp.where(lane == d, run, ends)
    first_row, end_row = firsts[0:1], ends[0:1]

    def member(position):
        return (position >= first_row) & (position < end_row)

    base = me * rows
    part = rows // heads
    tokens = tile // group
    steps = part // tokens
    chunk = max(128, tokens)

    def by_token(width, dim):
        return lax.broadcasted_iota(jnp.int32, (tokens, group, width), dim).reshape(tile, width)

    @pl.loop(0, total_rows // tile)
    def _(t):
        at = pl.ds(pl.multiple_of(t * tile, tile), tile)
        qaug[at, 0:hdim] = q_ref[at, :]
        qaug[at, hdim:] = jnp.where(member(base + t * tokens + by_token(128, 0)), 1.0, 0.0).astype(jnp.bfloat16)

    @pl.loop(0, 12)
    def _(s):
        kpos = (me - pos - 8 + s) * rows + lax.broadcasted_iota(jnp.int32, (rows, 128), 0)
        kdoc[s] = jnp.where(member(kpos), 0.0, -BIG).astype(jnp.bfloat16)

    @pl.when(me < 8)
    def _():
        @pl.loop(0, 4)
        def _(s):
            kbuf[s] = jnp.zeros((rows, hdim), jnp.bfloat16)
            vbuf[s] = jnp.zeros((rows, hdim), jnp.bfloat16)

    scale = math.log2(math.e) / hdim**0.5

    def spread(x, width):
        return jnp.concatenate([x] * (width // 128), axis=1)

    def score(at, keys, docs):
        return lax.dot_general(
            qaug[at, :], jnp.concatenate([keys, docs], axis=1), (((1,), (1,)), ((), ())),
            preferred_element_type=jnp.float32) * scale

    def spot(owner, t):
        return pl.multiple_of(owner * (part * group) + t * tile, tile)

    def diagonal(owner, t):
        at = pl.ds(spot(owner, t), tile)
        token = owner * part + t * tokens
        reach = (token + tokens + chunk - 1) // chunk

        def upto(k):
            width = k * chunk
            s = score(at, k_ref[0:width, :], kdoc[8 + pos, 0:width, :])
            edge = by_token(chunk, 2) - by_token(chunk, 0) <= token - (width - chunk)
            last = jnp.where(edge, s[:, width - chunk:], -BIG)
            s = last if k == 1 else jnp.concatenate([s[:, :width - chunk], last], axis=1)
            m = jnp.broadcast_to(jnp.max(s, axis=1, keepdims=True), (tile, 128))
            e = jnp.exp2(s - spread(m, width))
            top[at, :] = m
            acc[at, 0:128] = jnp.dot(
                e.astype(jnp.bfloat16), v_ref[0:width, :], preferred_element_type=jnp.float32)
            acc[at, 128:] = sum(e[:, i * 128:(i + 1) * 128] for i in range(width // 128))

        for k in range(1, rows // chunk + 1):
            pl.when(reach == k)(functools.partial(upto, k))

    def both(at, a, b):
        sa = score(at, kbuf[a], kdoc[a])
        sb = score(at, kbuf[b], kdoc[b])
        m0 = top[at, :]
        m = jnp.maximum(m0, jnp.max(jnp.maximum(sa, sb), axis=1, keepdims=True))
        wide = spread(m, rows)
        ea = jnp.exp2(sa - wide)
        eb = jnp.exp2(sb - wide)
        pa = ea.astype(jnp.bfloat16)
        pb = eb.astype(jnp.bfloat16)
        top[at, :] = m
        grown = jnp.dot(pa, vbuf[a], preferred_element_type=jnp.float32)
        grown = grown + jnp.dot(pb, vbuf[b], preferred_element_type=jnp.float32)
        factor = jnp.exp2(m0 - m)
        tot = sum(ea[:, k * 128:(k + 1) * 128] + eb[:, k * 128:(k + 1) * 128] for k in range(rows // 128))
        return jnp.concatenate([acc[at, 0:128] * factor + grown, acc[at, 128:] * factor + tot], axis=1)

    def pick(if_right, if_left):
        return col * if_right + (1 - col) * if_left

    g1 = (4 + pos, 4 + pos_m)
    g2 = (4 + pos_x, 4 + pos_d)
    g3 = (pick(8 + pos_x, pos_x), pick(8 + pos_d, pos_d))
    g4 = (pos, core * (8 + pos_m) + (1 - core) * pos_m)
    pairs = (
        (pick(g3[0], g1[0]), pick(g3[1], g1[1]), right | has1),
        (pick(g1[0], g2[0]), pick(g1[1], g2[1]), has1),
        (pick(g2[0], g4[0]), pick(g2[1], g4[1]), (right & has1) | (leftc & (has2 | (core == 1)))),
        (pick(g4[0], g3[0]), pick(g4[1], g3[1]), has2 | (right & (core == 1))),
    )
    last_a, last_b, last_valid = pairs[3]
    peers = (heads - 1) * steps

    def peer(u):
        return (mine + 1 + u // steps) % heads, u % steps

    def pair(a, b, valid, count, place):
        @pl.when(valid)
        def _():
            @pl.loop(0, count)
            def _(u):
                at = pl.ds(spot(*place(u)), tile)
                acc[at, :] = both(at, a, b)

    def local(t):
        return pl.ds(pl.multiple_of(t * tokens, tokens), tokens)

    def finish(owner, t, own):
        at = pl.ds(spot(owner, t), tile)

        def close(whole):
            norm[...] = whole[:, 0:hdim] / jnp.sum(whole[:, hdim:], axis=1, keepdims=True)

        @pl.when(last_valid)
        def _():
            close(both(at, last_a, last_b))

        @pl.when(jnp.logical_not(last_valid))
        def _():
            close(acc[at, :])

        for g in range(group):
            piece = norm[pl.ds(g, tokens, stride=group), :].astype(jnp.bfloat16)
            if own is None:
                where = pl.ds(pl.multiple_of(mine * (group * hdim) + g * hdim, hdim), hdim)
                out_ref[local(t), where] = piece
            else:
                stage[own, local(t), g * hdim:(g + 1) * hdim] = piece

    columns = pl.ds(pl.multiple_of(mine * (group * hdim), group * hdim), group * hdim)

    def outgoing(d, t):
        return pltpu.make_async_remote_copy(
            src_ref=stage.at[d - 1, local(t)],
            dst_ref=out_ref.at[local(t), columns],
            send_sem=osend_sem.at[d - 1, t],
            recv_sem=orecv_sem.at[d - 1, t],
            device_id={"head": (mine + d) % heads},
            device_id_type=MESH,
        )

    @pl.loop(0, peers)
    def _(u):
        diagonal(*peer(u))

    landed(4 + pos, has1)
    start("Z1")
    start("X1")
    start("D1")
    landed(8 + pos_x, right)
    start("D0x")
    landed(8 + pos_m, None)
    landed(4 + pos_m, has1)
    landed(8 + pos_d, right)
    pair(*pairs[0], peers, peer)

    @pl.loop(0, steps)
    def _(t):
        diagonal(mine, t)

    landed(pos, has2)
    start("X2")
    start("D2")
    landed(4 + pos_x, has1)
    start("D1x")
    landed(4 + pos_d, has1)
    pair(*pairs[1], peers, peer)

    landed(pos_m, has2)
    pair(*pairs[2], peers, peer)

    landed(pos_x, has2 & leftc)
    start("D2x")
    landed(pos_d, has2 & leftc)

    for d in range(1, heads):
        @pl.loop(0, steps)
        def _(t):
            finish((mine + d) % heads, t, d - 1)
            outgoing(d, t).start()

    def choose(p, k):
        return sum((p == i) * jnp.asarray(pairs[i][k], jnp.int32) for i in range(3))

    @pl.loop(0, 3)
    def _(p):
        pair(choose(p, 0), choose(p, 1), choose(p, 2) == 1, steps, lambda t: (mine, t))

    @pl.loop(0, steps)
    def _(t):
        finish(mine, t, None)

    for d in range(1, heads):
        @pl.loop(0, steps)
        def _(t):
            outgoing(d, t).wait_send()
            source = (mine + heads - d) % heads
            cols = pl.ds(pl.multiple_of(source * (group * hdim), group * hdim), group * hdim)
            got = out_ref.at[local(t), cols]
            pltpu.make_async_copy(got, got, orecv_sem.at[d - 1, t]).wait()

    for name in moves:
        sent(name)


def on_device(mesh, queries, keys, values, doc_lengths):
    rows, group, hdim = queries.shape
    heads = mesh.shape["head"]
    n = mesh.shape["ctx"]
    bf16, f32 = jnp.bfloat16, jnp.float32
    part = rows // heads
    tile = min(MOST, part * group)
    steps = part * group // tile
    vmem = pl.BlockSpec(memory_space=pltpu.VMEM)
    return pl.pallas_call(
        functools.partial(kernel, n, heads, tile),
        out_shape=jax.ShapeDtypeStruct((part, heads * group * hdim), bf16),
        in_specs=[pl.BlockSpec(memory_space=pltpu.SMEM), vmem, vmem, vmem],
        out_specs=vmem,
        scratch_shapes=[
            pltpu.VMEM((12, rows, hdim), bf16),
            pltpu.VMEM((12, rows, hdim), bf16),
            pltpu.VMEM((12, rows, 128), bf16),
            pltpu.VMEM((rows * group, hdim + 128), bf16),
            pltpu.VMEM((rows * group, hdim + 128), f32),
            pltpu.VMEM((rows * group, 128), f32),
            pltpu.VMEM((tile, hdim), f32),
            pltpu.VMEM((heads - 1, part, group * hdim), bf16),
            pltpu.SemaphoreType.DMA((11, 2)),
            pltpu.SemaphoreType.DMA((12, 2)),
            pltpu.SemaphoreType.DMA((heads - 1, steps)),
            pltpu.SemaphoreType.DMA((heads - 1, steps)),
        ],
        compiler_params=pltpu.CompilerParams(
            collective_id=0, has_side_effects=True, vmem_limit_bytes=56 * 1024 * 1024),
    )(doc_lengths, queries.reshape(rows * group, hdim), keys.reshape(rows, hdim), values.reshape(rows, hdim))


def solution(mesh):
    placed = (P("ctx", "head", None), P("ctx", "head", None), P("ctx", "head", None), P())
    return jax.shard_map(
        functools.partial(on_device, mesh), mesh=mesh, in_specs=placed,
        out_specs=P(("ctx", "head"), None), check_vma=False
    )
```

```python
import functools
import math

import jax
import jax.numpy as jnp
from jax import lax
from jax.experimental import pallas as pl
from jax.experimental.pallas import tpu as pltpu
from jax.sharding import PartitionSpec as P

MESH = pl.DeviceIdType.MESH
BIG = 1e30
MOST = 512
BAND = 128
ORDER = (0, 4, 1, 5, 2, 3, 6, 7)


def kernel(n, heads, tile, lens_ref, q_ref, k_ref, v_ref, out_ref,
           kbuf, vbuf, kdoc, qaug, acc, top, norm, stage,
           send_sem, recv_sem, osend_sem, orecv_sem, load_sem):
    rows, hdim = k_ref.shape
    total_rows = q_ref.shape[0]
    group = total_rows // rows
    me = lax.axis_index("ctx")
    mine = lax.axis_index("head")
    pos = me % 4
    core = pos % 2
    col = pos // 2
    mate = me + 1 - 2 * core
    across = me + 2 - 4 * col
    pos_m = pos + 1 - 2 * core
    pos_x = pos + 2 - 4 * col
    pos_d = pos_x + pos_m - pos
    has1 = me >= 4
    has2 = me >= 8
    feeds = me + 4 < n
    right = col == 1
    leftc = col == 0

    loads = (
        pltpu.make_async_copy(k_ref, kbuf.at[8 + pos], load_sem.at[0]),
        pltpu.make_async_copy(q_ref, qaug.at[:, 0:hdim], load_sem.at[1]),
        pltpu.make_async_copy(v_ref, vbuf.at[8 + pos], load_sem.at[2]),
    )
    for load in loads:
        load.start()

    barrier = pltpu.get_barrier_semaphore()
    for peer in (mate, across):
        pl.semaphore_signal(barrier, inc=1, device_id={"ctx": peer}, device_id_type=MESH)

    @pl.when(has1)
    def _():
        pl.semaphore_signal(barrier, inc=1, device_id={"ctx": me - 4}, device_id_type=MESH)

    @pl.when(feeds)
    def _():
        pl.semaphore_signal(barrier, inc=1, device_id={"ctx": me + 4}, device_id_type=MESH)

    for d in range(1, heads):
        pl.semaphore_signal(barrier, inc=1, device_id={"head": (mine + d) % heads}, device_id_type=MESH)
    pl.semaphore_wait(barrier, 1 + heads + has1.astype(jnp.int32) + feeds.astype(jnp.int32))

    def copies(lane, slot, to_slot, target):
        made = []
        for w, buf, own in ((0, kbuf, k_ref), (1, vbuf, v_ref)):
            made.append(pltpu.make_async_remote_copy(
                src_ref=own if slot is None else buf.at[slot],
                dst_ref=buf.at[to_slot],
                send_sem=send_sem.at[lane, w],
                recv_sem=recv_sem.at[to_slot, w],
                device_id={"ctx": target},
                device_id_type=MESH,
            ))
        return made

    moves = {
        "D0": (copies(0, None, 8 + pos, mate), None),
        "X0": (copies(1, None, 8 + pos, across), leftc),
        "Z0": (copies(2, None, 4 + pos, me + 4), feeds),
        "D0x": (copies(3, 8 + pos_x, 8 + pos_x, mate), right),
        "D1": (copies(4, 4 + pos, 4 + pos, mate), has1),
        "X1": (copies(5, 4 + pos, 4 + pos, across), has1),
        "Z1": (copies(6, 4 + pos, pos, me + 4), has1 & feeds),
        "D1x": (copies(7, 4 + pos_x, 4 + pos_x, mate), has1),
        "D2": (copies(8, pos, pos, mate), has2),
        "X2": (copies(9, pos, pos, across), has2 & right),
        "D2x": (copies(10, pos_x, pos_x, mate), has2 & leftc),
    }

    def when(cond, fn):
        if cond is None:
            fn()
        else:
            pl.when(cond)(fn)

    def start(*names):
        for name in names:
            made, cond = moves[name]

            def go():
                for copy in made:
                    copy.start()

            when(cond, go)

    def sent(name):
        made, cond = moves[name]

        def go():
            for copy in made:
                copy.wait_send()

        when(cond, go)

    def landed(slot, cond, *names):
        for w, buf in ((0, kbuf), (1, vbuf)):
            def go():
                pltpu.make_async_copy(buf.at[slot], buf.at[slot], recv_sem.at[slot, w]).wait()

            when(cond, go)
            for name in names:
                made, also = moves[name]
                when(also, made[w].start)

    start("Z0", "X0", "D0")

    lane = lax.broadcasted_iota(jnp.int32, (8, 128), 1)
    firsts = jnp.full((8, 128), 2**30, jnp.int32)
    ends = jnp.full((8, 128), 2**30, jnp.int32)
    run = jnp.int32(0)
    for d in range(lens_ref.shape[0]):
        firsts = jnp.where(lane == d, run, firsts)
        run = run + lens_ref[d]
        ends = jnp.where(lane == d, run, ends)
    first_row, end_row = firsts[0:1], ends[0:1]

    def member(position):
        return (position >= first_row) & (position < end_row)

    base = me * rows
    part = rows // heads
    tokens = tile // group
    steps = part // tokens
    span = part * group

    def by_token(width, dim):
        return lax.broadcasted_iota(jnp.int32, (tokens, group, width), dim).reshape(tile, width)

    @pl.loop(0, total_rows // tile)
    def _(t):
        at = pl.ds(pl.multiple_of(t * tile, tile), tile)
        qaug[at, hdim:] = jnp.where(member(base + t * tokens + by_token(128, 0)), 1.0, 0.0).astype(jnp.bfloat16)

    @pl.loop(0, 12)
    def _(s):
        kpos = (me - pos - 8 + s) * rows + lax.broadcasted_iota(jnp.int32, (rows, 128), 0)
        kdoc[s] = jnp.where(member(kpos), 0.0, -BIG).astype(jnp.bfloat16)

    @pl.when(me < 8)
    def _():
        @pl.loop(0, 4)
        def _(s):
            kbuf[s] = jnp.zeros((rows, hdim), jnp.bfloat16)
            vbuf[s] = jnp.zeros((rows, hdim), jnp.bfloat16)

    scale = math.log2(math.e) / hdim**0.5

    def spread(x, width):
        return jnp.concatenate([x] * (width // 128), axis=1)

    def raw(at, slot, width):
        return lax.dot_general(
            qaug[at, :], jnp.concatenate([kbuf[slot, 0:width, :], kdoc[slot, 0:width, :]], axis=1),
            (((1,), (1,)), ((), ())), preferred_element_type=jnp.float32)

    def mixed(weight, slot, width):
        ones = jnp.ones((width, 128), jnp.bfloat16)
        return jnp.dot(weight, jnp.concatenate([vbuf[slot, 0:width, :], ones], axis=1),
                       preferred_element_type=jnp.float32)

    def flow(count, one, two, three):
        scores, weights = {}, {}
        for u in range(count + 2):
            if u >= 2:
                three(u - 2, *weights.pop(u - 2))
            if 1 <= u <= count:
                weights[u - 1] = two(u - 1, scores.pop(u - 1))
            if u < count:
                scores[u] = one(u)

    def diagonal():
        def width(t):
            return -(-(t + 1) * tokens // 128) * 128

        def at(t):
            return pl.ds(t * tile, tile)

        def one(t):
            return raw(at(t), 8 + pos, width(t))

        def two(t, s):
            wide, done = width(t), []
            for r in range(0, tile, BAND):
                here = slice(r, r + BAND)
                x = s[here, :] * scale
                edge = by_token(128, 2)[here] - by_token(128, 0)[here] <= t * tokens - (wide - 128)
                last = jnp.where(edge, x[:, wide - 128:], -BIG)
                x = last if wide == 128 else jnp.concatenate([x[:, :wide - 128], last], axis=1)
                m = jnp.broadcast_to(jnp.max(x, axis=1, keepdims=True), (BAND, 128))
                top[pl.ds(t * tile + r, BAND), :] = m
                done.append(jnp.exp2(x - spread(m, wide)).astype(jnp.bfloat16))
            return (jnp.concatenate(done, axis=0),)

        def three(t, weight):
            acc[at(t), :] = mixed(weight, 8 + pos, width(t))

        flow(total_rows // tile, one, two, three)

    def unit(first, a, b):
        def at(u, r=0, size=tile):
            return pl.ds(pl.multiple_of(first + (u % steps) * tile + r, size), size)

        def slot(u):
            return a if u < steps else b

        def one(u):
            return raw(at(u), slot(u), rows)

        def two(u, s):
            done, factors = [], []
            for r in range(0, tile, BAND):
                x = s[r:r + BAND, :] * scale
                m0 = top[at(u, r, BAND), :]
                m = jnp.maximum(m0, jnp.max(x, axis=1, keepdims=True))
                top[at(u, r, BAND), :] = m
                factors.append(jnp.exp2(m0 - m))
                done.append(jnp.exp2(x - spread(m, rows)).astype(jnp.bfloat16))
            return jnp.concatenate(done, axis=0), jnp.concatenate(factors, axis=0)

        def three(u, weight, factor):
            acc[at(u), :] = acc[at(u), :] * spread(factor, 2 * hdim) + mixed(weight, slot(u), rows)

        flow(2 * steps, one, two, three)

    def pick(if_right, if_left):
        return col * if_right + (1 - col) * if_left

    g1 = (4 + pos, 4 + pos_m)
    g2 = (4 + pos_x, 4 + pos_d)
    g3 = (pick(8 + pos_x, pos_x), pick(8 + pos_d, pos_d))
    g4 = (pos, core * (8 + pos_m) + (1 - core) * pos_m)
    pairs = (
        (pick(g3[0], g1[0]), pick(g3[1], g1[1]), right | has1),
        (pick(g1[0], g2[0]), pick(g1[1], g2[1]), has1),
        (pick(g2[0], g4[0]), pick(g2[1], g4[1]), (right & has1) | (leftc & (has2 | (core == 1)))),
        (pick(g4[0], g3[0]), pick(g4[1], g3[1]), has2 | (right & (core == 1))),
    )

    def local(t):
        return pl.ds(pl.multiple_of(t * tokens, tokens), tokens)

    def finish(first, t, put):
        whole = acc[pl.ds(pl.multiple_of(first + t * tile, tile), tile), :]
        norm[...] = whole[:, 0:hdim] / whole[:, hdim:]
        for g in range(group):
            put(g, norm[pl.ds(g, tokens, stride=group), :].astype(jnp.bfloat16))

    columns = pl.ds(pl.multiple_of(mine * (group * hdim), group * hdim), group * hdim)

    def outgoing(d, t):
        return pltpu.make_async_remote_copy(
            src_ref=stage.at[d - 1, local(t)],
            dst_ref=out_ref.at[local(t), columns],
            send_sem=osend_sem.at[d - 1, t],
            recv_sem=orecv_sem.at[d - 1, t],
            device_id={"head": (mine + d) % heads},
            device_id_type=MESH,
        )

    for load in loads:
        load.wait()
    diagonal()

    def event0():
        landed(4 + pos, has1, "Z1", "X1", "D1")
        landed(8 + pos_x, right, "D0x")
        landed(8 + pos_m, None)
        landed(4 + pos_m, has1)
        landed(8 + pos_d, right)

    def event1():
        landed(pos, has2, "X2", "D2")
        landed(4 + pos_x, has1, "D1x")
        landed(4 + pos_d, has1)

    def event2():
        landed(pos_m, has2)

    def event3():
        landed(pos_x, has2 & leftc, "D2x")
        landed(pos_d, has2 & leftc)

    others = list(range(1, heads))
    order = [(p, d) for p in ORDER for d in (others if p < 4 else [heads])]
    order = [(p % 4, d) for p, d in order]
    events = (event0, event1, event2, event3)

    def choose(index, values):
        return sum((index == i) * jnp.asarray(x, jnp.int32) for i, x in enumerate(values))

    @pl.loop(0, len(order))
    def _(u):
        for p, event in enumerate(events):
            pl.when(u == [x for x, _ in order].index(p))(event)
        p = choose(u, [x for x, _ in order])
        d = choose(u, [x for _, x in order])
        first = (mine + d) % heads * span

        @pl.when(choose(p, [x[2] for x in pairs]) == 1)
        def _():
            unit(first, choose(p, [x[0] for x in pairs]), choose(p, [x[1] for x in pairs]))

        @pl.when((p == 3) & (d < heads))
        def _():
            @pl.loop(0, steps)
            def _(t):
                def put(g, piece):
                    stage[d - 1, local(t), g * hdim:(g + 1) * hdim] = piece

                finish(first, t, put)
                outgoing(d, t).start()

        @pl.when((p == 3) & (d == heads))
        def _():
            @pl.loop(0, steps)
            def _(t):
                def put(g, piece):
                    where = pl.ds(pl.multiple_of(mine * (group * hdim) + g * hdim, hdim), hdim)
                    out_ref[local(t), where] = piece

                finish(first, t, put)

    for d in range(1, heads):
        @pl.loop(0, steps)
        def _(t):
            outgoing(d, t).wait_send()
            source = (mine + heads - d) % heads
            cols = pl.ds(pl.multiple_of(source * (group * hdim), group * hdim), group * hdim)
            got = out_ref.at[local(t), cols]
            pltpu.make_async_copy(got, got, orecv_sem.at[d - 1, t]).wait()

    for name in moves:
        sent(name)


def on_device(mesh, queries, keys, values, doc_lengths):
    rows, group, hdim = queries.shape
    heads = mesh.shape["head"]
    n = mesh.shape["ctx"]
    bf16, f32 = jnp.bfloat16, jnp.float32
    part = rows // heads
    tile = min(MOST, part * group)
    steps = part * group // tile
    vmem = pl.BlockSpec(memory_space=pltpu.VMEM)
    anywhere = pl.BlockSpec(memory_space=pl.ANY)
    return pl.pallas_call(
        functools.partial(kernel, n, heads, tile),
        out_shape=pltpu.VMEM((part, heads * group * hdim), bf16),
        in_specs=[pl.BlockSpec(memory_space=pltpu.SMEM), anywhere, anywhere, anywhere],
        out_specs=vmem,
        scratch_shapes=[
            pltpu.VMEM((12, rows, hdim), bf16),
            pltpu.VMEM((12, rows, hdim), bf16),
            pltpu.VMEM((12, rows, 128), bf16),
            pltpu.VMEM((rows * group, hdim + 128), bf16),
            pltpu.VMEM((rows * group, hdim + 128), f32),
            pltpu.VMEM((rows * group, 128), f32),
            pltpu.VMEM((tile, hdim), f32),
            pltpu.VMEM((heads - 1, part, group * hdim), bf16),
            pltpu.SemaphoreType.DMA((11, 2)),
            pltpu.SemaphoreType.DMA((12, 2)),
            pltpu.SemaphoreType.DMA((heads - 1, steps)),
            pltpu.SemaphoreType.DMA((heads - 1, steps)),
            pltpu.SemaphoreType.DMA((3,)),
        ],
        compiler_params=pltpu.CompilerParams(
            collective_id=0, has_side_effects=True, vmem_limit_bytes=56 * 1024 * 1024),
    )(doc_lengths, queries.reshape(rows * group, hdim), keys.reshape(rows, hdim), values.reshape(rows, hdim))


def solution(mesh):
    placed = (P("ctx", "head", None), P("ctx", "head", None), P("ctx", "head", None), P())
    return jax.shard_map(
        functools.partial(on_device, mesh), mesh=mesh, in_specs=placed,
        out_specs=P(("ctx", "head"), None), check_vma=False
    )
```

```python
import functools
import math

import jax
import jax.numpy as jnp
from jax import lax
from jax.experimental import pallas as pl
from jax.experimental.pallas import tpu as pltpu
from jax.sharding import PartitionSpec as P

MESH = pl.DeviceIdType.MESH
BIG = 1e30
MOST = 512
BAND = 128
EDGE = 512
ORDER = (0, 4, 1, 2, 3, 5, 6, 7)


def kernel(n, heads, tile, lens_ref, q_ref, k_ref, v_ref, out_ref,
           kbuf, vbuf, kdoc, qaug, acc, top, norm, stage,
           send_sem, recv_sem, osend_sem, orecv_sem, load_sem):
    rows, hdim = k_ref.shape
    total_rows = q_ref.shape[0]
    group = total_rows // rows
    me = lax.axis_index("ctx")
    mine = lax.axis_index("head")
    pos = me % 4
    core = pos % 2
    col = pos // 2
    mate = me + 1 - 2 * core
    across = me + 2 - 4 * col
    pos_m = pos + 1 - 2 * core
    pos_x = pos + 2 - 4 * col
    pos_d = pos_x + pos_m - pos
    has1 = me >= 4
    has2 = me >= 8
    feeds = me + 4 < n
    right = col == 1
    leftc = col == 0

    loads = (
        pltpu.make_async_copy(k_ref, kbuf.at[8 + pos], load_sem.at[0]),
        pltpu.make_async_copy(q_ref, qaug.at[:, 0:hdim], load_sem.at[1]),
        pltpu.make_async_copy(v_ref, vbuf.at[8 + pos], load_sem.at[2]),
    )
    for load in loads:
        load.start()

    barrier = pltpu.get_barrier_semaphore()
    for peer in (mate, across):
        pl.semaphore_signal(barrier, inc=1, device_id={"ctx": peer}, device_id_type=MESH)

    @pl.when(has1)
    def _():
        pl.semaphore_signal(barrier, inc=1, device_id={"ctx": me - 4}, device_id_type=MESH)

    @pl.when(feeds)
    def _():
        pl.semaphore_signal(barrier, inc=1, device_id={"ctx": me + 4}, device_id_type=MESH)

    for d in range(1, heads):
        pl.semaphore_signal(barrier, inc=1, device_id={"head": (mine + d) % heads}, device_id_type=MESH)
    pl.semaphore_wait(barrier, 1 + heads + has1.astype(jnp.int32) + feeds.astype(jnp.int32))

    def copies(lane, slot, to_slot, target):
        made = []
        for w, buf, own in ((0, kbuf, k_ref), (1, vbuf, v_ref)):
            made.append(pltpu.make_async_remote_copy(
                src_ref=own if slot is None else buf.at[slot],
                dst_ref=buf.at[to_slot],
                send_sem=send_sem.at[lane, w],
                recv_sem=recv_sem.at[to_slot, w],
                device_id={"ctx": target},
                device_id_type=MESH,
            ))
        return made

    moves = {
        "D0": (copies(0, None, 8 + pos, mate), None),
        "X0": (copies(1, None, 8 + pos, across), leftc),
        "Z0": (copies(2, None, 4 + pos, me + 4), feeds),
        "D0x": (copies(3, 8 + pos_x, 8 + pos_x, mate), right),
        "D1": (copies(4, 4 + pos, 4 + pos, mate), has1),
        "X1": (copies(5, 4 + pos, 4 + pos, across), has1),
        "Z1": (copies(6, 4 + pos, pos, me + 4), has1 & feeds),
        "D1x": (copies(7, 4 + pos_x, 4 + pos_x, mate), has1),
        "D2": (copies(8, pos, pos, mate), has2),
        "X2": (copies(9, pos, pos, across), has2 & right),
        "D2x": (copies(10, pos_x, pos_x, mate), has2 & leftc),
    }

    def when(cond, fn):
        if cond is None:
            fn()
        else:
            pl.when(cond)(fn)

    def start(*names):
        for name in names:
            made, cond = moves[name]

            def go():
                for copy in made:
                    copy.start()

            when(cond, go)

    def sent(name):
        made, cond = moves[name]

        def go():
            for copy in made:
                copy.wait_send()

        when(cond, go)

    def landed(slot, cond, *names, which=(0, 1)):
        for w in which:
            buf = (kbuf, vbuf)[w]

            def go():
                pltpu.make_async_copy(buf.at[slot], buf.at[slot], recv_sem.at[slot, w]).wait()

            when(cond, go)
            for name in names:
                made, also = moves[name]
                when(also, made[w].start)

    start("Z0", "X0", "D0")

    lane = lax.broadcasted_iota(jnp.int32, (8, 128), 1)
    firsts = jnp.full((8, 128), 2**30, jnp.int32)
    ends = jnp.full((8, 128), 2**30, jnp.int32)
    run = jnp.int32(0)
    for d in range(lens_ref.shape[0]):
        firsts = jnp.where(lane == d, run, firsts)
        run = run + lens_ref[d]
        ends = jnp.where(lane == d, run, ends)
    first_row, end_row = firsts[0:1], ends[0:1]

    def member(position):
        return (position >= first_row) & (position < end_row)

    base = me * rows
    part = rows // heads
    tokens = tile // group
    steps = part // tokens
    span = part * group

    def by_token(width, dim):
        return lax.broadcasted_iota(jnp.int32, (tokens, group, width), dim).reshape(tile, width)

    @pl.loop(0, total_rows // tile)
    def _(t):
        at = pl.ds(pl.multiple_of(t * tile, tile), tile)
        qaug[at, hdim:] = jnp.where(member(base + t * tokens + by_token(128, 0)), 1.0, 0.0).astype(jnp.bfloat16)

    def mark(s):
        kpos = (me - pos - 8 + s) * rows + lax.broadcasted_iota(jnp.int32, (rows, 128), 0)
        kdoc[s] = jnp.where(member(kpos), 0.0, -BIG).astype(jnp.bfloat16)

    mark(8 + pos)

    scale = math.log2(math.e) / hdim**0.5

    def spread(x, width):
        return jnp.concatenate([x] * (width // 128), axis=1)

    def raw(at, slot, width):
        return lax.dot_general(
            qaug[at, :], jnp.concatenate([kbuf[slot, 0:width, :], kdoc[slot, 0:width, :]], axis=1),
            (((1,), (1,)), ((), ())), preferred_element_type=jnp.float32)

    def mixed(weight, slot, width):
        ones = jnp.ones((width, 128), jnp.bfloat16)
        return jnp.dot(weight, jnp.concatenate([vbuf[slot, 0:width, :], ones], axis=1),
                       preferred_element_type=jnp.float32)

    def flow(count, one, two, three):
        scores, weights = {}, {}
        for u in range(count + 2):
            if u >= 2:
                three(u - 2, *weights.pop(u - 2))
            if 1 <= u <= count:
                weights[u - 1] = two(u - 1, scores.pop(u - 1))
            if u < count:
                scores[u] = one(u)

    def diagonal():
        def width(t):
            return -(-(t + 1) * tokens // 128) * 128

        def at(t):
            return pl.ds(t * tile, tile)

        def one(t):
            return raw(at(t), 8 + pos, width(t))

        def two(t, s):
            wide, done = width(t), []
            for r in range(0, tile, BAND):
                here = slice(r, r + BAND)
                x = s[here, :] * scale
                edge = by_token(128, 2)[here] - by_token(128, 0)[here] <= t * tokens - (wide - 128)
                last = jnp.where(edge, x[:, wide - 128:], -BIG)
                x = last if wide == 128 else jnp.concatenate([x[:, :wide - 128], last], axis=1)
                m = jnp.broadcast_to(jnp.max(x, axis=1, keepdims=True), (BAND, 128))
                top[pl.ds(t * tile + r, BAND), :] = m
                done.append(jnp.exp2(x - spread(m, wide)).astype(jnp.bfloat16))
            return (jnp.concatenate(done, axis=0),)

        def three(t, weight):
            acc[at(t), :] = mixed(weight, 8 + pos, width(t))

        flow(total_rows // tile, one, two, three)

    def cuts(extent):
        if extent < 4 * tile or tile % 256:
            return [(r, min(tile, extent)) for r in range(0, extent, min(tile, extent))]
        sizes = [EDGE] + [tile] * ((extent - 2 * EDGE) // tile) + [(extent - 2 * EDGE) % tile] * ((extent - 2 * EDGE) % tile > 0) + [EDGE]
        return [(sum(sizes[:i]), x) for i, x in enumerate(sizes)]

    def unit(first, a, b, extent):
        pieces = [(r, size, slot) for r, size in cuts(extent) for slot in (a, b)]

        def at(r, size):
            return pl.ds(pl.multiple_of(first + r, 128), size)

        def one(u):
            r, size, slot = pieces[u]
            return raw(at(r, size), slot, rows)

        def two(u, s):
            start_row, size, _ = pieces[u]
            done, factors = [], []
            for r in range(0, size, BAND):
                x = s[r:r + BAND, :] * scale
                here = at(start_row + r, BAND)
                m0 = top[here, :]
                m = jnp.maximum(m0, jnp.max(x, axis=1, keepdims=True))
                top[here, :] = m
                factors.append(jnp.exp2(m0 - m))
                done.append(jnp.exp2(x - spread(m, rows)).astype(jnp.bfloat16))
            return jnp.concatenate(done, axis=0), jnp.concatenate(factors, axis=0)

        def three(u, weight, factor):
            r, size, slot = pieces[u]
            here = at(r, size)
            acc[here, :] = acc[here, :] * spread(factor, 2 * hdim) + mixed(weight, slot, rows)

        flow(len(pieces), one, two, three)

    def pick(if_right, if_left):
        return col * if_right + (1 - col) * if_left

    g1 = (4 + pos, 4 + pos_m)
    g2 = (4 + pos_x, 4 + pos_d)
    g3 = (pick(8 + pos_x, pos_x), pick(8 + pos_d, pos_d))
    g4 = (pos, core * (8 + pos_m) + (1 - core) * pos_m)
    pairs = (
        (pick(g3[0], g1[0]), pick(g3[1], g1[1]), right | has1),
        (pick(g1[0], g2[0]), pick(g1[1], g2[1]), has1),
        (pick(g2[0], g4[0]), pick(g2[1], g4[1]), (right & has1) | (leftc & (has2 | (core == 1)))),
        (pick(g4[0], g3[0]), pick(g4[1], g3[1]), has2 | (right & (core == 1))),
    )

    def local(t):
        return pl.ds(pl.multiple_of(t * tokens, tokens), tokens)

    def finish(first, t, put):
        whole = acc[pl.ds(pl.multiple_of(first + t * tile, tile), tile), :]
        norm[...] = whole[:, 0:hdim] / whole[:, hdim:]
        for g in range(group):
            put(g, norm[pl.ds(g, tokens, stride=group), :].astype(jnp.bfloat16))

    columns = pl.ds(pl.multiple_of(mine * (group * hdim), group * hdim), group * hdim)

    def outgoing(d, t):
        return pltpu.make_async_remote_copy(
            src_ref=stage.at[d - 1, local(t)],
            dst_ref=out_ref.at[local(t), columns],
            send_sem=osend_sem.at[d - 1, t],
            recv_sem=orecv_sem.at[d - 1, t],
            device_id={"head": (mine + d) % heads},
            device_id_type=MESH,
        )

    for load in loads:
        load.wait()
    diagonal()

    @pl.loop(1, 12)
    def _(s):
        mark((8 + pos + s) % 12)

    @pl.when(me < 8)
    def _():
        @pl.loop(0, 4)
        def _(s):
            kbuf[s] = jnp.zeros((rows, hdim), jnp.bfloat16)
            vbuf[s] = jnp.zeros((rows, hdim), jnp.bfloat16)

    def event0():
        landed(4 + pos, has1, "Z1", "X1", "D1")
        landed(8 + pos_x, right, "D0x")
        landed(8 + pos_m, None)
        landed(4 + pos_m, has1)
        landed(8 + pos_d, right)

    def event1():
        landed(pos, has2, "X2", "D2", which=(0,))

    def event2():
        landed(pos, has2, "X2", "D2", which=(1,))
        landed(4 + pos_x, has1, "D1x")
        landed(4 + pos_d, has1)

    def event3():
        landed(pos_m, has2)
        landed(pos_x, has2 & leftc, "D2x", which=(0,))

    def event4():
        landed(pos_x, has2 & leftc, "D2x", which=(1,))
        landed(pos_d, has2 & leftc)

    others = list(range(1, heads))
    order = [(p, d) for p in ORDER for d in (others if p < 4 else [heads])]
    order = [(p % 4, d) for p, d in order]
    kinds = [p if d < heads else p + 4 for p, d in order]
    events = ((0, event0), (4, event1), (1, event2), (2, event3), (3, event4))
    half = span // 2 if steps % 2 == 0 else span

    def choose(index, values):
        return sum((index == i) * jnp.asarray(x, jnp.int32) for i, x in enumerate(values))

    @pl.loop(0, len(order))
    def _(u):
        for kind, event in events:
            pl.when(u == kinds.index(kind))(event)
        p = choose(u, [x for x, _ in order])
        d = choose(u, [x for _, x in order])
        first = (mine + d) % heads * span

        valid = choose(p, [x[2] for x in pairs]) == 1
        slots = choose(p, [x[0] for x in pairs]), choose(p, [x[1] for x in pairs])
        closing = (p == 3) & (d < heads)

        @pl.when(valid & jnp.logical_not(closing))
        def _():
            unit(first, *slots, span)

        @pl.when(closing)
        def _():
            @pl.loop(0, span // half)
            def _(h):
                @pl.when(valid)
                def _():
                    unit(first + h * half, *slots, half)

                @pl.loop(0, half // tile)
                def _(x):
                    t = h * (half // tile) + x

                    def put(g, piece):
                        stage[d - 1, local(t), g * hdim:(g + 1) * hdim] = piece

                    finish(first, t, put)
                    outgoing(d, t).start()

        @pl.when((p == 3) & (d == heads))
        def _():
            @pl.loop(0, steps)
            def _(t):
                def put(g, piece):
                    where = pl.ds(pl.multiple_of(mine * (group * hdim) + g * hdim, hdim), hdim)
                    out_ref[local(t), where] = piece

                finish(first, t, put)

    for d in range(1, heads):
        @pl.loop(0, steps)
        def _(t):
            outgoing(d, t).wait_send()
            source = (mine + heads - d) % heads
            cols = pl.ds(pl.multiple_of(source * (group * hdim), group * hdim), group * hdim)
            got = out_ref.at[local(t), cols]
            pltpu.make_async_copy(got, got, orecv_sem.at[d - 1, t]).wait()

    for name in moves:
        sent(name)


def on_device(mesh, queries, keys, values, doc_lengths):
    rows, group, hdim = queries.shape
    heads = mesh.shape["head"]
    n = mesh.shape["ctx"]
    bf16, f32 = jnp.bfloat16, jnp.float32
    part = rows // heads
    tile = min(MOST, part * group)
    steps = part * group // tile
    vmem = pl.BlockSpec(memory_space=pltpu.VMEM)
    anywhere = pl.BlockSpec(memory_space=pl.ANY)
    return pl.pallas_call(
        functools.partial(kernel, n, heads, tile),
        out_shape=pltpu.VMEM((part, heads * group * hdim), bf16),
        in_specs=[pl.BlockSpec(memory_space=pltpu.SMEM), anywhere, anywhere, anywhere],
        out_specs=vmem,
        scratch_shapes=[
            pltpu.VMEM((12, rows, hdim), bf16),
            pltpu.VMEM((12, rows, hdim), bf16),
            pltpu.VMEM((12, rows, 128), bf16),
            pltpu.VMEM((rows * group, hdim + 128), bf16),
            pltpu.VMEM((rows * group, hdim + 128), f32),
            pltpu.VMEM((rows * group, 128), f32),
            pltpu.VMEM((tile, hdim), f32),
            pltpu.VMEM((heads - 1, part, group * hdim), bf16),
            pltpu.SemaphoreType.DMA((11, 2)),
            pltpu.SemaphoreType.DMA((12, 2)),
            pltpu.SemaphoreType.DMA((heads - 1, steps)),
            pltpu.SemaphoreType.DMA((heads - 1, steps)),
            pltpu.SemaphoreType.DMA((3,)),
        ],
        compiler_params=pltpu.CompilerParams(
            collective_id=0, has_side_effects=True, vmem_limit_bytes=56 * 1024 * 1024),
    )(doc_lengths, queries.reshape(rows * group, hdim), keys.reshape(rows, hdim), values.reshape(rows, hdim))


def solution(mesh):
    placed = (P("ctx", "head", None), P("ctx", "head", None), P("ctx", "head", None), P())
    return jax.shard_map(
        functools.partial(on_device, mesh), mesh=mesh, in_specs=placed,
        out_specs=P(("ctx", "head"), None), check_vma=False
    )
```

```python
import functools
import math

import jax
import jax.numpy as jnp
from jax import lax
from jax.experimental import pallas as pl
from jax.experimental.pallas import tpu as pltpu
from jax.sharding import PartitionSpec as P

MESH = pl.DeviceIdType.MESH
BIG = 1e30
MOST = 512
BAND = 128
ORDER = (1, 2, 3, 5, 6, 7)
LOW, HIGH = (0, 1), (2, 3)
ALL = LOW + HIGH


def kernel(n, heads, tile, lens_ref, q_ref, k_ref, v_ref, out_ref,
           kbuf, vbuf, kdoc, qaug, acc, top, norm, stage,
           send_sem, recv_sem, osend_sem, orecv_sem, load_sem):
    rows, hdim = k_ref.shape
    total_rows = q_ref.shape[0]
    group = total_rows // rows
    me = lax.axis_index("ctx")
    mine = lax.axis_index("head")
    pos = me % 4
    core = pos % 2
    col = pos // 2
    mate = me + 1 - 2 * core
    across = me + 2 - 4 * col
    pos_m = pos + 1 - 2 * core
    pos_x = pos + 2 - 4 * col
    pos_d = pos_x + pos_m - pos
    has1 = me >= 4
    has2 = me >= 8
    feeds = me + 4 < n
    right = col == 1
    leftc = col == 0

    loads = (
        pltpu.make_async_copy(k_ref, kbuf.at[8 + pos], load_sem.at[0]),
        pltpu.make_async_copy(q_ref, qaug.at[:, 0:hdim], load_sem.at[1]),
        pltpu.make_async_copy(v_ref, vbuf.at[8 + pos], load_sem.at[2]),
    )
    for load in loads:
        load.start()

    barrier = pltpu.get_barrier_semaphore()
    for peer in (mate, across):
        pl.semaphore_signal(barrier, inc=1, device_id={"ctx": peer}, device_id_type=MESH)

    @pl.when(has1)
    def _():
        pl.semaphore_signal(barrier, inc=1, device_id={"ctx": me - 4}, device_id_type=MESH)

    @pl.when(feeds)
    def _():
        pl.semaphore_signal(barrier, inc=1, device_id={"ctx": me + 4}, device_id_type=MESH)

    for d in range(1, heads):
        pl.semaphore_signal(barrier, inc=1, device_id={"head": (mine + d) % heads}, device_id_type=MESH)
    pl.semaphore_wait(barrier, 1 + heads + has1.astype(jnp.int32) + feeds.astype(jnp.int32))

    half_keys = rows // 2
    parts = [(own, buf, pl.ds(h * half_keys, half_keys)) for h in range(2) for own, buf in ((k_ref, kbuf), (v_ref, vbuf))]

    def copies(lane, slot, to_slot, target):
        return [pltpu.make_async_remote_copy(
            src_ref=own.at[where] if slot is None else buf.at[slot, where],
            dst_ref=buf.at[to_slot, where],
            send_sem=send_sem.at[lane, w],
            recv_sem=recv_sem.at[to_slot, w],
            device_id={"ctx": target},
            device_id_type=MESH,
        ) for w, (own, buf, where) in enumerate(parts)]

    moves = {
        "D0": (copies(0, None, 8 + pos, mate), None),
        "X0": (copies(1, None, 8 + pos, across), leftc),
        "Z0": (copies(2, None, 4 + pos, me + 4), feeds),
        "D0x": (copies(3, 8 + pos_x, 8 + pos_x, mate), right),
        "D1": (copies(4, 4 + pos, 4 + pos, mate), has1),
        "X1": (copies(5, 4 + pos, 4 + pos, across), has1),
        "Z1": (copies(6, 4 + pos, pos, me + 4), has1 & feeds),
        "D1x": (copies(7, 4 + pos_x, 4 + pos_x, mate), has1),
        "D2": (copies(8, pos, pos, mate), has2),
        "X2": (copies(9, pos, pos, across), has2 & right),
        "D2x": (copies(10, pos_x, pos_x, mate), has2 & leftc),
    }

    def when(cond, fn):
        if cond is None:
            fn()
        else:
            pl.when(cond)(fn)

    def sent(name):
        made, cond = moves[name]

        def go():
            for copy in made:
                copy.wait_send()

        when(cond, go)

    def landed(slot, cond, *names, which=ALL):
        for w in which:
            _, buf, where = parts[w]

            def go():
                spot = buf.at[slot, where]
                pltpu.make_async_copy(spot, spot, recv_sem.at[slot, w]).wait()

            when(cond, go)
            for name in names:
                made, also = moves[name]
                when(also, made[w].start)

    for w in ALL:
        for name in ("Z0", "X0", "D0"):
            made, also = moves[name]
            when(also, made[w].start)

    lane = lax.broadcasted_iota(jnp.int32, (8, 128), 1)
    firsts = jnp.full((8, 128), 2**30, jnp.int32)
    ends = jnp.full((8, 128), 2**30, jnp.int32)
    run = jnp.int32(0)
    for d in range(lens_ref.shape[0]):
        firsts = jnp.where(lane == d, run, firsts)
        run = run + lens_ref[d]
        ends = jnp.where(lane == d, run, ends)
    first_row, end_row = firsts[0:1], ends[0:1]

    def member(position):
        return (position >= first_row) & (position < end_row)

    base = me * rows
    part = rows // heads
    tokens = tile // group
    steps = part // tokens
    span = part * group

    def by_token(width, dim):
        return lax.broadcasted_iota(jnp.int32, (tokens, group, width), dim).reshape(tile, width)

    @pl.loop(0, total_rows // tile)
    def _(t):
        at = pl.ds(pl.multiple_of(t * tile, tile), tile)
        qaug[at, hdim:] = jnp.where(member(base + t * tokens + by_token(128, 0)), 1.0, 0.0).astype(jnp.bfloat16)

    def mark(s):
        kpos = (me - pos - 8 + s) * rows + lax.broadcasted_iota(jnp.int32, (rows, 128), 0)
        kdoc[s] = jnp.where(member(kpos), 0.0, -BIG).astype(jnp.bfloat16)

    mark(8 + pos)

    scale = math.log2(math.e) / hdim**0.5

    def spread(x, width):
        return jnp.concatenate([x] * (width // 128), axis=1)

    def raw(at, slot, width):
        return lax.dot_general(
            qaug[at, :], jnp.concatenate([kbuf[slot, 0:width, :], kdoc[slot, 0:width, :]], axis=1),
            (((1,), (1,)), ((), ())), preferred_element_type=jnp.float32)

    def mixed(weight, slot, width):
        ones = jnp.ones((width, 128), jnp.bfloat16)
        return jnp.dot(weight, jnp.concatenate([vbuf[slot, 0:width, :], ones], axis=1),
                       preferred_element_type=jnp.float32)

    def raw_pair(at, a, b, where):
        keys = [jnp.concatenate([kbuf[x, where, :], kdoc[x, where, :]], axis=1) for x in (a, b)]
        return lax.dot_general(
            qaug[at, :], jnp.concatenate(keys, axis=0), (((1,), (1,)), ((), ())), preferred_element_type=jnp.float32)

    def mixed_pair(weight, a, b, where):
        ones = jnp.ones((rows, 128), jnp.bfloat16)
        vals = jnp.concatenate([vbuf[a, where, :], vbuf[b, where, :]], axis=0)
        return jnp.dot(weight, jnp.concatenate([vals, ones], axis=1), preferred_element_type=jnp.float32)

    def flow(count, one, two, three):
        scores, weights = {}, {}
        for u in range(count + 2):
            if u >= 2:
                three(u - 2, *weights.pop(u - 2))
            if 1 <= u <= count:
                weights[u - 1] = two(u - 1, scores.pop(u - 1))
            if u < count:
                scores[u] = one(u)

    def diagonal():
        def width(t):
            return -(-(t + 1) * tokens // 128) * 128

        def at(t):
            return pl.ds(t * tile, tile)

        def one(t):
            return raw(at(t), 8 + pos, width(t))

        def two(t, s):
            wide, done = width(t), []
            for r in range(0, tile, BAND):
                here = slice(r, r + BAND)
                x = s[here, :] * scale
                edge = by_token(128, 2)[here] - by_token(128, 0)[here] <= t * tokens - (wide - 128)
                last = jnp.where(edge, x[:, wide - 128:], -BIG)
                x = last if wide == 128 else jnp.concatenate([x[:, :wide - 128], last], axis=1)
                m = jnp.broadcast_to(jnp.max(x, axis=1, keepdims=True), (BAND, 128))
                top[pl.ds(t * tile + r, BAND), :] = m
                done.append(jnp.exp2(x - spread(m, wide)).astype(jnp.bfloat16))
            return (jnp.concatenate(done, axis=0),)

        def three(t, weight):
            acc[at(t), :] = mixed(weight, 8 + pos, width(t))

        flow(total_rows // tile, one, two, three)

    def work(first, a, b, pieces):
        def at(r, size):
            return pl.ds(pl.multiple_of(first + r, BAND), size)

        def one(u):
            r, where = pieces[u]
            return raw_pair(at(r, tile), a, b, where)

        def two(u, s):
            done, factors = [], []
            for r in range(0, tile, BAND):
                x = s[r:r + BAND, :] * scale
                here = at(pieces[u][0] + r, BAND)
                m0 = top[here, :]
                m = jnp.maximum(m0, jnp.max(x, axis=1, keepdims=True))
                top[here, :] = m
                factors.append(jnp.exp2(m0 - m))
                done.append(jnp.exp2(x - spread(m, rows)).astype(jnp.bfloat16))
            return jnp.concatenate(done, axis=0), jnp.concatenate(factors, axis=0)

        def three(u, weight, factor):
            r, where = pieces[u]
            here = at(r, tile)
            acc[here, :] = acc[here, :] * spread(factor, 2 * hdim) + mixed_pair(weight, a, b, where)

        flow(len(pieces), one, two, three)

    def unit(first, a, b, extent):
        work(first, a, b, [(r, parts[w][2]) for r in range(0, extent, tile) for w in (0, 2)])

    def sweep(a, b, h):
        where = pl.ds(pl.multiple_of(h * half_keys, half_keys), half_keys)
        work(0, a, b, [(r, where) for r in range(0, total_rows, tile)])

    def pick(if_right, if_left):
        return col * if_right + (1 - col) * if_left

    near = core * (8 + pos_m) + (1 - core) * pos_m
    pairs = (
        (pick(8 + pos_x, 4 + pos), pick(8 + pos_d, 4 + pos_m), right | has1),
        (pick(4 + pos, 4 + pos_x), pick(4 + pos_m, pos), has1),
        (pick(4 + pos_x, 4 + pos_d), pick(4 + pos_d, near), has1 | (leftc & (core == 1))),
        (pick(pos, pos_x), pick(near, pos_d), has2 | (right & (core == 1))),
    )

    def local(t):
        return pl.ds(pl.multiple_of(t * tokens, tokens), tokens)

    def finish(first, t, put):
        whole = acc[pl.ds(pl.multiple_of(first + t * tile, tile), tile), :]
        norm[...] = whole[:, 0:hdim] / whole[:, hdim:]
        for g in range(group):
            put(g, norm[pl.ds(g, tokens, stride=group), :].astype(jnp.bfloat16))

    columns = pl.ds(pl.multiple_of(mine * (group * hdim), group * hdim), group * hdim)

    def outgoing(d, t):
        return pltpu.make_async_remote_copy(
            src_ref=stage.at[d - 1, local(t)],
            dst_ref=out_ref.at[local(t), columns],
            send_sem=osend_sem.at[d - 1, t],
            recv_sem=orecv_sem.at[d - 1, t],
            device_id={"head": (mine + d) % heads},
            device_id_type=MESH,
        )

    for load in loads:
        load.wait()
    diagonal()

    def first_in(which):
        landed(4 + pos, has1, "Z1", "X1", "D1", which=which)
        landed(8 + pos_x, right, "D0x", which=which)

    def first_over(which):
        landed(4 + pos_m, has1, which=which)
        landed(8 + pos_d, right, which=which)

    first_in(LOW)

    @pl.loop(1, 12)
    def _(s):
        mark((8 + pos + s) % 12)

    @pl.loop(0, 4 * (me < 8).astype(jnp.int32) + 4 * (me < 4).astype(jnp.int32))
    def _(s):
        kbuf[s] = jnp.zeros((rows, hdim), jnp.bfloat16)
        vbuf[s] = jnp.zeros((rows, hdim), jnp.bfloat16)

    first_over(LOW)

    @pl.loop(0, 2)
    def _(h):
        @pl.when(h == 1)
        def _():
            first_in(HIGH)
            first_over(HIGH)
            landed(pos, has2, "X2", "D2", which=LOW)
            landed(4 + pos_x, has1, "D1x", which=LOW)

        @pl.when(pairs[0][2])
        def _():
            sweep(pairs[0][0], pairs[0][1], h)

    def event1():
        landed(pos, has2, "X2", "D2", which=HIGH)
        landed(4 + pos_x, has1, "D1x", which=HIGH)

    def event2():
        landed(8 + pos_m, None)
        landed(4 + pos_d, has1)
        landed(pos_m, has2)
        landed(pos_x, has2 & leftc, "D2x", which=LOW)

    def event3():
        landed(pos_x, has2 & leftc, "D2x", which=HIGH)
        landed(pos_d, has2 & leftc)

    others = list(range(1, heads))
    order = [(p, d) for p in ORDER for d in (others if p < 4 else [heads])]
    order = [(p % 4, d) for p, d in order]
    kinds = [p if d < heads else p + 4 for p, d in order]
    events = ((1, event1), (2, event2), (3, event3))
    half = span // 2 if steps % 2 == 0 else span

    def choose(index, values):
        return sum((index == i) * jnp.asarray(x, jnp.int32) for i, x in enumerate(values))

    @pl.loop(0, len(order))
    def _(u):
        for kind, event in events:
            pl.when(u == kinds.index(kind))(event)
        p = choose(u, [x for x, _ in order])
        d = choose(u, [x for _, x in order])
        first = (mine + d) % heads * span

        valid = choose(p, [x[2] for x in pairs]) == 1
        slots = choose(p, [x[0] for x in pairs]), choose(p, [x[1] for x in pairs])
        closing = (p == 3) & (d < heads)

        @pl.when(valid & jnp.logical_not(closing))
        def _():
            unit(first, *slots, span)

        @pl.when(closing)
        def _():
            @pl.loop(0, span // half)
            def _(h):
                @pl.when(valid)
                def _():
                    unit(first + h * half, *slots, half)

                @pl.loop(0, half // tile)
                def _(x):
                    t = h * (half // tile) + x

                    def put(g, piece):
                        stage[d - 1, local(t), g * hdim:(g + 1) * hdim] = piece

                    finish(first, t, put)
                    outgoing(d, t).start()

        @pl.when((p == 3) & (d == heads))
        def _():
            @pl.loop(0, steps)
            def _(t):
                def put(g, piece):
                    where = pl.ds(pl.multiple_of(mine * (group * hdim) + g * hdim, hdim), hdim)
                    out_ref[local(t), where] = piece

                finish(first, t, put)

    for d in range(1, heads):
        @pl.loop(0, steps)
        def _(t):
            outgoing(d, t).wait_send()
            source = (mine + heads - d) % heads
            cols = pl.ds(pl.multiple_of(source * (group * hdim), group * hdim), group * hdim)
            got = out_ref.at[local(t), cols]
            pltpu.make_async_copy(got, got, orecv_sem.at[d - 1, t]).wait()

    for name in moves:
        sent(name)


def on_device(mesh, queries, keys, values, doc_lengths):
    rows, group, hdim = queries.shape
    heads = mesh.shape["head"]
    n = mesh.shape["ctx"]
    bf16, f32 = jnp.bfloat16, jnp.float32
    part = rows // heads
    tile = min(MOST, part * group)
    steps = part * group // tile
    vmem = pl.BlockSpec(memory_space=pltpu.VMEM)
    anywhere = pl.BlockSpec(memory_space=pl.ANY)
    return pl.pallas_call(
        functools.partial(kernel, n, heads, tile),
        out_shape=pltpu.VMEM((part, heads * group * hdim), bf16),
        in_specs=[pl.BlockSpec(memory_space=pltpu.SMEM), anywhere, anywhere, anywhere],
        out_specs=vmem,
        scratch_shapes=[
            pltpu.VMEM((12, rows, hdim), bf16),
            pltpu.VMEM((12, rows, hdim), bf16),
            pltpu.VMEM((12, rows, 128), bf16),
            pltpu.VMEM((rows * group, hdim + 128), bf16),
            pltpu.VMEM((rows * group, hdim + 128), f32),
            pltpu.VMEM((rows * group, 128), f32),
            pltpu.VMEM((tile, hdim), f32),
            pltpu.VMEM((heads - 1, part, group * hdim), bf16),
            pltpu.SemaphoreType.DMA((11, 4)),
            pltpu.SemaphoreType.DMA((12, 4)),
            pltpu.SemaphoreType.DMA((heads - 1, steps)),
            pltpu.SemaphoreType.DMA((heads - 1, steps)),
            pltpu.SemaphoreType.DMA((3,)),
        ],
        compiler_params=pltpu.CompilerParams(
            collective_id=0, has_side_effects=True, vmem_limit_bytes=56 * 1024 * 1024),
    )(doc_lengths, queries.reshape(rows * group, hdim), keys.reshape(rows, hdim), values.reshape(rows, hdim))


def solution(mesh):
    placed = (P("ctx", "head", None), P("ctx", "head", None), P("ctx", "head", None), P())
    return jax.shard_map(
        functools.partial(on_device, mesh), mesh=mesh, in_specs=placed,
        out_specs=P(("ctx", "head"), None), check_vma=False
    )
```

```python
import functools
import math

import jax
import jax.numpy as jnp
from jax import lax
from jax.experimental import pallas as pl
from jax.experimental.pallas import tpu as pltpu
from jax.sharding import PartitionSpec as P

MESH = pl.DeviceIdType.MESH
BIG = 1e30
MOST = 512
BAND = 128
ORDER = (1, 2, 3, 5, 6, 7)
LOW, HIGH = (0, 1), (2, 3)
ALL = LOW + HIGH


def kernel(n, heads, tile, lens_in, q_ref, k_ref, v_ref, out_ref,
           kbuf, vbuf, kdoc, qaug, acc, top, norm, stage,
           lens_ref, send_sem, recv_sem, osend_sem, orecv_sem, load_sem):
    rows, hdim = k_ref.shape
    total_rows = q_ref.shape[0]
    group = total_rows // rows
    me = lax.axis_index("ctx")
    mine = lax.axis_index("head")
    pos = me % 4
    core = pos % 2
    col = pos // 2
    mate = me + 1 - 2 * core
    across = me + 2 - 4 * col
    pos_m = pos + 1 - 2 * core
    pos_x = pos + 2 - 4 * col
    pos_d = pos_x + pos_m - pos
    has1 = me >= 4
    has2 = me >= 8
    feeds = me + 4 < n
    right = col == 1
    leftc = col == 0

    lens_load = pltpu.make_async_copy(lens_in, lens_ref, load_sem.at[3])
    lens_load.start()
    loads = (
        pltpu.make_async_copy(k_ref, kbuf.at[8 + pos], load_sem.at[0]),
        pltpu.make_async_copy(q_ref, qaug.at[:, 0:hdim], load_sem.at[1]),
        pltpu.make_async_copy(v_ref, vbuf.at[8 + pos], load_sem.at[2]),
    )
    for load in loads:
        load.start()

    barrier = pltpu.get_barrier_semaphore()
    for peer in (mate, across):
        pl.semaphore_signal(barrier, inc=1, device_id={"ctx": peer}, device_id_type=MESH)

    @pl.when(has1)
    def _():
        pl.semaphore_signal(barrier, inc=1, device_id={"ctx": me - 4}, device_id_type=MESH)

    @pl.when(feeds)
    def _():
        pl.semaphore_signal(barrier, inc=1, device_id={"ctx": me + 4}, device_id_type=MESH)

    for d in range(1, heads):
        pl.semaphore_signal(barrier, inc=1, device_id={"head": (mine + d) % heads}, device_id_type=MESH)

    half_keys = rows // 2
    parts = [(own, buf, pl.ds(h * half_keys, half_keys)) for h in range(2) for own, buf in ((k_ref, kbuf), (v_ref, vbuf))]

    def copies(lane, slot, to_slot, target):
        return [pltpu.make_async_remote_copy(
            src_ref=own.at[where] if slot is None else buf.at[slot, where],
            dst_ref=buf.at[to_slot, where],
            send_sem=send_sem.at[lane, w],
            recv_sem=recv_sem.at[to_slot, w],
            device_id={"ctx": target},
            device_id_type=MESH,
        ) for w, (own, buf, where) in enumerate(parts)]

    moves = {
        "D0": (copies(0, None, 8 + pos, mate), None),
        "X0": (copies(1, None, 8 + pos, across), leftc),
        "Z0": (copies(2, None, 4 + pos, me + 4), feeds),
        "D0x": (copies(3, 8 + pos_x, 8 + pos_x, mate), right),
        "D1": (copies(4, 4 + pos, 4 + pos, mate), has1),
        "X1": (copies(5, 4 + pos, 4 + pos, across), has1),
        "Z1": (copies(6, 4 + pos, pos, me + 4), has1 & feeds),
        "D1x": (copies(7, 4 + pos_x, 4 + pos_x, mate), has1),
        "D2": (copies(8, pos, pos, mate), has2),
        "X2": (copies(9, pos, pos, across), has2 & right),
        "D2x": (copies(10, pos_x, pos_x, mate), has2 & leftc),
    }

    def when(cond, fn):
        if cond is None:
            fn()
        else:
            pl.when(cond)(fn)

    def sent(name):
        made, cond = moves[name]

        def go():
            for copy in made:
                copy.wait_send()

        when(cond, go)

    def landed(slot, cond, *names, which=ALL):
        for w in which:
            _, buf, where = parts[w]

            def go():
                spot = buf.at[slot, where]
                pltpu.make_async_copy(spot, spot, recv_sem.at[slot, w]).wait()

            when(cond, go)
            for name in names:
                made, also = moves[name]
                when(also, made[w].start)

    def begin(which):
        for w in which:
            for name in ("Z0", "X0", "D0"):
                made, also = moves[name]
                when(also, made[w].start)

    lens_load.wait()

    lane = lax.broadcasted_iota(jnp.int32, (8, 128), 1)
    firsts = jnp.full((8, 128), 2**30, jnp.int32)
    ends = jnp.full((8, 128), 2**30, jnp.int32)
    run = jnp.int32(0)
    for d in range(lens_ref.shape[0]):
        firsts = jnp.where(lane == d, run, firsts)
        run = run + lens_ref[d]
        ends = jnp.where(lane == d, run, ends)
    first_row, end_row = firsts[0:1], ends[0:1]

    def member(position):
        return (position >= first_row) & (position < end_row)

    base = me * rows
    part = rows // heads
    tokens = tile // group
    steps = part // tokens
    span = part * group

    def by_token(width, dim):
        return lax.broadcasted_iota(jnp.int32, (tokens, group, width), dim).reshape(tile, width)

    @pl.loop(0, total_rows // tile)
    def _(t):
        at = pl.ds(pl.multiple_of(t * tile, tile), tile)
        qaug[at, hdim:] = jnp.where(member(base + t * tokens + by_token(128, 0)), 1.0, 0.0).astype(jnp.bfloat16)

    def mark(s):
        kpos = (me - pos - 8 + s) * rows + lax.broadcasted_iota(jnp.int32, (rows, 128), 0)
        kdoc[s] = jnp.where(member(kpos), 0.0, -BIG).astype(jnp.bfloat16)

    mark(8 + pos)
    pl.semaphore_wait(barrier, 1 + heads + has1.astype(jnp.int32) + feeds.astype(jnp.int32))
    begin(LOW)

    scale = math.log2(math.e) / hdim**0.5

    def spread(x, width):
        return jnp.concatenate([x] * (width // 128), axis=1)

    def raw(at, slot, width):
        return lax.dot_general(
            qaug[at, :], jnp.concatenate([kbuf[slot, 0:width, :], kdoc[slot, 0:width, :]], axis=1),
            (((1,), (1,)), ((), ())), preferred_element_type=jnp.float32)

    def mixed(weight, slot, width):
        ones = jnp.ones((width, 128), jnp.bfloat16)
        return jnp.dot(weight, jnp.concatenate([vbuf[slot, 0:width, :], ones], axis=1),
                       preferred_element_type=jnp.float32)

    def raw_pair(at, a, b, where):
        keys = [jnp.concatenate([kbuf[x, where, :], kdoc[x, where, :]], axis=1) for x in (a, b)]
        return lax.dot_general(
            qaug[at, :], jnp.concatenate(keys, axis=0), (((1,), (1,)), ((), ())), preferred_element_type=jnp.float32)

    def mixed_pair(weight, a, b, where):
        ones = jnp.ones((rows, 128), jnp.bfloat16)
        vals = jnp.concatenate([vbuf[a, where, :], vbuf[b, where, :]], axis=0)
        return jnp.dot(weight, jnp.concatenate([vals, ones], axis=1), preferred_element_type=jnp.float32)

    def flow(count, one, two, three):
        scores, weights = {}, {}
        for u in range(count + 2):
            if u >= 2:
                three(u - 2, *weights.pop(u - 2))
            if 1 <= u <= count:
                weights[u - 1] = two(u - 1, scores.pop(u - 1))
            if u < count:
                scores[u] = one(u)

    def diagonal():
        def width(t):
            return -(-(t + 1) * tokens // 128) * 128

        def at(t):
            return pl.ds(t * tile, tile)

        def one(t):
            return raw(at(t), 8 + pos, width(t))

        def two(t, s):
            wide, done = width(t), []
            for r in range(0, tile, BAND):
                here = slice(r, r + BAND)
                x = s[here, :] * scale
                edge = by_token(128, 2)[here] - by_token(128, 0)[here] <= t * tokens - (wide - 128)
                last = jnp.where(edge, x[:, wide - 128:], -BIG)
                x = last if wide == 128 else jnp.concatenate([x[:, :wide - 128], last], axis=1)
                m = jnp.broadcast_to(jnp.max(x, axis=1, keepdims=True), (BAND, 128))
                top[pl.ds(t * tile + r, BAND), :] = m
                done.append(jnp.exp2(x - spread(m, wide)).astype(jnp.bfloat16))
            return (jnp.concatenate(done, axis=0),)

        def three(t, weight):
            acc[at(t), :] = mixed(weight, 8 + pos, width(t))

        flow(total_rows // tile, one, two, three)

    def work(first, a, b, pieces):
        def at(r, size):
            return pl.ds(pl.multiple_of(first + r, BAND), size)

        def one(u):
            r, where = pieces[u]
            return raw_pair(at(r, tile), a, b, where)

        def two(u, s):
            done, factors = [], []
            for r in range(0, tile, BAND):
                x = s[r:r + BAND, :] * scale
                here = at(pieces[u][0] + r, BAND)
                m0 = top[here, :]
                m = jnp.maximum(m0, jnp.max(x, axis=1, keepdims=True))
                top[here, :] = m
                factors.append(jnp.exp2(m0 - m))
                done.append(jnp.exp2(x - spread(m, rows)).astype(jnp.bfloat16))
            return jnp.concatenate(done, axis=0), jnp.concatenate(factors, axis=0)

        def three(u, weight, factor):
            r, where = pieces[u]
            here = at(r, tile)
            acc[here, :] = acc[here, :] * spread(factor, 2 * hdim) + mixed_pair(weight, a, b, where)

        flow(len(pieces), one, two, three)

    def unit(first, a, b, extent):
        work(first, a, b, [(r, parts[w][2]) for r in range(0, extent, tile) for w in (0, 2)])

    def sweep(a, b, h):
        where = pl.ds(pl.multiple_of(h * half_keys, half_keys), half_keys)
        work(0, a, b, [(r, where) for r in range(0, total_rows, tile)])

    def pick(if_right, if_left):
        return col * if_right + (1 - col) * if_left

    near = core * (8 + pos_m) + (1 - core) * pos_m
    pairs = (
        (pick(8 + pos_x, 4 + pos), pick(8 + pos_d, 4 + pos_m), right | has1),
        (pick(4 + pos, 4 + pos_x), pick(4 + pos_m, pos), has1),
        (pick(4 + pos_x, 4 + pos_d), pick(4 + pos_d, near), has1 | (leftc & (core == 1))),
        (pick(pos, pos_x), pick(near, pos_d), has2 | (right & (core == 1))),
    )

    def local(t):
        return pl.ds(pl.multiple_of(t * tokens, tokens), tokens)

    def finish(first, t, put):
        whole = acc[pl.ds(pl.multiple_of(first + t * tile, tile), tile), :]
        norm[...] = whole[:, 0:hdim] / whole[:, hdim:]
        for g in range(group):
            put(g, norm[pl.ds(g, tokens, stride=group), :].astype(jnp.bfloat16))

    columns = pl.ds(pl.multiple_of(mine * (group * hdim), group * hdim), group * hdim)

    def outgoing(d, t):
        return pltpu.make_async_remote_copy(
            src_ref=stage.at[d - 1, local(t)],
            dst_ref=out_ref.at[local(t), columns],
            send_sem=osend_sem.at[d - 1, t],
            recv_sem=orecv_sem.at[d - 1, t],
            device_id={"head": (mine + d) % heads},
            device_id_type=MESH,
        )

    for load in loads:
        load.wait()
    diagonal()
    begin(HIGH)

    def first_in(which):
        landed(4 + pos, has1, "Z1", "X1", "D1", which=which)
        landed(8 + pos_x, right, "D0x", which=which)

    def first_over(which):
        landed(4 + pos_m, has1, which=which)
        landed(8 + pos_d, right, which=which)

    first_in(LOW)

    @pl.loop(1, 12)
    def _(s):
        mark((8 + pos + s) % 12)

    @pl.loop(0, 4 * (me < 8).astype(jnp.int32) + 4 * (me < 4).astype(jnp.int32))
    def _(s):
        kbuf[s] = jnp.zeros((rows, hdim), jnp.bfloat16)
        vbuf[s] = jnp.zeros((rows, hdim), jnp.bfloat16)

    first_over(LOW)

    @pl.loop(0, 2)
    def _(h):
        @pl.when(h == 1)
        def _():
            first_in(HIGH)
            first_over(HIGH)
            landed(pos, has2, "X2", "D2", which=LOW)
            landed(4 + pos_x, has1, "D1x", which=LOW)

        @pl.when(pairs[0][2])
        def _():
            sweep(pairs[0][0], pairs[0][1], h)

    def event1():
        landed(pos, has2, "X2", "D2", which=HIGH)
        landed(4 + pos_x, has1, "D1x", which=HIGH)

    def event2():
        landed(8 + pos_m, None)
        landed(4 + pos_d, has1)
        landed(pos_m, has2)
        landed(pos_x, has2 & leftc, "D2x", which=LOW)

    def event3():
        landed(pos_d, has2 & leftc)

    others = list(range(1, heads))
    order = [(p, d) for p in ORDER for d in (others if p < 4 else [heads])]
    order = [(p % 4, d) for p, d in order]
    kinds = [p if d < heads else p + 4 for p, d in order]
    events = ((1, event1), (2, event2), (3, event3))
    half = span // 2 if steps % 2 == 0 else span

    def choose(index, values):
        return sum((index == i) * jnp.asarray(x, jnp.int32) for i, x in enumerate(values))

    @pl.loop(0, len(order))
    def _(u):
        for kind, event in events:
            pl.when(u == kinds.index(kind))(event)
        p = choose(u, [x for x, _ in order])
        d = choose(u, [x for _, x in order])
        first = (mine + d) % heads * span

        valid = choose(p, [x[2] for x in pairs]) == 1
        slots = choose(p, [x[0] for x in pairs]), choose(p, [x[1] for x in pairs])
        closing = (p >= 2) & (d < heads)

        @pl.when(valid & jnp.logical_not(closing))
        def _():
            unit(first, *slots, span)

        @pl.when(closing)
        def _():
            @pl.loop(0, span // half)
            def _(h):
                @pl.when((u == kinds.index(2)) & (h == span // half - 1))
                def _():
                    landed(pos_x, has2 & leftc, "D2x", which=HIGH)

                @pl.when(valid)
                def _():
                    unit(first + h * half, *slots, half)

                @pl.loop(0, jnp.where(p == 3, half // tile, 0))
                def _(x):
                    t = h * (half // tile) + x

                    def put(g, piece):
                        stage[d - 1, local(t), g * hdim:(g + 1) * hdim] = piece

                    finish(first, t, put)
                    outgoing(d, t).start()

        @pl.when((p == 3) & (d == heads))
        def _():
            @pl.loop(0, steps)
            def _(t):
                def put(g, piece):
                    where = pl.ds(pl.multiple_of(mine * (group * hdim) + g * hdim, hdim), hdim)
                    out_ref[local(t), where] = piece

                finish(first, t, put)

    for d in range(1, heads):
        @pl.loop(0, steps)
        def _(t):
            outgoing(d, t).wait_send()
            source = (mine + heads - d) % heads
            cols = pl.ds(pl.multiple_of(source * (group * hdim), group * hdim), group * hdim)
            got = out_ref.at[local(t), cols]
            pltpu.make_async_copy(got, got, orecv_sem.at[d - 1, t]).wait()

    for name in moves:
        sent(name)


def on_device(mesh, queries, keys, values, doc_lengths):
    rows, group, hdim = queries.shape
    heads = mesh.shape["head"]
    n = mesh.shape["ctx"]
    bf16, f32 = jnp.bfloat16, jnp.float32
    part = rows // heads
    tile = min(MOST, part * group)
    steps = part * group // tile
    vmem = pl.BlockSpec(memory_space=pltpu.VMEM)
    anywhere = pl.BlockSpec(memory_space=pl.ANY)
    return pl.pallas_call(
        functools.partial(kernel, n, heads, tile),
        out_shape=pltpu.VMEM((part, heads * group * hdim), bf16),
        in_specs=[anywhere] * 4,
        out_specs=vmem,
        scratch_shapes=[
            pltpu.VMEM((12, rows, hdim), bf16),
            pltpu.VMEM((12, rows, hdim), bf16),
            pltpu.VMEM((12, rows, 128), bf16),
            pltpu.VMEM((rows * group, hdim + 128), bf16),
            pltpu.VMEM((rows * group, hdim + 128), f32),
            pltpu.VMEM((rows * group, 128), f32),
            pltpu.VMEM((tile, hdim), f32),
            pltpu.VMEM((heads - 1, part, group * hdim), bf16),
            pltpu.SMEM(doc_lengths.shape, jnp.int32),
            pltpu.SemaphoreType.DMA((11, 4)),
            pltpu.SemaphoreType.DMA((12, 4)),
            pltpu.SemaphoreType.DMA((heads - 1, steps)),
            pltpu.SemaphoreType.DMA((heads - 1, steps)),
            pltpu.SemaphoreType.DMA((4,)),
        ],
        compiler_params=pltpu.CompilerParams(
            collective_id=0, has_side_effects=True, vmem_limit_bytes=56 * 1024 * 1024),
    )(doc_lengths, queries.reshape(rows * group, hdim), keys.reshape(rows, hdim), values.reshape(rows, hdim))


def solution(mesh):
    placed = (P("ctx", "head", None), P("ctx", "head", None), P("ctx", "head", None), P())
    return jax.shard_map(
        functools.partial(on_device, mesh), mesh=mesh, in_specs=placed,
        out_specs=P(("ctx", "head"), None), check_vma=False
    )
```

```python
import functools
import math

import jax
import jax.numpy as jnp
from jax import lax
from jax.experimental import pallas as pl
from jax.experimental.pallas import tpu as pltpu
from jax.sharding import PartitionSpec as P

MESH = pl.DeviceIdType.MESH
BIG = 1e30
MOST = 512
BAND = 128
ORDER = (1, 2, 3, 5, 6, 7)
LOW, HIGH = (0, 1), (2, 3)
ALL = LOW + HIGH


def kernel(n, heads, tile, lens_in, q_ref, k_ref, v_ref, out_ref,
           kbuf, vbuf, kdoc, qaug, acc, top, norm, stage,
           lens_ref, send_sem, recv_sem, osend_sem, orecv_sem, load_sem):
    rows, hdim = k_ref.shape
    total_rows = q_ref.shape[0]
    group = total_rows // rows
    me = lax.axis_index("ctx")
    mine = lax.axis_index("head")
    pos = me % 4
    core = pos % 2
    col = pos // 2
    mate = me + 1 - 2 * core
    across = me + 2 - 4 * col
    pos_m = pos + 1 - 2 * core
    pos_x = pos + 2 - 4 * col
    pos_d = pos_x + pos_m - pos
    has1 = me >= 4
    has2 = me >= 8
    feeds = me + 4 < n
    right = col == 1
    leftc = col == 0

    lens_load = pltpu.make_async_copy(lens_in, lens_ref, load_sem.at[3])
    lens_load.start()
    loads = (
        pltpu.make_async_copy(k_ref, kbuf.at[8 + pos], load_sem.at[0]),
        pltpu.make_async_copy(q_ref, qaug.at[:, 0:hdim], load_sem.at[1]),
        pltpu.make_async_copy(v_ref, vbuf.at[8 + pos], load_sem.at[2]),
    )
    for load in loads:
        load.start()

    barrier = pltpu.get_barrier_semaphore()
    for peer in (mate, across):
        pl.semaphore_signal(barrier, inc=1, device_id={"ctx": peer}, device_id_type=MESH)

    @pl.when(has1)
    def _():
        pl.semaphore_signal(barrier, inc=1, device_id={"ctx": me - 4}, device_id_type=MESH)

    @pl.when(feeds)
    def _():
        pl.semaphore_signal(barrier, inc=1, device_id={"ctx": me + 4}, device_id_type=MESH)

    for d in range(1, heads):
        pl.semaphore_signal(barrier, inc=1, device_id={"head": (mine + d) % heads}, device_id_type=MESH)

    half_keys = rows // 2
    parts = [(own, buf, pl.ds(h * half_keys, half_keys)) for h in range(2) for own, buf in ((k_ref, kbuf), (v_ref, vbuf))]

    def copies(lane, slot, to_slot, target):
        return [pltpu.make_async_remote_copy(
            src_ref=own.at[where] if slot is None else buf.at[slot, where],
            dst_ref=buf.at[to_slot, where],
            send_sem=send_sem.at[lane, w],
            recv_sem=recv_sem.at[to_slot, w],
            device_id={"ctx": target},
            device_id_type=MESH,
        ) for w, (own, buf, where) in enumerate(parts)]

    moves = {
        "D0": (copies(0, None, 8 + pos, mate), None),
        "X0": (copies(1, None, 8 + pos, across), leftc),
        "Z0": (copies(2, None, 4 + pos, me + 4), feeds),
        "D0x": (copies(3, 8 + pos_x, 8 + pos_x, mate), right),
        "D1": (copies(4, 4 + pos, 4 + pos, mate), has1),
        "X1": (copies(5, 4 + pos, 4 + pos, across), has1),
        "Z1": (copies(6, 4 + pos, pos, me + 4), has1 & feeds),
        "D1x": (copies(7, 4 + pos_x, 4 + pos_x, mate), has1),
        "D2": (copies(8, pos, pos, mate), has2),
        "X2": (copies(9, pos, pos, across), has2 & right),
        "D2x": (copies(10, pos_x, pos_x, mate), has2 & leftc),
    }

    def when(cond, fn):
        if cond is None:
            fn()
        else:
            pl.when(cond)(fn)

    def sent(name):
        made, cond = moves[name]

        def go():
            for copy in made:
                copy.wait_send()

        when(cond, go)

    def landed(slot, cond, *names, which=ALL):
        for w in which:
            _, buf, where = parts[w]

            def go():
                spot = buf.at[slot, where]
                pltpu.make_async_copy(spot, spot, recv_sem.at[slot, w]).wait()

            when(cond, go)
            for name in names:
                made, also = moves[name]
                when(also, made[w].start)

    def begin(which):
        for w in which:
            for name in ("Z0", "X0", "D0"):
                made, also = moves[name]
                when(also, made[w].start)

    lens_load.wait()

    lane = lax.broadcasted_iota(jnp.int32, (8, 128), 1)
    firsts = jnp.full((8, 128), 2**30, jnp.int32)
    ends = jnp.full((8, 128), 2**30, jnp.int32)
    run = jnp.int32(0)
    for d in range(lens_ref.shape[0]):
        firsts = jnp.where(lane == d, run, firsts)
        run = run + lens_ref[d]
        ends = jnp.where(lane == d, run, ends)
    first_row, end_row = firsts[0:1], ends[0:1]

    def member(position):
        return (position >= first_row) & (position < end_row)

    base = me * rows
    part = rows // heads
    tokens = tile // group
    steps = part // tokens
    span = part * group
    swath = total_rows // 2

    def by_token(width, dim):
        return lax.broadcasted_iota(jnp.int32, (tokens, group, width), dim).reshape(tile, width)

    @pl.loop(0, total_rows // tile)
    def _(t):
        at = pl.ds(pl.multiple_of(t * tile, tile), tile)
        qaug[at, hdim:] = jnp.where(member(base + t * tokens + by_token(128, 0)), 1.0, 0.0).astype(jnp.bfloat16)

    def mark(s):
        kpos = (me - pos - 8 + s) * rows + lax.broadcasted_iota(jnp.int32, (rows, 128), 0)
        kdoc[s] = jnp.where(member(kpos), 0.0, -BIG).astype(jnp.bfloat16)

    mark(8 + pos)
    pl.semaphore_wait(barrier, 1 + heads + has1.astype(jnp.int32) + feeds.astype(jnp.int32))
    begin(LOW)

    scale = math.log2(math.e) / hdim**0.5

    def spread(x, width):
        return jnp.concatenate([x] * (width // 128), axis=1)

    def raw(at, slot, width):
        return lax.dot_general(
            qaug[at, :], jnp.concatenate([kbuf[slot, 0:width, :], kdoc[slot, 0:width, :]], axis=1),
            (((1,), (1,)), ((), ())), preferred_element_type=jnp.float32)

    def mixed(weight, slot, width):
        ones = jnp.ones((width, 128), jnp.bfloat16)
        return jnp.dot(weight, jnp.concatenate([vbuf[slot, 0:width, :], ones], axis=1),
                       preferred_element_type=jnp.float32)

    def raw_pair(at, a, b, where):
        keys = [jnp.concatenate([kbuf[x, where, :], kdoc[x, where, :]], axis=1) for x in (a, b)]
        return lax.dot_general(
            qaug[at, :], jnp.concatenate(keys, axis=0), (((1,), (1,)), ((), ())), preferred_element_type=jnp.float32)

    def mixed_pair(weight, a, b, where):
        ones = jnp.ones((rows, 128), jnp.bfloat16)
        vals = jnp.concatenate([vbuf[a, where, :], vbuf[b, where, :]], axis=0)
        return jnp.dot(weight, jnp.concatenate([vals, ones], axis=1), preferred_element_type=jnp.float32)

    def flow(count, one, two, three):
        scores, weights = {}, {}
        for u in range(count + 2):
            if u >= 2:
                three(u - 2, *weights.pop(u - 2))
            if 1 <= u <= count:
                weights[u - 1] = two(u - 1, scores.pop(u - 1))
            if u < count:
                scores[u] = one(u)

    def diagonal():
        def width(t):
            return -(-(t + 1) * tokens // 128) * 128

        def at(t):
            return pl.ds(t * tile, tile)

        def one(t):
            return raw(at(t), 8 + pos, width(t))

        def two(t, s):
            wide, done = width(t), []
            for r in range(0, tile, BAND):
                here = slice(r, r + BAND)
                x = s[here, :] * scale
                edge = by_token(128, 2)[here] - by_token(128, 0)[here] <= t * tokens - (wide - 128)
                last = jnp.where(edge, x[:, wide - 128:], -BIG)
                x = last if wide == 128 else jnp.concatenate([x[:, :wide - 128], last], axis=1)
                m = jnp.broadcast_to(jnp.max(x, axis=1, keepdims=True), (BAND, 128))
                top[pl.ds(t * tile + r, BAND), :] = m
                done.append(jnp.exp2(x - spread(m, wide)).astype(jnp.bfloat16))
            return (jnp.concatenate(done, axis=0),)

        def three(t, weight):
            acc[at(t), :] = mixed(weight, 8 + pos, width(t))

        flow(total_rows // tile, one, two, three)

    def work(first, a, b, pieces):
        def at(r, size):
            return pl.ds(pl.multiple_of(first + r, BAND), size)

        def one(u):
            r, where = pieces[u]
            return raw_pair(at(r, tile), a, b, where)

        def two(u, s):
            done, factors = [], []
            for r in range(0, tile, BAND):
                x = s[r:r + BAND, :] * scale
                here = at(pieces[u][0] + r, BAND)
                m0 = top[here, :]
                m = jnp.maximum(m0, jnp.max(x, axis=1, keepdims=True))
                top[here, :] = m
                factors.append(jnp.exp2(m0 - m))
                done.append(jnp.exp2(x - spread(m, rows)).astype(jnp.bfloat16))
            return jnp.concatenate(done, axis=0), jnp.concatenate(factors, axis=0)

        def three(u, weight, factor):
            r, where = pieces[u]
            here = at(r, tile)
            acc[here, :] = acc[here, :] * spread(factor, 2 * hdim) + mixed_pair(weight, a, b, where)

        flow(len(pieces), one, two, three)

    def unit(first, a, b, extent):
        work(first, a, b, [(r, parts[w][2]) for r in range(0, extent, tile) for w in (0, 2)])

    def sweep(first, a, b, h):
        where = pl.ds(pl.multiple_of(h * half_keys, half_keys), half_keys)
        work(first, a, b, [(r, where) for r in range(0, swath, tile)])

    def pick(if_right, if_left):
        return col * if_right + (1 - col) * if_left

    near = core * (8 + pos_m) + (1 - core) * pos_m
    pairs = (
        (pick(8 + pos_x, 4 + pos), pick(8 + pos_d, 4 + pos_m), right | has1),
        (pick(4 + pos, 4 + pos_x), pick(4 + pos_m, pos), has1),
        (pick(4 + pos_x, 4 + pos_d), pick(4 + pos_d, near), has1 | (leftc & (core == 1))),
        (pick(pos, pos_x), pick(near, pos_d), has2 | (right & (core == 1))),
    )

    def local(t):
        return pl.ds(pl.multiple_of(t * tokens, tokens), tokens)

    def finish(first, t, put):
        whole = acc[pl.ds(pl.multiple_of(first + t * tile, tile), tile), :]
        norm[...] = whole[:, 0:hdim] / whole[:, hdim:]
        for g in range(group):
            put(g, norm[pl.ds(g, tokens, stride=group), :].astype(jnp.bfloat16))

    columns = pl.ds(pl.multiple_of(mine * (group * hdim), group * hdim), group * hdim)

    def outgoing(d, t):
        return pltpu.make_async_remote_copy(
            src_ref=stage.at[d - 1, local(t)],
            dst_ref=out_ref.at[local(t), columns],
            send_sem=osend_sem.at[d - 1, t],
            recv_sem=orecv_sem.at[d - 1, t],
            device_id={"head": (mine + d) % heads},
            device_id_type=MESH,
        )

    for load in loads:
        load.wait()
    diagonal()
    begin(HIGH)

    def first_in(which):
        landed(4 + pos, has1, "Z1", "X1", "D1", which=which)
        landed(8 + pos_x, right, "D0x", which=which)

    def first_over(which):
        landed(4 + pos_m, has1, which=which)
        landed(8 + pos_d, right, which=which)

    first_in(LOW)

    @pl.loop(1, 12)
    def _(s):
        mark((8 + pos + s) % 12)

    @pl.loop(0, 4 * (me < 8).astype(jnp.int32) + 4 * (me < 4).astype(jnp.int32))
    def _(s):
        kbuf[s] = jnp.zeros((rows, hdim), jnp.bfloat16)
        vbuf[s] = jnp.zeros((rows, hdim), jnp.bfloat16)

    first_over(LOW)

    @pl.loop(0, 4)
    def _(i):
        @pl.when(i == 1)
        def _():
            first_in(HIGH)

        @pl.when(i == 2)
        def _():
            first_over(HIGH)

        @pl.when(i == 3)
        def _():
            landed(pos, has2, "X2", "D2", which=LOW)
            landed(4 + pos_x, has1, "D1x", which=LOW)

        @pl.when(pairs[0][2])
        def _():
            sweep(i % 2 * swath, pairs[0][0], pairs[0][1], i // 2)

    def event1():
        landed(pos, has2, "X2", "D2", which=HIGH)
        landed(4 + pos_x, has1, "D1x", which=HIGH)

    def event2():
        landed(8 + pos_m, None)
        landed(4 + pos_d, has1)
        landed(pos_m, has2)
        landed(pos_x, has2 & leftc, "D2x", which=LOW)

    def event3():
        landed(pos_d, has2 & leftc)

    others = list(range(1, heads))
    order = [(p, d) for p in ORDER for d in (others if p < 4 else [heads])]
    order = [(p % 4, d) for p, d in order]
    kinds = [p if d < heads else p + 4 for p, d in order]
    events = ((1, event1), (2, event2), (3, event3))
    half = span // 2 if steps % 2 == 0 else span

    def choose(index, values):
        return sum((index == i) * jnp.asarray(x, jnp.int32) for i, x in enumerate(values))

    @pl.loop(0, len(order))
    def _(u):
        for kind, event in events:
            pl.when(u == kinds.index(kind))(event)
        p = choose(u, [x for x, _ in order])
        d = choose(u, [x for _, x in order])
        first = (mine + d) % heads * span

        valid = choose(p, [x[2] for x in pairs]) == 1
        slots = choose(p, [x[0] for x in pairs]), choose(p, [x[1] for x in pairs])
        closing = (p >= 2) & (d < heads)

        @pl.when(valid & jnp.logical_not(closing))
        def _():
            unit(first, *slots, span)

        @pl.when(closing)
        def _():
            @pl.loop(0, span // half)
            def _(h):
                @pl.when((u == kinds.index(2)) & (h == span // half - 1))
                def _():
                    landed(pos_x, has2 & leftc, "D2x", which=HIGH)

                @pl.when(valid)
                def _():
                    unit(first + h * half, *slots, half)

                @pl.loop(0, jnp.where(p == 3, half // tile, 0))
                def _(x):
                    t = h * (half // tile) + x

                    def put(g, piece):
                        stage[d - 1, local(t), g * hdim:(g + 1) * hdim] = piece

                    finish(first, t, put)
                    outgoing(d, t).start()

        @pl.when((p == 3) & (d == heads))
        def _():
            @pl.loop(0, steps)
            def _(t):
                def put(g, piece):
                    where = pl.ds(pl.multiple_of(mine * (group * hdim) + g * hdim, hdim), hdim)
                    out_ref[local(t), where] = piece

                finish(first, t, put)

    for d in range(1, heads):
        @pl.loop(0, steps)
        def _(t):
            outgoing(d, t).wait_send()
            source = (mine + heads - d) % heads
            cols = pl.ds(pl.multiple_of(source * (group * hdim), group * hdim), group * hdim)
            got = out_ref.at[local(t), cols]
            pltpu.make_async_copy(got, got, orecv_sem.at[d - 1, t]).wait()

    for name in moves:
        sent(name)


def on_device(mesh, queries, keys, values, doc_lengths):
    rows, group, hdim = queries.shape
    heads = mesh.shape["head"]
    n = mesh.shape["ctx"]
    bf16, f32 = jnp.bfloat16, jnp.float32
    part = rows // heads
    tile = min(MOST, part * group)
    steps = part * group // tile
    vmem = pl.BlockSpec(memory_space=pltpu.VMEM)
    anywhere = pl.BlockSpec(memory_space=pl.ANY)
    return pl.pallas_call(
        functools.partial(kernel, n, heads, tile),
        out_shape=pltpu.VMEM((part, heads * group * hdim), bf16),
        in_specs=[anywhere] * 4,
        out_specs=vmem,
        scratch_shapes=[
            pltpu.VMEM((12, rows, hdim), bf16),
            pltpu.VMEM((12, rows, hdim), bf16),
            pltpu.VMEM((12, rows, 128), bf16),
            pltpu.VMEM((rows * group, hdim + 128), bf16),
            pltpu.VMEM((rows * group, hdim + 128), f32),
            pltpu.VMEM((rows * group, 128), f32),
            pltpu.VMEM((tile, hdim), f32),
            pltpu.VMEM((heads - 1, part, group * hdim), bf16),
            pltpu.SMEM(doc_lengths.shape, jnp.int32),
            pltpu.SemaphoreType.DMA((11, 4)),
            pltpu.SemaphoreType.DMA((12, 4)),
            pltpu.SemaphoreType.DMA((heads - 1, steps)),
            pltpu.SemaphoreType.DMA((heads - 1, steps)),
            pltpu.SemaphoreType.DMA((4,)),
        ],
        compiler_params=pltpu.CompilerParams(
            collective_id=0, has_side_effects=True, vmem_limit_bytes=56 * 1024 * 1024),
    )(doc_lengths, queries.reshape(rows * group, hdim), keys.reshape(rows, hdim), values.reshape(rows, hdim))


def solution(mesh):
    placed = (P("ctx", "head", None), P("ctx", "head", None), P("ctx", "head", None), P())
    return jax.shard_map(
        functools.partial(on_device, mesh), mesh=mesh, in_specs=placed,
        out_specs=P(("ctx", "head"), None), check_vma=False
    )
```

```python
import functools
import math

import jax
import jax.numpy as jnp
from jax import lax
from jax.experimental import pallas as pl
from jax.experimental.pallas import tpu as pltpu
from jax.sharding import PartitionSpec as P

MESH = pl.DeviceIdType.MESH
BIG = 1e30
MOST = 512
BAND = 128
ORDER = (1, 2, 3, 5, 6, 7)
LOW, HIGH = (0, 1), (2, 3)
ALL = LOW + HIGH


def kernel(n, heads, tile, lens_in, q_ref, k_ref, v_ref, out_ref,
           kbuf, vbuf, kdoc, qaug, acc, top, norm, stage,
           lens_ref, send_sem, recv_sem, osend_sem, orecv_sem, load_sem):
    rows, hdim = k_ref.shape
    total_rows = q_ref.shape[0]
    group = total_rows // rows
    me = lax.axis_index("ctx")
    mine = lax.axis_index("head")
    pos = me % 4
    core = pos % 2
    col = pos // 2
    mate = me + 1 - 2 * core
    across = me + 2 - 4 * col
    pos_m = pos + 1 - 2 * core
    pos_x = pos + 2 - 4 * col
    pos_d = pos_x + pos_m - pos
    has1 = me >= 4
    has2 = me >= 8
    feeds = me + 4 < n
    right = col == 1
    leftc = col == 0

    lens_load = pltpu.make_async_copy(lens_in, lens_ref, load_sem.at[3])
    lens_load.start()
    loads = (
        pltpu.make_async_copy(k_ref, kbuf.at[8 + pos], load_sem.at[0]),
        pltpu.make_async_copy(q_ref, qaug.at[:, 0:hdim], load_sem.at[1]),
        pltpu.make_async_copy(v_ref, vbuf.at[8 + pos], load_sem.at[2]),
    )
    for load in loads:
        load.start()

    barrier = pltpu.get_barrier_semaphore()
    for peer in (mate, across):
        pl.semaphore_signal(barrier, inc=1, device_id={"ctx": peer}, device_id_type=MESH)

    @pl.when(has1)
    def _():
        pl.semaphore_signal(barrier, inc=1, device_id={"ctx": me - 4}, device_id_type=MESH)

    @pl.when(feeds)
    def _():
        pl.semaphore_signal(barrier, inc=1, device_id={"ctx": me + 4}, device_id_type=MESH)

    for d in range(1, heads):
        pl.semaphore_signal(barrier, inc=1, device_id={"head": (mine + d) % heads}, device_id_type=MESH)

    half_keys = rows // 2
    parts = [(own, buf, pl.ds(h * half_keys, half_keys)) for h in range(2) for own, buf in ((k_ref, kbuf), (v_ref, vbuf))]

    def copies(lane, slot, to_slot, target):
        return [pltpu.make_async_remote_copy(
            src_ref=own.at[where] if slot is None else buf.at[slot, where],
            dst_ref=buf.at[to_slot, where],
            send_sem=send_sem.at[lane, w],
            recv_sem=recv_sem.at[to_slot, w],
            device_id={"ctx": target},
            device_id_type=MESH,
        ) for w, (own, buf, where) in enumerate(parts)]

    moves = {
        "D0": (copies(0, None, 8 + pos, mate), None),
        "X0": (copies(1, None, 8 + pos, across), leftc),
        "Z0": (copies(2, None, 4 + pos, me + 4), feeds),
        "D0x": (copies(3, 8 + pos_x, 8 + pos_x, mate), right),
        "D1": (copies(4, 4 + pos, 4 + pos, mate), has1),
        "X1": (copies(5, 4 + pos, 4 + pos, across), has1),
        "Z1": (copies(6, 4 + pos, pos, me + 4), has1 & feeds),
        "D1x": (copies(7, 4 + pos_x, 4 + pos_x, mate), has1),
        "D2": (copies(8, pos, pos, mate), has2),
        "X2": (copies(9, pos, pos, across), has2 & right),
        "D2x": (copies(10, pos_x, pos_x, mate), has2 & leftc),
    }

    def when(cond, fn):
        if cond is None:
            fn()
        else:
            pl.when(cond)(fn)

    def sent(name):
        made, cond = moves[name]

        def go():
            for copy in made:
                copy.wait_send()

        when(cond, go)

    def landed(slot, cond, *names, which=ALL):
        for w in which:
            _, buf, where = parts[w]

            def go():
                spot = buf.at[slot, where]
                pltpu.make_async_copy(spot, spot, recv_sem.at[slot, w]).wait()

            when(cond, go)
            for name in names:
                made, also = moves[name]
                when(also, made[w].start)

    def begin(which):
        for w in which:
            for name in ("Z0", "X0", "D0"):
                made, also = moves[name]
                when(also, made[w].start)

    lens_load.wait()

    lane = lax.broadcasted_iota(jnp.int32, (8, 128), 1)
    firsts = jnp.full((8, 128), 2**30, jnp.int32)
    ends = jnp.full((8, 128), 2**30, jnp.int32)
    run = jnp.int32(0)
    for d in range(lens_ref.shape[0]):
        firsts = jnp.where(lane == d, run, firsts)
        run = run + lens_ref[d]
        ends = jnp.where(lane == d, run, ends)
    first_row, end_row = firsts[0:1], ends[0:1]

    def member(position):
        return (position >= first_row) & (position < end_row)

    base = me * rows
    part = rows // heads
    tokens = tile // group
    steps = part // tokens
    span = part * group
    swath = total_rows // 2

    def by_token(width, dim):
        return lax.broadcasted_iota(jnp.int32, (tokens, group, width), dim).reshape(tile, width)

    @pl.loop(0, total_rows // tile)
    def _(t):
        at = pl.ds(pl.multiple_of(t * tile, tile), tile)
        qaug[at, hdim:] = jnp.where(member(base + t * tokens + by_token(128, 0)), 1.0, 0.0).astype(jnp.bfloat16)

    def mark(s):
        kpos = (me - pos - 8 + s) * rows + lax.broadcasted_iota(jnp.int32, (rows, 128), 0)
        kdoc[s] = jnp.where(member(kpos), 0.0, -BIG).astype(jnp.bfloat16)

    mark(8 + pos)
    pl.semaphore_wait(barrier, 1 + heads + has1.astype(jnp.int32) + feeds.astype(jnp.int32))
    begin(LOW)

    scale = math.log2(math.e) / hdim**0.5

    def spread(x, width):
        return jnp.concatenate([x] * (width // 128), axis=1)

    def raw(at, slot, width):
        return lax.dot_general(
            qaug[at, :], jnp.concatenate([kbuf[slot, 0:width, :], kdoc[slot, 0:width, :]], axis=1),
            (((1,), (1,)), ((), ())), preferred_element_type=jnp.float32)

    def mixed(weight, slot, width):
        ones = jnp.ones((width, 128), jnp.bfloat16)
        return jnp.dot(weight, jnp.concatenate([vbuf[slot, 0:width, :], ones], axis=1),
                       preferred_element_type=jnp.float32)

    def raw_pair(at, a, b, where):
        keys = [jnp.concatenate([kbuf[x, where, :], kdoc[x, where, :]], axis=1) for x in (a, b)]
        return lax.dot_general(
            qaug[at, :], jnp.concatenate(keys, axis=0), (((1,), (1,)), ((), ())), preferred_element_type=jnp.float32)

    def mixed_pair(weight, a, b, where):
        ones = jnp.ones((rows, 128), jnp.bfloat16)
        vals = jnp.concatenate([vbuf[a, where, :], vbuf[b, where, :]], axis=0)
        return jnp.dot(weight, jnp.concatenate([vals, ones], axis=1), preferred_element_type=jnp.float32)

    def flow(count, one, two, three):
        scores, weights = {}, {}
        for u in range(count + 2):
            if u >= 2:
                three(u - 2, *weights.pop(u - 2))
            if 1 <= u <= count:
                weights[u - 1] = two(u - 1, scores.pop(u - 1))
            if u < count:
                scores[u] = one(u)

    def diagonal():
        def width(t):
            return -(-(t + 1) * tokens // 128) * 128

        def at(t):
            return pl.ds(t * tile, tile)

        def one(t):
            return raw(at(t), 8 + pos, width(t))

        def two(t, s):
            wide, done = width(t), []
            for r in range(0, tile, BAND):
                here = slice(r, r + BAND)
                x = s[here, :] * scale
                edge = by_token(128, 2)[here] - by_token(128, 0)[here] <= t * tokens - (wide - 128)
                last = jnp.where(edge, x[:, wide - 128:], -BIG)
                x = last if wide == 128 else jnp.concatenate([x[:, :wide - 128], last], axis=1)
                m = jnp.broadcast_to(jnp.max(x, axis=1, keepdims=True), (BAND, 128))
                top[pl.ds(t * tile + r, BAND), :] = m
                done.append(jnp.exp2(x - spread(m, wide)).astype(jnp.bfloat16))
            return (jnp.concatenate(done, axis=0),)

        def three(t, weight):
            acc[at(t), :] = mixed(weight, 8 + pos, width(t))

        flow(total_rows // tile, one, two, three)

    def work(first, a, b, pieces):
        def at(r, size):
            return pl.ds(pl.multiple_of(first + r, BAND), size)

        def one(u):
            r, where = pieces[u]
            return raw_pair(at(r, tile), a, b, where)

        def two(u, s):
            done, factors = [], []
            for r in range(0, tile, BAND):
                x = s[r:r + BAND, :] * scale
                here = at(pieces[u][0] + r, BAND)
                m0 = top[here, :]
                m = jnp.maximum(m0, jnp.max(x, axis=1, keepdims=True))
                top[here, :] = m
                factors.append(jnp.exp2(m0 - m))
                done.append(jnp.exp2(x - spread(m, rows)).astype(jnp.bfloat16))
            return jnp.concatenate(done, axis=0), jnp.concatenate(factors, axis=0)

        def three(u, weight, factor):
            r, where = pieces[u]
            here = at(r, tile)
            acc[here, :] = acc[here, :] * spread(factor, 2 * hdim) + mixed_pair(weight, a, b, where)

        flow(len(pieces), one, two, three)

    def unit(first, a, b, extent):
        work(first, a, b, [(r, parts[w][2]) for r in range(0, extent, tile) for w in (0, 2)])

    def sweep(first, a, b, h):
        where = pl.ds(pl.multiple_of(h * half_keys, half_keys), half_keys)
        work(first, a, b, [(r, where) for r in range(0, swath, tile)])

    def pick(if_right, if_left):
        return col * if_right + (1 - col) * if_left

    near = core * (8 + pos_m) + (1 - core) * pos_m
    pairs = (
        (pick(8 + pos_x, 4 + pos), pick(8 + pos_d, 4 + pos_m), right | has1),
        (pick(4 + pos, 4 + pos_x), pick(4 + pos_m, pos), has1),
        (pick(4 + pos_x, 4 + pos_d), pick(4 + pos_d, near), has1 | (leftc & (core == 1))),
        (pick(pos, pos_x), pick(near, pos_d), has2 | (right & (core == 1))),
    )

    def local(t):
        return pl.ds(pl.multiple_of(t * tokens, tokens), tokens)

    def finish(first, t, put):
        whole = acc[pl.ds(pl.multiple_of(first + t * tile, tile), tile), :]
        norm[...] = whole[:, 0:hdim] / whole[:, hdim:]
        for g in range(group):
            put(g, norm[pl.ds(g, tokens, stride=group), :].astype(jnp.bfloat16))

    columns = pl.ds(pl.multiple_of(mine * (group * hdim), group * hdim), group * hdim)

    def outgoing(d, t):
        return pltpu.make_async_remote_copy(
            src_ref=stage.at[d - 1, local(t)],
            dst_ref=out_ref.at[local(t), columns],
            send_sem=osend_sem.at[d - 1, t],
            recv_sem=orecv_sem.at[d - 1, t],
            device_id={"head": (mine + d) % heads},
            device_id_type=MESH,
        )

    for load in loads:
        load.wait()
    diagonal()
    begin(HIGH)

    def first_in(which):
        landed(4 + pos, has1, "Z1", "X1", "D1", which=which)
        landed(8 + pos_x, right, "D0x", which=which)

    def first_over(which):
        landed(4 + pos_m, has1, which=which)
        landed(8 + pos_d, right, which=which)

    @pl.loop(1, 12)
    def _(s):
        mark((8 + pos + s) % 12)

    @pl.loop(0, 4 * (me < 8).astype(jnp.int32) + 4 * (me < 4).astype(jnp.int32))
    def _(s):
        kbuf[s] = jnp.zeros((rows, hdim), jnp.bfloat16)
        vbuf[s] = jnp.zeros((rows, hdim), jnp.bfloat16)

    first_in(LOW)
    first_over(LOW)

    @pl.loop(0, 4)
    def _(i):
        @pl.when(i == 1)
        def _():
            first_in(HIGH)

        @pl.when(i == 2)
        def _():
            first_over(HIGH)

        @pl.when(i == 3)
        def _():
            landed(pos, has2, "X2", "D2", which=LOW)
            landed(4 + pos_x, has1, "D1x", which=LOW)

        @pl.when(pairs[0][2])
        def _():
            sweep(i % 2 * swath, pairs[0][0], pairs[0][1], i // 2)

    def event1():
        landed(pos, has2, "X2", "D2", which=HIGH)
        landed(4 + pos_x, has1, "D1x", which=HIGH)

    def event2():
        landed(8 + pos_m, None)
        landed(4 + pos_d, has1)
        landed(pos_m, has2)
        landed(pos_x, has2 & leftc, "D2x", which=LOW)

    def event3():
        landed(pos_x, has2 & leftc, "D2x", which=HIGH)
        landed(pos_d, has2 & leftc)

    others = list(range(1, heads))
    order = [(p, d) for p in ORDER for d in (others if p < 4 else [heads])]
    order = [(p % 4, d) for p, d in order]
    kinds = [p if d < heads else p + 4 for p, d in order]
    events = ((1, event1), (2, event2), (3, event3))

    def choose(index, values):
        return sum((index == i) * jnp.asarray(x, jnp.int32) for i, x in enumerate(values))

    @pl.loop(0, len(order))
    def _(u):
        for kind, event in events:
            pl.when(u == kinds.index(kind))(event)
        p = choose(u, [x for x, _ in order])
        d = choose(u, [x for _, x in order])
        first = (mine + d) % heads * span

        valid = choose(p, [x[2] for x in pairs]) == 1
        slots = choose(p, [x[0] for x in pairs]), choose(p, [x[1] for x in pairs])
        closing = (p == 3) & (d < heads)

        @pl.when(valid & jnp.logical_not(closing))
        def _():
            unit(first, *slots, span)

        @pl.when(closing)
        def _():
            @pl.loop(0, steps)
            def _(t):
                @pl.when(valid)
                def _():
                    unit(first + t * tile, *slots, tile)

                def put(g, piece):
                    stage[d - 1, local(t), g * hdim:(g + 1) * hdim] = piece

                finish(first, t, put)
                outgoing(d, t).start()

        @pl.when((p == 3) & (d == heads))
        def _():
            @pl.loop(0, steps)
            def _(t):
                def put(g, piece):
                    where = pl.ds(pl.multiple_of(mine * (group * hdim) + g * hdim, hdim), hdim)
                    out_ref[local(t), where] = piece

                finish(first, t, put)

    for d in range(1, heads):
        @pl.loop(0, steps)
        def _(t):
            outgoing(d, t).wait_send()
            source = (mine + heads - d) % heads
            cols = pl.ds(pl.multiple_of(source * (group * hdim), group * hdim), group * hdim)
            got = out_ref.at[local(t), cols]
            pltpu.make_async_copy(got, got, orecv_sem.at[d - 1, t]).wait()

    for name in moves:
        sent(name)


def on_device(mesh, queries, keys, values, doc_lengths):
    rows, group, hdim = queries.shape
    heads = mesh.shape["head"]
    n = mesh.shape["ctx"]
    bf16, f32 = jnp.bfloat16, jnp.float32
    part = rows // heads
    tile = min(MOST, part * group)
    steps = part * group // tile
    vmem = pl.BlockSpec(memory_space=pltpu.VMEM)
    anywhere = pl.BlockSpec(memory_space=pl.ANY)
    return pl.pallas_call(
        functools.partial(kernel, n, heads, tile),
        out_shape=pltpu.VMEM((part, heads * group * hdim), bf16),
        in_specs=[anywhere] * 4,
        out_specs=vmem,
        scratch_shapes=[
            pltpu.VMEM((12, rows, hdim), bf16),
            pltpu.VMEM((12, rows, hdim), bf16),
            pltpu.VMEM((12, rows, 128), bf16),
            pltpu.VMEM((rows * group, hdim + 128), bf16),
            pltpu.VMEM((rows * group, hdim + 128), f32),
            pltpu.VMEM((rows * group, 128), f32),
            pltpu.VMEM((tile, hdim), f32),
            pltpu.VMEM((heads - 1, part, group * hdim), bf16),
            pltpu.SMEM(doc_lengths.shape, jnp.int32),
            pltpu.SemaphoreType.DMA((11, 4)),
            pltpu.SemaphoreType.DMA((12, 4)),
            pltpu.SemaphoreType.DMA((heads - 1, steps)),
            pltpu.SemaphoreType.DMA((heads - 1, steps)),
            pltpu.SemaphoreType.DMA((4,)),
        ],
        compiler_params=pltpu.CompilerParams(
            collective_id=0, has_side_effects=True, vmem_limit_bytes=56 * 1024 * 1024),
    )(doc_lengths, queries.reshape(rows * group, hdim), keys.reshape(rows, hdim), values.reshape(rows, hdim))


def solution(mesh):
    placed = (P("ctx", "head", None), P("ctx", "head", None), P("ctx", "head", None), P())
    return jax.shard_map(
        functools.partial(on_device, mesh), mesh=mesh, in_specs=placed,
        out_specs=P(("ctx", "head"), None), check_vma=False
    )
```

```python
import functools
import math

import jax
import jax.numpy as jnp
from jax import lax
from jax.experimental import pallas as pl
from jax.experimental.pallas import tpu as pltpu
from jax.sharding import PartitionSpec as P

MESH = pl.DeviceIdType.MESH
BIG = 1e30
MOST = 512
BAND = 128
ORDER = (1, 2, 3, 5, 6, 7)
LOW, HIGH = (0, 1), (2, 3)
ALL = LOW + HIGH


def kernel(n, heads, tile, lens_in, q_ref, k_ref, v_ref, out_ref,
           kbuf, vbuf, kdoc, qaug, acc, top, norm, stage,
           lens_ref, send_sem, recv_sem, osend_sem, orecv_sem, load_sem):
    rows, hdim = k_ref.shape
    total_rows = q_ref.shape[0]
    group = total_rows // rows
    me = lax.axis_index("ctx")
    mine = lax.axis_index("head")
    pos = me % 4
    core = pos % 2
    col = pos // 2
    mate = me + 1 - 2 * core
    across = me + 2 - 4 * col
    pos_m = pos + 1 - 2 * core
    pos_x = pos + 2 - 4 * col
    pos_d = pos_x + pos_m - pos
    has1 = me >= 4
    has2 = me >= 8
    feeds = me + 4 < n
    right = col == 1
    leftc = col == 0

    lens_load = pltpu.make_async_copy(lens_in, lens_ref, load_sem.at[3])
    lens_load.start()
    loads = (
        pltpu.make_async_copy(k_ref, kbuf.at[8 + pos], load_sem.at[0]),
        pltpu.make_async_copy(q_ref, qaug.at[:, 0:hdim], load_sem.at[1]),
        pltpu.make_async_copy(v_ref, vbuf.at[8 + pos], load_sem.at[2]),
    )
    for load in loads:
        load.start()

    barrier = pltpu.get_barrier_semaphore()
    for peer in (mate, across):
        pl.semaphore_signal(barrier, inc=1, device_id={"ctx": peer}, device_id_type=MESH)

    @pl.when(has1)
    def _():
        pl.semaphore_signal(barrier, inc=1, device_id={"ctx": me - 4}, device_id_type=MESH)

    @pl.when(feeds)
    def _():
        pl.semaphore_signal(barrier, inc=1, device_id={"ctx": me + 4}, device_id_type=MESH)

    for d in range(1, heads):
        pl.semaphore_signal(barrier, inc=1, device_id={"head": (mine + d) % heads}, device_id_type=MESH)

    half_keys = rows // 2
    parts = [(own, buf, pl.ds(h * half_keys, half_keys)) for h in range(2) for own, buf in ((k_ref, kbuf), (v_ref, vbuf))]

    def copies(lane, slot, to_slot, target):
        return [pltpu.make_async_remote_copy(
            src_ref=own.at[where] if slot is None else buf.at[slot, where],
            dst_ref=buf.at[to_slot, where],
            send_sem=send_sem.at[lane, w],
            recv_sem=recv_sem.at[to_slot, w],
            device_id={"ctx": target},
            device_id_type=MESH,
        ) for w, (own, buf, where) in enumerate(parts)]

    moves = {
        "D0": (copies(0, None, 8 + pos, mate), None),
        "X0": (copies(1, None, 8 + pos, across), leftc),
        "Z0": (copies(2, None, 4 + pos, me + 4), feeds),
        "D0x": (copies(3, 8 + pos_x, 8 + pos_x, mate), right),
        "D1": (copies(4, 4 + pos, 4 + pos, mate), has1),
        "X1": (copies(5, 4 + pos, 4 + pos, across), has1),
        "Z1": (copies(6, 4 + pos, pos, me + 4), has1 & feeds),
        "D1x": (copies(7, 4 + pos_x, 4 + pos_x, mate), has1),
        "D2": (copies(8, pos, pos, mate), has2),
        "X2": (copies(9, pos, pos, across), has2 & right),
        "D2x": (copies(10, pos_x, pos_x, mate), has2 & leftc),
    }

    def when(cond, fn):
        if cond is None:
            fn()
        else:
            pl.when(cond)(fn)

    def sent(name):
        made, cond = moves[name]

        def go():
            for copy in made:
                copy.wait_send()

        when(cond, go)

    def landed(slot, cond, *names, which=ALL):
        for w in which:
            _, buf, where = parts[w]

            def go():
                spot = buf.at[slot, where]
                pltpu.make_async_copy(spot, spot, recv_sem.at[slot, w]).wait()

            when(cond, go)
            for name in names:
                made, also = moves[name]
                when(cond if also is None else cond & also, made[w].start)

    def begin(which):
        for w in which:
            for name in ("Z0", "X0", "D0"):
                made, also = moves[name]
                when(also, made[w].start)

    lens_load.wait()

    lane = lax.broadcasted_iota(jnp.int32, (8, 128), 1)
    firsts = jnp.full((8, 128), 2**30, jnp.int32)
    ends = jnp.full((8, 128), 2**30, jnp.int32)
    run = jnp.int32(0)
    for d in range(lens_ref.shape[0]):
        firsts = jnp.where(lane == d, run, firsts)
        run = run + lens_ref[d]
        ends = jnp.where(lane == d, run, ends)
    first_row, end_row = firsts[0:1], ends[0:1]

    def member(position):
        return (position >= first_row) & (position < end_row)

    base = me * rows
    part = rows // heads
    tokens = tile // group
    steps = part // tokens
    span = part * group
    swath = total_rows // 2

    def by_token(width, dim):
        return lax.broadcasted_iota(jnp.int32, (tokens, group, width), dim).reshape(tile, width)

    @pl.loop(0, total_rows // tile)
    def _(t):
        at = pl.ds(pl.multiple_of(t * tile, tile), tile)
        qaug[at, hdim:] = jnp.where(member(base + t * tokens + by_token(128, 0)), 1.0, 0.0).astype(jnp.bfloat16)

    def mark(s):
        kpos = (me - pos - 8 + s) * rows + lax.broadcasted_iota(jnp.int32, (rows, 128), 0)
        kdoc[s] = jnp.where(member(kpos), 0.0, -BIG).astype(jnp.bfloat16)

    mark(8 + pos)
    pl.semaphore_wait(barrier, 1 + heads + has1.astype(jnp.int32) + feeds.astype(jnp.int32))
    begin(LOW)

    scale = math.log2(math.e) / hdim**0.5

    def spread(x, width):
        return jnp.concatenate([x] * (width // 128), axis=1)

    def raw(at, slot, width):
        return lax.dot_general(
            qaug[at, :], jnp.concatenate([kbuf[slot, 0:width, :], kdoc[slot, 0:width, :]], axis=1),
            (((1,), (1,)), ((), ())), preferred_element_type=jnp.float32)

    def mixed(weight, slot, width):
        ones = jnp.ones((width, 128), jnp.bfloat16)
        return jnp.dot(weight, jnp.concatenate([vbuf[slot, 0:width, :], ones], axis=1),
                       preferred_element_type=jnp.float32)

    def raw_pair(at, a, b, where):
        keys = [jnp.concatenate([kbuf[x, where, :], kdoc[x, where, :]], axis=1) for x in (a, b)]
        return lax.dot_general(
            qaug[at, :], jnp.concatenate(keys, axis=0), (((1,), (1,)), ((), ())), preferred_element_type=jnp.float32)

    def mixed_pair(weight, a, b, where):
        ones = jnp.ones((rows, 128), jnp.bfloat16)
        vals = jnp.concatenate([vbuf[a, where, :], vbuf[b, where, :]], axis=0)
        return jnp.dot(weight, jnp.concatenate([vals, ones], axis=1), preferred_element_type=jnp.float32)

    def flow(count, one, two, three):
        scores, weights = {}, {}
        for u in range(count + 2):
            if u >= 2:
                three(u - 2, *weights.pop(u - 2))
            if 1 <= u <= count:
                weights[u - 1] = two(u - 1, scores.pop(u - 1))
            if u < count:
                scores[u] = one(u)

    def diagonal():
        def width(t):
            return -(-(t + 1) * tokens // 128) * 128

        def at(t):
            return pl.ds(t * tile, tile)

        def one(t):
            return raw(at(t), 8 + pos, width(t))

        def two(t, s):
            wide, done = width(t), []
            for r in range(0, tile, BAND):
                here = slice(r, r + BAND)
                x = s[here, :] * scale
                edge = by_token(128, 2)[here] - by_token(128, 0)[here] <= t * tokens - (wide - 128)
                last = jnp.where(edge, x[:, wide - 128:], -BIG)
                x = last if wide == 128 else jnp.concatenate([x[:, :wide - 128], last], axis=1)
                m = jnp.broadcast_to(jnp.max(x, axis=1, keepdims=True), (BAND, 128))
                top[pl.ds(t * tile + r, BAND), :] = m
                done.append(jnp.exp2(x - spread(m, wide)).astype(jnp.bfloat16))
            return (jnp.concatenate(done, axis=0),)

        def three(t, weight):
            acc[at(t), :] = mixed(weight, 8 + pos, width(t))

        flow(total_rows // tile, one, two, three)

    def work(first, a, b, pieces):
        def at(r, size):
            return pl.ds(pl.multiple_of(first + r, BAND), size)

        def one(u):
            r, where = pieces[u]
            return raw_pair(at(r, tile), a, b, where)

        def two(u, s):
            done, factors = [], []
            for r in range(0, tile, BAND):
                x = s[r:r + BAND, :] * scale
                here = at(pieces[u][0] + r, BAND)
                m0 = top[here, :]
                m = jnp.maximum(m0, jnp.max(x, axis=1, keepdims=True))
                top[here, :] = m
                factors.append(jnp.exp2(m0 - m))
                done.append(jnp.exp2(x - spread(m, rows)).astype(jnp.bfloat16))
            return jnp.concatenate(done, axis=0), jnp.concatenate(factors, axis=0)

        def three(u, weight, factor):
            r, where = pieces[u]
            here = at(r, tile)
            acc[here, :] = acc[here, :] * spread(factor, 2 * hdim) + mixed_pair(weight, a, b, where)

        flow(len(pieces), one, two, three)

    def unit(first, a, b, extent):
        work(first, a, b, [(r, parts[w][2]) for r in range(0, extent, tile) for w in (0, 2)])

    def sweep(first, a, b, h):
        where = pl.ds(pl.multiple_of(h * half_keys, half_keys), half_keys)
        work(first, a, b, [(r, where) for r in range(0, swath, tile)])

    def pick(if_right, if_left):
        return col * if_right + (1 - col) * if_left

    def sel(if_one, if_zero):
        return core * if_one + (1 - core) * if_zero

    core0, core1 = core == 0, core == 1
    pairs = (
        (pick(8 + pos_x, 4 + pos), sel(8 + pos_m, pick(8 + pos_d, 4 + pos_m)), right | has1 | core1),
        (pick(4 + pos, 4 + pos_x), pick(4 + pos_m, sel(4 + pos_m, pos)), has1),
        (pick(4 + pos_x, 4 + pos_d), pick(4 + pos_d, sel(pos, pos_m)), has1),
        (pick(pos, pos_x), pick(sel(8 + pos_d, pos_m), pos_d), has2 | (right & core1)),
    )

    def local(t):
        return pl.ds(pl.multiple_of(t * tokens, tokens), tokens)

    def finish(first, t, put):
        whole = acc[pl.ds(pl.multiple_of(first + t * tile, tile), tile), :]
        norm[...] = whole[:, 0:hdim] / whole[:, hdim:]
        for g in range(group):
            put(g, norm[pl.ds(g, tokens, stride=group), :].astype(jnp.bfloat16))

    columns = pl.ds(pl.multiple_of(mine * (group * hdim), group * hdim), group * hdim)

    def outgoing(d, t):
        return pltpu.make_async_remote_copy(
            src_ref=stage.at[d - 1, local(t)],
            dst_ref=out_ref.at[local(t), columns],
            send_sem=osend_sem.at[d - 1, t],
            recv_sem=orecv_sem.at[d - 1, t],
            device_id={"head": (mine + d) % heads},
            device_id_type=MESH,
        )

    for load in loads:
        load.wait()
    diagonal()
    begin(HIGH)

    def first_in(which):
        landed(4 + pos, has1, "Z1", "X1", "D1", which=which)
        landed(8 + pos_x, right, "D0x", which=which)

    def first_over(which):
        landed(4 + pos_m, has1 & leftc & core0, which=which)
        landed(8 + pos_d, right & core0, which=which)
        landed(8 + pos_m, core1, which=which)

    @pl.loop(1, 12)
    def _(s):
        mark((8 + pos + s) % 12)

    @pl.loop(0, 4 * (me < 8).astype(jnp.int32) + 4 * (me < 4).astype(jnp.int32))
    def _(s):
        kbuf[s] = jnp.zeros((rows, hdim), jnp.bfloat16)
        vbuf[s] = jnp.zeros((rows, hdim), jnp.bfloat16)

    first_in(LOW)
    first_over(LOW)

    @pl.loop(0, 4)
    def _(i):
        @pl.when(i == 2)
        def _():
            first_in(HIGH)
            first_over(HIGH)

        @pl.when(i == 3)
        def _():
            landed(pos, has2 & core0, "X2", "D2", which=LOW)
            landed(4 + pos_x, has1 & core0, "D1x", which=LOW)

        @pl.when(pairs[0][2])
        def _():
            sweep(i % 2 * swath, pairs[0][0], pairs[0][1], i // 2)

    def event1():
        landed(pos, has2 & core1, "X2", "D2", which=LOW)
        landed(4 + pos_x, has1 & core1, "D1x", which=LOW)
        landed(4 + pos_x, has1, "D1x", which=HIGH)
        landed(pos, has2 & core0, "X2", "D2", which=HIGH)
        landed(4 + pos_m, has1 & (right | core1))

    def event2():
        landed(pos, has2 & core1, "X2", "D2", which=HIGH)
        landed(8 + pos_m, core0)
        landed(8 + pos_d, right & core1)
        landed(4 + pos_d, has1)
        landed(pos_m, has2)
        landed(pos_x, has2 & leftc & core0, "D2x", which=LOW)

    def event3():
        landed(pos_x, has2 & leftc & core1, "D2x", which=LOW)
        landed(pos_x, has2 & leftc, "D2x", which=HIGH)
        landed(pos_d, has2 & leftc)

    others = list(range(1, heads))
    order = [(p, d) for p in ORDER for d in (others if p < 4 else [heads])]
    order = [(p % 4, d) for p, d in order]
    kinds = [p if d < heads else p + 4 for p, d in order]
    events = ((1, event1), (2, event2), (3, event3))

    def choose(index, values):
        return sum((index == i) * jnp.asarray(x, jnp.int32) for i, x in enumerate(values))

    @pl.loop(0, len(order))
    def _(u):
        for kind, event in events:
            pl.when(u == kinds.index(kind))(event)
        p = choose(u, [x for x, _ in order])
        d = choose(u, [x for _, x in order])
        first = (mine + d) % heads * span

        valid = choose(p, [x[2] for x in pairs]) == 1
        slots = choose(p, [x[0] for x in pairs]), choose(p, [x[1] for x in pairs])
        closing = (p == 3) & (d < heads)

        @pl.when(valid & jnp.logical_not(closing))
        def _():
            unit(first, *slots, span)

        @pl.when(closing)
        def _():
            @pl.loop(0, steps)
            def _(t):
                @pl.when(valid)
                def _():
                    unit(first + t * tile, *slots, tile)

                def put(g, piece):
                    stage[d - 1, local(t), g * hdim:(g + 1) * hdim] = piece

                finish(first, t, put)
                outgoing(d, t).start()

        @pl.when((p == 3) & (d == heads))
        def _():
            @pl.loop(0, steps)
            def _(t):
                def put(g, piece):
                    where = pl.ds(pl.multiple_of(mine * (group * hdim) + g * hdim, hdim), hdim)
                    out_ref[local(t), where] = piece

                finish(first, t, put)

    for d in range(1, heads):
        @pl.loop(0, steps)
        def _(t):
            outgoing(d, t).wait_send()
            source = (mine + heads - d) % heads
            cols = pl.ds(pl.multiple_of(source * (group * hdim), group * hdim), group * hdim)
            got = out_ref.at[local(t), cols]
            pltpu.make_async_copy(got, got, orecv_sem.at[d - 1, t]).wait()

    for name in moves:
        sent(name)


def on_device(mesh, queries, keys, values, doc_lengths):
    rows, group, hdim = queries.shape
    heads = mesh.shape["head"]
    n = mesh.shape["ctx"]
    bf16, f32 = jnp.bfloat16, jnp.float32
    part = rows // heads
    tile = min(MOST, part * group)
    steps = part * group // tile
    vmem = pl.BlockSpec(memory_space=pltpu.VMEM)
    anywhere = pl.BlockSpec(memory_space=pl.ANY)
    return pl.pallas_call(
        functools.partial(kernel, n, heads, tile),
        out_shape=pltpu.VMEM((part, heads * group * hdim), bf16),
        in_specs=[anywhere] * 4,
        out_specs=vmem,
        scratch_shapes=[
            pltpu.VMEM((12, rows, hdim), bf16),
            pltpu.VMEM((12, rows, hdim), bf16),
            pltpu.VMEM((12, rows, 128), bf16),
            pltpu.VMEM((rows * group, hdim + 128), bf16),
            pltpu.VMEM((rows * group, hdim + 128), f32),
            pltpu.VMEM((rows * group, 128), f32),
            pltpu.VMEM((tile, hdim), f32),
            pltpu.VMEM((heads - 1, part, group * hdim), bf16),
            pltpu.SMEM(doc_lengths.shape, jnp.int32),
            pltpu.SemaphoreType.DMA((11, 4)),
            pltpu.SemaphoreType.DMA((12, 4)),
            pltpu.SemaphoreType.DMA((heads - 1, steps)),
            pltpu.SemaphoreType.DMA((heads - 1, steps)),
            pltpu.SemaphoreType.DMA((4,)),
        ],
        compiler_params=pltpu.CompilerParams(
            collective_id=0, has_side_effects=True, vmem_limit_bytes=56 * 1024 * 1024),
    )(doc_lengths, queries.reshape(rows * group, hdim), keys.reshape(rows, hdim), values.reshape(rows, hdim))


def solution(mesh):
    placed = (P("ctx", "head", None), P("ctx", "head", None), P("ctx", "head", None), P())
    return jax.shard_map(
        functools.partial(on_device, mesh), mesh=mesh, in_specs=placed,
        out_specs=P(("ctx", "head"), None), check_vma=False
    )
```

```python
import functools
import math

import jax
import jax.numpy as jnp
from jax import lax
from jax.experimental import pallas as pl
from jax.experimental.pallas import tpu as pltpu
from jax.sharding import PartitionSpec as P

MESH = pl.DeviceIdType.MESH
BIG = 1e30
MOST = 512
BAND = 128
ORDER = (1, 2, 3, 5, 6, 7)
LOW, HIGH = (0, 1), (2, 3)
ALL = LOW + HIGH


def kernel(n, heads, tile, lens_in, q_ref, k_ref, v_ref, out_ref,
           kbuf, vbuf, kdoc, qaug, acc, top, norm, stage,
           lens_ref, send_sem, recv_sem, osend_sem, orecv_sem, load_sem):
    rows, hdim = k_ref.shape
    total_rows = q_ref.shape[0]
    group = total_rows // rows
    me = lax.axis_index("ctx")
    mine = lax.axis_index("head")
    pos = me % 4
    core = pos % 2
    col = pos // 2
    mate = me + 1 - 2 * core
    across = me + 2 - 4 * col
    pos_m = pos + 1 - 2 * core
    pos_x = pos + 2 - 4 * col
    pos_d = pos_x + pos_m - pos
    has1 = me >= 4
    has2 = me >= 8
    feeds = me + 4 < n
    right = col == 1
    leftc = col == 0

    lens_load = pltpu.make_async_copy(lens_in, lens_ref, load_sem.at[3])
    lens_load.start()
    loads = (
        pltpu.make_async_copy(k_ref, kbuf.at[8 + pos], load_sem.at[0]),
        pltpu.make_async_copy(q_ref, qaug.at[:, 0:hdim], load_sem.at[1]),
        pltpu.make_async_copy(v_ref, vbuf.at[8 + pos], load_sem.at[2]),
    )
    for load in loads:
        load.start()

    barrier = pltpu.get_barrier_semaphore()
    for peer in (mate, across):
        pl.semaphore_signal(barrier, inc=1, device_id={"ctx": peer}, device_id_type=MESH)

    @pl.when(has1)
    def _():
        pl.semaphore_signal(barrier, inc=1, device_id={"ctx": me - 4}, device_id_type=MESH)

    @pl.when(feeds)
    def _():
        pl.semaphore_signal(barrier, inc=1, device_id={"ctx": me + 4}, device_id_type=MESH)

    for d in range(1, heads):
        pl.semaphore_signal(barrier, inc=1, device_id={"head": (mine + d) % heads}, device_id_type=MESH)

    half_keys = rows // 2
    parts = [(own, buf, pl.ds(h * half_keys, half_keys)) for h in range(2) for own, buf in ((k_ref, kbuf), (v_ref, vbuf))]

    def copies(lane, slot, to_slot, target):
        return [pltpu.make_async_remote_copy(
            src_ref=own.at[where] if slot is None else buf.at[slot, where],
            dst_ref=buf.at[to_slot, where],
            send_sem=send_sem.at[lane, w],
            recv_sem=recv_sem.at[to_slot, w],
            device_id={"ctx": target},
            device_id_type=MESH,
        ) for w, (own, buf, where) in enumerate(parts)]

    moves = {
        "D0": (copies(0, None, 8 + pos, mate), None),
        "X0": (copies(1, None, 8 + pos, across), leftc),
        "Z0": (copies(2, None, 4 + pos, me + 4), feeds),
        "D0x": (copies(3, 8 + pos_x, 8 + pos_x, mate), right),
        "D1": (copies(4, 4 + pos, 4 + pos, mate), has1),
        "X1": (copies(5, 4 + pos, 4 + pos, across), has1),
        "Z1": (copies(6, 4 + pos, pos, me + 4), has1 & feeds),
        "D1x": (copies(7, 4 + pos_x, 4 + pos_x, mate), has1),
        "D2": (copies(8, pos, pos, mate), has2),
        "X2": (copies(9, pos, pos, across), has2 & right),
        "D2x": (copies(10, pos_x, pos_x, mate), has2 & leftc),
    }

    def when(cond, fn):
        if cond is None:
            fn()
        else:
            pl.when(cond)(fn)

    def sent(name):
        made, cond = moves[name]

        def go():
            for copy in made:
                copy.wait_send()

        when(cond, go)

    def landed(slot, cond, *names, which=ALL):
        for w in which:
            _, buf, where = parts[w]

            def go():
                spot = buf.at[slot, where]
                pltpu.make_async_copy(spot, spot, recv_sem.at[slot, w]).wait()

            when(cond, go)
            for name in names:
                made, also = moves[name]
                when(cond if also is None else cond & also, made[w].start)

    def begin(which):
        for w in which:
            for name in ("Z0", "X0", "D0"):
                made, also = moves[name]
                when(also, made[w].start)

    lens_load.wait()

    lane = lax.broadcasted_iota(jnp.int32, (8, 128), 1)
    firsts = jnp.full((8, 128), 2**30, jnp.int32)
    ends = jnp.full((8, 128), 2**30, jnp.int32)
    run = jnp.int32(0)
    for d in range(lens_ref.shape[0]):
        firsts = jnp.where(lane == d, run, firsts)
        run = run + lens_ref[d]
        ends = jnp.where(lane == d, run, ends)
    first_row, end_row = firsts[0:1], ends[0:1]

    def member(position):
        return (position >= first_row) & (position < end_row)

    base = me * rows
    part = rows // heads
    tokens = tile // group
    steps = part // tokens
    span = part * group

    def by_token(width, dim):
        return lax.broadcasted_iota(jnp.int32, (tokens, group, width), dim).reshape(tile, width)

    @pl.loop(0, total_rows // tile)
    def _(t):
        at = pl.ds(pl.multiple_of(t * tile, tile), tile)
        qaug[at, hdim:] = jnp.where(member(base + t * tokens + by_token(128, 0)), 1.0, 0.0).astype(jnp.bfloat16)

    def mark(s):
        kpos = (me - pos - 8 + s) * rows + lax.broadcasted_iota(jnp.int32, (rows, 128), 0)
        kdoc[s] = jnp.where(member(kpos), 0.0, -BIG).astype(jnp.bfloat16)

    mark(8 + pos)
    pl.semaphore_wait(barrier, 1 + heads + has1.astype(jnp.int32) + feeds.astype(jnp.int32))
    begin(LOW)

    scale = math.log2(math.e) / hdim**0.5

    def spread(x, width):
        return jnp.concatenate([x] * (width // 128), axis=1)

    def raw(at, slot, width):
        return lax.dot_general(
            qaug[at, :], jnp.concatenate([kbuf[slot, 0:width, :], kdoc[slot, 0:width, :]], axis=1),
            (((1,), (1,)), ((), ())), preferred_element_type=jnp.float32)

    def mixed(weight, slot, width):
        ones = jnp.ones((width, 128), jnp.bfloat16)
        return jnp.dot(weight, jnp.concatenate([vbuf[slot, 0:width, :], ones], axis=1),
                       preferred_element_type=jnp.float32)

    def raw_pair(at, a, b, where):
        keys = [jnp.concatenate([kbuf[x, where, :], kdoc[x, where, :]], axis=1) for x in (a, b)]
        return lax.dot_general(
            qaug[at, :], jnp.concatenate(keys, axis=0), (((1,), (1,)), ((), ())), preferred_element_type=jnp.float32)

    def mixed_pair(weight, a, b, where):
        ones = jnp.ones((rows, 128), jnp.bfloat16)
        vals = jnp.concatenate([vbuf[a, where, :], vbuf[b, where, :]], axis=0)
        return jnp.dot(weight, jnp.concatenate([vals, ones], axis=1), preferred_element_type=jnp.float32)

    def flow(count, one, two, three):
        scores, weights = {}, {}
        for u in range(count + 2):
            if u >= 2:
                three(u - 2, *weights.pop(u - 2))
            if 1 <= u <= count:
                weights[u - 1] = two(u - 1, scores.pop(u - 1))
            if u < count:
                scores[u] = one(u)

    def diagonal():
        def width(t):
            return -(-(t + 1) * tokens // 128) * 128

        def at(t):
            return pl.ds(t * tile, tile)

        def one(t):
            return raw(at(t), 8 + pos, width(t))

        def two(t, s):
            wide, done = width(t), []
            for r in range(0, tile, BAND):
                here = slice(r, r + BAND)
                x = s[here, :] * scale
                edge = by_token(128, 2)[here] - by_token(128, 0)[here] <= t * tokens - (wide - 128)
                last = jnp.where(edge, x[:, wide - 128:], -BIG)
                x = last if wide == 128 else jnp.concatenate([x[:, :wide - 128], last], axis=1)
                m = jnp.broadcast_to(jnp.max(x, axis=1, keepdims=True), (BAND, 128))
                top[pl.ds(t * tile + r, BAND), :] = m
                done.append(jnp.exp2(x - spread(m, wide)).astype(jnp.bfloat16))
            return (jnp.concatenate(done, axis=0),)

        def three(t, weight):
            acc[at(t), :] = mixed(weight, 8 + pos, width(t))

        flow(total_rows // tile, one, two, three)

    def work(first, a, b, pieces):
        def at(r, size):
            return pl.ds(pl.multiple_of(first + r, BAND), size)

        def one(u):
            r, where = pieces[u]
            return raw_pair(at(r, tile), a, b, where)

        def two(u, s):
            done, factors = [], []
            for r in range(0, tile, BAND):
                x = s[r:r + BAND, :] * scale
                here = at(pieces[u][0] + r, BAND)
                m0 = top[here, :]
                m = jnp.maximum(m0, jnp.max(x, axis=1, keepdims=True))
                top[here, :] = m
                factors.append(jnp.exp2(m0 - m))
                done.append(jnp.exp2(x - spread(m, rows)).astype(jnp.bfloat16))
            return jnp.concatenate(done, axis=0), jnp.concatenate(factors, axis=0)

        def three(u, weight, factor):
            r, where = pieces[u]
            here = at(r, tile)
            acc[here, :] = acc[here, :] * spread(factor, 2 * hdim) + mixed_pair(weight, a, b, where)

        flow(len(pieces), one, two, three)

    def unit(first, a, b, extent):
        work(first, a, b, [(r, parts[w][2]) for r in range(0, extent, tile) for w in (0, 2)])

    def sweep(a, b, h):
        where = pl.ds(pl.multiple_of(h * half_keys, half_keys), half_keys)
        work(0, a, b, [(r, where) for r in range(0, total_rows, tile)])

    def pick(if_right, if_left):
        return col * if_right + (1 - col) * if_left

    def sel(if_one, if_zero):
        return core * if_one + (1 - core) * if_zero

    core0, core1 = core == 0, core == 1
    pairs = (
        (pick(8 + pos_x, 4 + pos), sel(8 + pos_m, pick(8 + pos_d, 4 + pos_m)), right | has1 | core1),
        (pick(4 + pos, 4 + pos_x), pick(4 + pos_m, sel(4 + pos_m, 4 + pos_d)), has1),
        (pick(4 + pos_x, sel(4 + pos_d, pos)), pick(4 + pos_d, sel(pos, pos_m)), has2 | (has1 & (right | core1))),
        (pick(pos, pos_x), pick(sel(8 + pos_d, pos_m), pos_d), has2 | (right & core1)),
    )

    def local(t):
        return pl.ds(pl.multiple_of(t * tokens, tokens), tokens)

    def finish(first, t, put):
        whole = acc[pl.ds(pl.multiple_of(first + t * tile, tile), tile), :]
        norm[...] = whole[:, 0:hdim] / whole[:, hdim:]
        for g in range(group):
            put(g, norm[pl.ds(g, tokens, stride=group), :].astype(jnp.bfloat16))

    columns = pl.ds(pl.multiple_of(mine * (group * hdim), group * hdim), group * hdim)

    def outgoing(d, t):
        return pltpu.make_async_remote_copy(
            src_ref=stage.at[d - 1, local(t)],
            dst_ref=out_ref.at[local(t), columns],
            send_sem=osend_sem.at[d - 1, t],
            recv_sem=orecv_sem.at[d - 1, t],
            device_id={"head": (mine + d) % heads},
            device_id_type=MESH,
        )

    for load in loads:
        load.wait()
    diagonal()
    begin(HIGH)

    def first_in(which):
        landed(4 + pos, has1, "Z1", "X1", "D1", which=which)
        landed(8 + pos_x, right, "D0x", which=which)

    def first_over(which):
        landed(4 + pos_m, has1 & leftc & core0, which=which)
        landed(8 + pos_d, right & core0, which=which)
        landed(8 + pos_m, core1, which=which)

    @pl.loop(1, 12)
    def _(s):
        mark((8 + pos + s) % 12)

    @pl.loop(0, 4 * (me < 8).astype(jnp.int32) + 4 * (me < 4).astype(jnp.int32))
    def _(s):
        kbuf[s] = jnp.zeros((rows, hdim), jnp.bfloat16)
        vbuf[s] = jnp.zeros((rows, hdim), jnp.bfloat16)

    first_in(LOW)
    first_over(LOW)

    @pl.loop(0, 2)
    def _(h):
        @pl.when(h == 1)
        def _():
            first_in(HIGH)
            first_over(HIGH)

        @pl.when(pairs[0][2])
        def _():
            sweep(pairs[0][0], pairs[0][1], h)

    def event1():
        landed(4 + pos_x, has1 & leftc, "D1x")
        landed(4 + pos_x, has1 & right, "D1x", which=LOW)
        landed(pos, has2 & right, "X2", "D2", which=LOW)
        landed(pos, has2 & right & core0, "X2", "D2", which=HIGH)
        landed(4 + pos_m, has1 & (right | core1))
        landed(4 + pos_d, has1 & leftc & core0)

    def event2():
        landed(pos, has2 & leftc, "D2")
        landed(pos, has2 & right & core1, "X2", "D2", which=HIGH)
        landed(4 + pos_x, has1 & right, "D1x", which=HIGH)
        landed(8 + pos_m, core0)
        landed(8 + pos_d, right & core1)
        landed(4 + pos_d, has1 & (right | core1))
        landed(pos_m, has2)

    def event3():
        landed(pos_x, has2 & leftc, "D2x")
        landed(pos_d, has2 & leftc)

    others = list(range(1, heads))
    order = [(p, d) for p in ORDER for d in (others if p < 4 else [heads])]
    order = [(p % 4, d) for p, d in order]
    kinds = [p if d < heads else p + 4 for p, d in order]
    events = ((1, event1), (2, event2), (3, event3))

    def choose(index, values):
        return sum((index == i) * jnp.asarray(x, jnp.int32) for i, x in enumerate(values))

    @pl.loop(0, len(order))
    def _(u):
        for kind, event in events:
            pl.when(u == kinds.index(kind))(event)
        p = choose(u, [x for x, _ in order])
        d = choose(u, [x for _, x in order])
        first = (mine + d) % heads * span

        valid = choose(p, [x[2] for x in pairs]) == 1
        slots = choose(p, [x[0] for x in pairs]), choose(p, [x[1] for x in pairs])
        closing = (p == 3) & (d < heads)

        @pl.when(valid & jnp.logical_not(closing))
        def _():
            unit(first, *slots, span)

        @pl.when(closing)
        def _():
            @pl.loop(0, steps)
            def _(t):
                @pl.when(valid)
                def _():
                    unit(first + t * tile, *slots, tile)

                def put(g, piece):
                    stage[d - 1, local(t), g * hdim:(g + 1) * hdim] = piece

                finish(first, t, put)
                outgoing(d, t).start()

        @pl.when((p == 3) & (d == heads))
        def _():
            @pl.loop(0, steps)
            def _(t):
                def put(g, piece):
                    where = pl.ds(pl.multiple_of(mine * (group * hdim) + g * hdim, hdim), hdim)
                    out_ref[local(t), where] = piece

                finish(first, t, put)

    for d in range(1, heads):
        @pl.loop(0, steps)
        def _(t):
            outgoing(d, t).wait_send()
            source = (mine + heads - d) % heads
            cols = pl.ds(pl.multiple_of(source * (group * hdim), group * hdim), group * hdim)
            got = out_ref.at[local(t), cols]
            pltpu.make_async_copy(got, got, orecv_sem.at[d - 1, t]).wait()

    for name in moves:
        sent(name)


def on_device(mesh, queries, keys, values, doc_lengths):
    rows, group, hdim = queries.shape
    heads = mesh.shape["head"]
    n = mesh.shape["ctx"]
    bf16, f32 = jnp.bfloat16, jnp.float32
    part = rows // heads
    tile = min(MOST, part * group)
    steps = part * group // tile
    vmem = pl.BlockSpec(memory_space=pltpu.VMEM)
    anywhere = pl.BlockSpec(memory_space=pl.ANY)
    return pl.pallas_call(
        functools.partial(kernel, n, heads, tile),
        out_shape=pltpu.VMEM((part, heads * group * hdim), bf16),
        in_specs=[anywhere] * 4,
        out_specs=vmem,
        scratch_shapes=[
            pltpu.VMEM((12, rows, hdim), bf16),
            pltpu.VMEM((12, rows, hdim), bf16),
            pltpu.VMEM((12, rows, 128), bf16),
            pltpu.VMEM((rows * group, hdim + 128), bf16),
            pltpu.VMEM((rows * group, hdim + 128), f32),
            pltpu.VMEM((rows * group, 128), f32),
            pltpu.VMEM((tile, hdim), f32),
            pltpu.VMEM((heads - 1, part, group * hdim), bf16),
            pltpu.SMEM(doc_lengths.shape, jnp.int32),
            pltpu.SemaphoreType.DMA((11, 4)),
            pltpu.SemaphoreType.DMA((12, 4)),
            pltpu.SemaphoreType.DMA((heads - 1, steps)),
            pltpu.SemaphoreType.DMA((heads - 1, steps)),
            pltpu.SemaphoreType.DMA((4,)),
        ],
        compiler_params=pltpu.CompilerParams(
            collective_id=0, has_side_effects=True, vmem_limit_bytes=56 * 1024 * 1024),
    )(doc_lengths, queries.reshape(rows * group, hdim), keys.reshape(rows, hdim), values.reshape(rows, hdim))


def solution(mesh):
    placed = (P("ctx", "head", None), P("ctx", "head", None), P("ctx", "head", None), P())
    return jax.shard_map(
        functools.partial(on_device, mesh), mesh=mesh, in_specs=placed,
        out_specs=P(("ctx", "head"), None), check_vma=False
    )
```

```python
import functools
import math

import jax
import jax.numpy as jnp
from jax import lax
from jax.experimental import pallas as pl
from jax.experimental.pallas import tpu as pltpu
from jax.sharding import PartitionSpec as P

MESH = pl.DeviceIdType.MESH
BIG = 1e30
MOST = 512
BAND = 128
ORDER = (1, 2, 3, 5, 6, 7)
LOW, HIGH = (0, 1), (2, 3)
ALL = LOW + HIGH


def kernel(n, heads, tile, lens_in, q_ref, k_ref, v_ref, out_ref,
           kbuf, vbuf, kdoc, qaug, acc, top, norm, stage,
           lens_ref, send_sem, recv_sem, osend_sem, orecv_sem, load_sem):
    rows, hdim = k_ref.shape
    total_rows = q_ref.shape[0]
    group = total_rows // rows
    me = lax.axis_index("ctx")
    mine = lax.axis_index("head")
    pos = me % 4
    core = pos % 2
    col = pos // 2
    mate = me + 1 - 2 * core
    across = me + 2 - 4 * col
    pos_m = pos + 1 - 2 * core
    pos_x = pos + 2 - 4 * col
    pos_d = pos_x + pos_m - pos
    has1 = me >= 4
    has2 = me >= 8
    feeds = me + 4 < n
    right = col == 1
    leftc = col == 0

    lens_load = pltpu.make_async_copy(lens_in, lens_ref, load_sem.at[3])
    lens_load.start()
    loads = (
        pltpu.make_async_copy(k_ref, kbuf.at[8 + pos], load_sem.at[0]),
        pltpu.make_async_copy(q_ref, qaug.at[:, 0:hdim], load_sem.at[1]),
        pltpu.make_async_copy(v_ref, vbuf.at[8 + pos], load_sem.at[2]),
    )
    for load in loads:
        load.start()

    barrier = pltpu.get_barrier_semaphore()
    for peer in (mate, across):
        pl.semaphore_signal(barrier, inc=1, device_id={"ctx": peer}, device_id_type=MESH)

    @pl.when(has1)
    def _():
        pl.semaphore_signal(barrier, inc=1, device_id={"ctx": me - 4}, device_id_type=MESH)

    @pl.when(feeds)
    def _():
        pl.semaphore_signal(barrier, inc=1, device_id={"ctx": me + 4}, device_id_type=MESH)

    for d in range(1, heads):
        pl.semaphore_signal(barrier, inc=1, device_id={"head": (mine + d) % heads}, device_id_type=MESH)

    half_keys = rows // 2
    parts = [(own, buf, pl.ds(h * half_keys, half_keys)) for h in range(2) for own, buf in ((k_ref, kbuf), (v_ref, vbuf))]

    def copies(lane, slot, to_slot, target):
        return [pltpu.make_async_remote_copy(
            src_ref=own.at[where] if slot is None else buf.at[slot, where],
            dst_ref=buf.at[to_slot, where],
            send_sem=send_sem.at[lane, w],
            recv_sem=recv_sem.at[to_slot, w],
            device_id={"ctx": target},
            device_id_type=MESH,
        ) for w, (own, buf, where) in enumerate(parts)]

    moves = {
        "D0": (copies(0, None, 8 + pos, mate), None),
        "X0": (copies(1, None, 8 + pos, across), leftc),
        "Z0": (copies(2, None, 4 + pos, me + 4), feeds),
        "D0x": (copies(3, 8 + pos_x, 8 + pos_x, mate), right),
        "D1": (copies(4, 4 + pos, 4 + pos, mate), has1),
        "X1": (copies(5, 4 + pos, 4 + pos, across), has1),
        "Z1": (copies(6, 4 + pos, pos, me + 4), has1 & feeds),
        "D1x": (copies(7, 4 + pos_x, 4 + pos_x, mate), has1),
        "D2": (copies(8, pos, pos, mate), has2),
        "X2": (copies(9, pos, pos, across), has2 & right),
        "D2x": (copies(10, pos_x, pos_x, mate), has2 & leftc),
    }

    def when(cond, fn):
        if cond is None:
            fn()
        else:
            pl.when(cond)(fn)

    def sent(name):
        made, cond = moves[name]

        def go():
            for copy in made:
                copy.wait_send()

        when(cond, go)

    def landed(slot, cond, *names, which=ALL):
        for w in which:
            _, buf, where = parts[w]

            def go():
                spot = buf.at[slot, where]
                pltpu.make_async_copy(spot, spot, recv_sem.at[slot, w]).wait()

            when(cond, go)
            for name in names:
                made, also = moves[name]
                when(cond if also is None else cond & also, made[w].start)

    def begin(which):
        for w in which:
            for name in ("Z0", "X0", "D0"):
                made, also = moves[name]
                when(also, made[w].start)

    lens_load.wait()

    lane = lax.broadcasted_iota(jnp.int32, (8, 128), 1)
    firsts = jnp.full((8, 128), 2**30, jnp.int32)
    ends = jnp.full((8, 128), 2**30, jnp.int32)
    run = jnp.int32(0)
    for d in range(lens_ref.shape[0]):
        firsts = jnp.where(lane == d, run, firsts)
        run = run + lens_ref[d]
        ends = jnp.where(lane == d, run, ends)
    first_row, end_row = firsts[0:1], ends[0:1]

    def member(position):
        return (position >= first_row) & (position < end_row)

    base = me * rows
    part = rows // heads
    tokens = tile // group
    steps = part // tokens
    span = part * group

    def by_token(width, dim):
        return lax.broadcasted_iota(jnp.int32, (tokens, group, width), dim).reshape(tile, width)

    @pl.loop(0, total_rows // tile)
    def _(t):
        at = pl.ds(pl.multiple_of(t * tile, tile), tile)
        qaug[at, hdim:] = jnp.where(member(base + t * tokens + by_token(128, 0)), 1.0, 0.0).astype(jnp.bfloat16)

    def mark(s):
        kpos = (me - pos - 8 + s) * rows + lax.broadcasted_iota(jnp.int32, (rows, 128), 0)
        kdoc[s] = jnp.where(member(kpos), 0.0, -BIG).astype(jnp.bfloat16)

    mark(8 + pos)
    pl.semaphore_wait(barrier, 1 + heads + has1.astype(jnp.int32) + feeds.astype(jnp.int32))
    begin(LOW)

    scale = math.log2(math.e) / hdim**0.5

    def spread(x, width):
        return jnp.concatenate([x] * (width // 128), axis=1)

    def raw(at, slot, width):
        return lax.dot_general(
            qaug[at, :], jnp.concatenate([kbuf[slot, 0:width, :], kdoc[slot, 0:width, :]], axis=1),
            (((1,), (1,)), ((), ())), preferred_element_type=jnp.float32)

    def mixed(weight, slot, width):
        ones = jnp.ones((width, 128), jnp.bfloat16)
        return jnp.dot(weight, jnp.concatenate([vbuf[slot, 0:width, :], ones], axis=1),
                       preferred_element_type=jnp.float32)

    def raw_pair(at, a, b, where):
        keys = [jnp.concatenate([kbuf[x, where, :], kdoc[x, where, :]], axis=1) for x in (a, b)]
        return lax.dot_general(
            qaug[at, :], jnp.concatenate(keys, axis=0), (((1,), (1,)), ((), ())), preferred_element_type=jnp.float32)

    def mixed_pair(weight, a, b, where):
        ones = jnp.ones((rows, 128), jnp.bfloat16)
        vals = jnp.concatenate([vbuf[a, where, :], vbuf[b, where, :]], axis=0)
        return jnp.dot(weight, jnp.concatenate([vals, ones], axis=1), preferred_element_type=jnp.float32)

    def flow(count, one, two, three):
        scores, weights = {}, {}
        for u in range(count + 2):
            if u >= 2:
                three(u - 2, *weights.pop(u - 2))
            if 1 <= u <= count:
                weights[u - 1] = two(u - 1, scores.pop(u - 1))
            if u < count:
                scores[u] = one(u)

    def diagonal():
        def width(t):
            return -(-(t + 1) * tokens // 128) * 128

        def at(t):
            return pl.ds(t * tile, tile)

        def one(t):
            return raw(at(t), 8 + pos, width(t))

        def two(t, s):
            wide, done = width(t), []
            for r in range(0, tile, BAND):
                here = slice(r, r + BAND)
                x = s[here, :] * scale
                edge = by_token(128, 2)[here] - by_token(128, 0)[here] <= t * tokens - (wide - 128)
                last = jnp.where(edge, x[:, wide - 128:], -BIG)
                x = last if wide == 128 else jnp.concatenate([x[:, :wide - 128], last], axis=1)
                m = jnp.broadcast_to(jnp.max(x, axis=1, keepdims=True), (BAND, 128))
                top[pl.ds(t * tile + r, BAND), :] = m
                done.append(jnp.exp2(x - spread(m, wide)).astype(jnp.bfloat16))
            return (jnp.concatenate(done, axis=0),)

        def three(t, weight):
            acc[at(t), :] = mixed(weight, 8 + pos, width(t))

        flow(total_rows // tile, one, two, three)

    def work(first, a, b, pieces):
        def at(r, size):
            return pl.ds(pl.multiple_of(first + r, BAND), size)

        def one(u):
            r, where = pieces[u]
            return raw_pair(at(r, tile), a, b, where)

        def two(u, s):
            done, factors = [], []
            for r in range(0, tile, BAND):
                x = s[r:r + BAND, :] * scale
                here = at(pieces[u][0] + r, BAND)
                m0 = top[here, :]
                m = jnp.maximum(m0, jnp.max(x, axis=1, keepdims=True))
                top[here, :] = m
                factors.append(jnp.exp2(m0 - m))
                done.append(jnp.exp2(x - spread(m, rows)).astype(jnp.bfloat16))
            return jnp.concatenate(done, axis=0), jnp.concatenate(factors, axis=0)

        def three(u, weight, factor):
            r, where = pieces[u]
            here = at(r, tile)
            acc[here, :] = acc[here, :] * spread(factor, 2 * hdim) + mixed_pair(weight, a, b, where)

        flow(len(pieces), one, two, three)

    def unit(first, a, b, extent):
        work(first, a, b, [(r, parts[w][2]) for r in range(0, extent, tile) for w in (0, 2)])

    def sweep(a, b, h):
        where = pl.ds(pl.multiple_of(h * half_keys, half_keys), half_keys)
        work(0, a, b, [(r, where) for r in range(0, total_rows, tile)])

    def pick(if_right, if_left):
        return col * if_right + (1 - col) * if_left

    def sel(if_one, if_zero):
        return core * if_one + (1 - core) * if_zero

    core0, core1 = core == 0, core == 1
    pairs = (
        (pick(8 + pos_x, 4 + pos), sel(8 + pos_m, pick(8 + pos_d, 4 + pos_m)), right | has1 | core1),
        (pick(4 + pos, 4 + pos_x), pick(4 + pos_m, sel(4 + pos_m, 4 + pos_d)), has1),
        (pick(4 + pos_x, sel(4 + pos_d, pos)), pick(4 + pos_d, sel(pos, pos_m)), has2 | (has1 & (right | core1))),
        (pick(pos, pos_x), pick(sel(8 + pos_d, pos_m), pos_d), has2 | (right & core1)),
    )

    def local(t):
        return pl.ds(pl.multiple_of(t * tokens, tokens), tokens)

    def finish(first, t, put):
        whole = acc[pl.ds(pl.multiple_of(first + t * tile, tile), tile), :]
        norm[...] = whole[:, 0:hdim] / whole[:, hdim:]
        for g in range(group):
            put(g, norm[pl.ds(g, tokens, stride=group), :].astype(jnp.bfloat16))

    columns = pl.ds(pl.multiple_of(mine * (group * hdim), group * hdim), group * hdim)

    def outgoing(d, t):
        return pltpu.make_async_remote_copy(
            src_ref=stage.at[d - 1, local(t)],
            dst_ref=out_ref.at[local(t), columns],
            send_sem=osend_sem.at[d - 1, t],
            recv_sem=orecv_sem.at[d - 1, t],
            device_id={"head": (mine + d) % heads},
            device_id_type=MESH,
        )

    for load in loads:
        load.wait()
    diagonal()
    begin(HIGH)

    def first_in(which):
        landed(4 + pos, has1, "Z1", "X1", "D1", which=which)
        landed(8 + pos_x, right, "D0x", which=which)

    def first_over(which):
        landed(4 + pos_m, has1 & leftc & core0, which=which)
        landed(8 + pos_d, right & core0, which=which)
        landed(8 + pos_m, core1, which=which)

    @pl.loop(1, 12)
    def _(s):
        mark((8 + pos + s) % 12)

    @pl.loop(0, 4 * (me < 8).astype(jnp.int32) + 4 * (me < 4).astype(jnp.int32))
    def _(s):
        kbuf[s] = jnp.zeros((rows, hdim), jnp.bfloat16)
        vbuf[s] = jnp.zeros((rows, hdim), jnp.bfloat16)

    first_in(LOW)
    first_over(LOW)

    @pl.loop(0, 2)
    def _(h):
        @pl.when(h == 1)
        def _():
            first_in(HIGH)
            first_over(HIGH)

        @pl.when(pairs[0][2])
        def _():
            sweep(pairs[0][0], pairs[0][1], h)

    def event1():
        landed(4 + pos_x, has1 & leftc, "D1x")
        landed(4 + pos_x, has1 & right, "D1x", which=LOW)
        landed(pos, has2 & right, "X2", "D2", which=LOW)
        landed(pos, has2 & right & core0, "X2", "D2", which=HIGH)
        landed(4 + pos_x, has1 & right & core0, "D1x", which=HIGH)
        landed(4 + pos_m, has1 & (right | core1))
        landed(4 + pos_d, has1 & leftc & core0)

    def event2():
        landed(pos, has2 & leftc, "D2")
        landed(pos, has2 & right & core1, "X2", "D2", which=HIGH)
        landed(4 + pos_x, has1 & right & core1, "D1x", which=HIGH)
        landed(4 + pos_d, has1 & (right | core1))
        landed(pos_m, has2 & leftc & core0)

    def event3():
        landed(pos_x, has2 & leftc, "D2x")
        landed(pos_d, has2 & leftc)
        landed(8 + pos_m, core0)
        landed(8 + pos_d, right & core1)
        landed(pos_m, has2 & (right | core1))

    others = list(range(1, heads))
    order = [(p, d) for p in ORDER for d in (others if p < 4 else [heads])]
    order = [(p % 4, d) for p, d in order]
    kinds = [p if d < heads else p + 4 for p, d in order]
    events = ((1, event1), (2, event2), (3, event3))

    def choose(index, values):
        return sum((index == i) * jnp.asarray(x, jnp.int32) for i, x in enumerate(values))

    @pl.loop(0, len(order))
    def _(u):
        for kind, event in events:
            pl.when(u == kinds.index(kind))(event)
        p = choose(u, [x for x, _ in order])
        d = choose(u, [x for _, x in order])
        first = (mine + d) % heads * span

        valid = choose(p, [x[2] for x in pairs]) == 1
        slots = choose(p, [x[0] for x in pairs]), choose(p, [x[1] for x in pairs])
        closing = (p == 3) & (d < heads)

        @pl.when(valid & jnp.logical_not(closing))
        def _():
            unit(first, *slots, span)

        @pl.when(closing)
        def _():
            @pl.loop(0, steps)
            def _(t):
                @pl.when(valid)
                def _():
                    unit(first + t * tile, *slots, tile)

                def put(g, piece):
                    stage[d - 1, local(t), g * hdim:(g + 1) * hdim] = piece

                finish(first, t, put)
                outgoing(d, t).start()

        @pl.when((p == 3) & (d == heads))
        def _():
            @pl.loop(0, steps)
            def _(t):
                def put(g, piece):
                    where = pl.ds(pl.multiple_of(mine * (group * hdim) + g * hdim, hdim), hdim)
                    out_ref[local(t), where] = piece

                finish(first, t, put)

    for d in range(1, heads):
        @pl.loop(0, steps)
        def _(t):
            outgoing(d, t).wait_send()
            source = (mine + heads - d) % heads
            cols = pl.ds(pl.multiple_of(source * (group * hdim), group * hdim), group * hdim)
            got = out_ref.at[local(t), cols]
            pltpu.make_async_copy(got, got, orecv_sem.at[d - 1, t]).wait()

    for name in moves:
        sent(name)


def on_device(mesh, queries, keys, values, doc_lengths):
    rows, group, hdim = queries.shape
    heads = mesh.shape["head"]
    n = mesh.shape["ctx"]
    bf16, f32 = jnp.bfloat16, jnp.float32
    part = rows // heads
    tile = min(MOST, part * group)
    steps = part * group // tile
    vmem = pl.BlockSpec(memory_space=pltpu.VMEM)
    anywhere = pl.BlockSpec(memory_space=pl.ANY)
    return pl.pallas_call(
        functools.partial(kernel, n, heads, tile),
        out_shape=pltpu.VMEM((part, heads * group * hdim), bf16),
        in_specs=[anywhere] * 4,
        out_specs=vmem,
        scratch_shapes=[
            pltpu.VMEM((12, rows, hdim), bf16),
            pltpu.VMEM((12, rows, hdim), bf16),
            pltpu.VMEM((12, rows, 128), bf16),
            pltpu.VMEM((rows * group, hdim + 128), bf16),
            pltpu.VMEM((rows * group, hdim + 128), f32),
            pltpu.VMEM((rows * group, 128), f32),
            pltpu.VMEM((tile, hdim), f32),
            pltpu.VMEM((heads - 1, part, group * hdim), bf16),
            pltpu.SMEM(doc_lengths.shape, jnp.int32),
            pltpu.SemaphoreType.DMA((11, 4)),
            pltpu.SemaphoreType.DMA((12, 4)),
            pltpu.SemaphoreType.DMA((heads - 1, steps)),
            pltpu.SemaphoreType.DMA((heads - 1, steps)),
            pltpu.SemaphoreType.DMA((4,)),
        ],
        compiler_params=pltpu.CompilerParams(
            collective_id=0, has_side_effects=True, vmem_limit_bytes=56 * 1024 * 1024),
    )(doc_lengths, queries.reshape(rows * group, hdim), keys.reshape(rows, hdim), values.reshape(rows, hdim))


def solution(mesh):
    placed = (P("ctx", "head", None), P("ctx", "head", None), P("ctx", "head", None), P())
    return jax.shard_map(
        functools.partial(on_device, mesh), mesh=mesh, in_specs=placed,
        out_specs=P(("ctx", "head"), None), check_vma=False
    )
```

```python
import functools
import math

import jax
import jax.numpy as jnp
from jax import lax
from jax.experimental import pallas as pl
from jax.experimental.pallas import tpu as pltpu
from jax.sharding import PartitionSpec as P

MESH = pl.DeviceIdType.MESH
BIG = 1e30
MOST = 512
BAND = 128
ORDER = (1, 2, 3, 5, 6, 7)
LOW, HIGH = (0, 1), (2, 3)
ALL = LOW + HIGH


def kernel(n, heads, tile, lens_in, q_ref, k_ref, v_ref, out_ref,
           kbuf, vbuf, kdoc, qaug, acc, top, norm, stage,
           lens_ref, send_sem, recv_sem, osend_sem, orecv_sem, load_sem):
    rows, hdim = k_ref.shape
    total_rows = q_ref.shape[0]
    group = total_rows // rows
    me = lax.axis_index("ctx")
    mine = lax.axis_index("head")
    pos = me % 4
    core = pos % 2
    col = pos // 2
    mate = me + 1 - 2 * core
    across = me + 2 - 4 * col
    pos_m = pos + 1 - 2 * core
    pos_x = pos + 2 - 4 * col
    pos_d = pos_x + pos_m - pos
    has1 = me >= 4
    has2 = me >= 8
    feeds = me + 4 < n
    right = col == 1
    leftc = col == 0

    lens_load = pltpu.make_async_copy(lens_in, lens_ref, load_sem.at[3])
    lens_load.start()
    loads = (
        pltpu.make_async_copy(k_ref, kbuf.at[8 + pos], load_sem.at[0]),
        pltpu.make_async_copy(q_ref, qaug.at[:, 0:hdim], load_sem.at[1]),
        pltpu.make_async_copy(v_ref, vbuf.at[8 + pos], load_sem.at[2]),
    )
    for load in loads:
        load.start()

    barrier = pltpu.get_barrier_semaphore()
    for peer in (mate, across):
        pl.semaphore_signal(barrier, inc=1, device_id={"ctx": peer}, device_id_type=MESH)

    @pl.when(has1)
    def _():
        pl.semaphore_signal(barrier, inc=1, device_id={"ctx": me - 4}, device_id_type=MESH)

    @pl.when(feeds)
    def _():
        pl.semaphore_signal(barrier, inc=1, device_id={"ctx": me + 4}, device_id_type=MESH)

    for d in range(1, heads):
        pl.semaphore_signal(barrier, inc=1, device_id={"head": (mine + d) % heads}, device_id_type=MESH)

    half_keys = rows // 2
    parts = [(own, buf, pl.ds(h * half_keys, half_keys)) for h in range(2) for own, buf in ((k_ref, kbuf), (v_ref, vbuf))]

    def copies(lane, slot, to_slot, target):
        return [pltpu.make_async_remote_copy(
            src_ref=own.at[where] if slot is None else buf.at[slot, where],
            dst_ref=buf.at[to_slot, where],
            send_sem=send_sem.at[lane, w],
            recv_sem=recv_sem.at[to_slot, w],
            device_id={"ctx": target},
            device_id_type=MESH,
        ) for w, (own, buf, where) in enumerate(parts)]

    moves = {
        "D0": (copies(0, None, 8 + pos, mate), None),
        "X0": (copies(1, None, 8 + pos, across), leftc),
        "Z0": (copies(2, None, 4 + pos, me + 4), feeds),
        "D0x": (copies(3, 8 + pos_x, 8 + pos_x, mate), right),
        "D1": (copies(4, 4 + pos, 4 + pos, mate), has1),
        "X1": (copies(5, 4 + pos, 4 + pos, across), has1),
        "Z1": (copies(6, 4 + pos, pos, me + 4), has1 & feeds),
        "D1x": (copies(7, 4 + pos_x, 4 + pos_x, mate), has1),
        "D2": (copies(8, pos, pos, mate), has2),
        "X2": (copies(9, pos, pos, across), has2 & right),
        "D2x": (copies(10, pos_x, pos_x, mate), has2 & leftc),
    }

    def when(cond, fn):
        if cond is None:
            fn()
        else:
            pl.when(cond)(fn)

    def sent(name):
        made, cond = moves[name]

        def go():
            for copy in made:
                copy.wait_send()

        when(cond, go)

    def landed(slot, cond, *names, which=ALL):
        for w in which:
            _, buf, where = parts[w]

            def go():
                spot = buf.at[slot, where]
                pltpu.make_async_copy(spot, spot, recv_sem.at[slot, w]).wait()

            when(cond, go)
            for name in names:
                made, also = moves[name]
                when(cond if also is None else cond & also, made[w].start)

    def begin(which):
        for w in which:
            for name in ("Z0", "X0", "D0"):
                made, also = moves[name]
                when(also, made[w].start)

    lens_load.wait()

    lane = lax.broadcasted_iota(jnp.int32, (8, 128), 1)
    firsts = jnp.full((8, 128), 2**30, jnp.int32)
    ends = jnp.full((8, 128), 2**30, jnp.int32)
    run = jnp.int32(0)
    for d in range(lens_ref.shape[0]):
        firsts = jnp.where(lane == d, run, firsts)
        run = run + lens_ref[d]
        ends = jnp.where(lane == d, run, ends)
    first_row, end_row = firsts[0:1], ends[0:1]

    def member(position):
        return (position >= first_row) & (position < end_row)

    base = me * rows
    part = rows // heads
    tokens = tile // group
    steps = part // tokens
    span = part * group

    def by_token(width, dim):
        return lax.broadcasted_iota(jnp.int32, (tokens, group, width), dim).reshape(tile, width)

    @pl.loop(0, total_rows // tile)
    def _(t):
        at = pl.ds(pl.multiple_of(t * tile, tile), tile)
        qaug[at, hdim:] = jnp.where(member(base + t * tokens + by_token(128, 0)), 1.0, 0.0).astype(jnp.bfloat16)

    def mark(s):
        kpos = (me - pos - 8 + s) * rows + lax.broadcasted_iota(jnp.int32, (rows, 128), 0)
        kdoc[s] = jnp.where(member(kpos), 0.0, -BIG).astype(jnp.bfloat16)

    mark(8 + pos)
    pl.semaphore_wait(barrier, 1 + heads + has1.astype(jnp.int32) + feeds.astype(jnp.int32))
    begin(LOW)

    scale = math.log2(math.e) / hdim**0.5

    def spread(x, width):
        return jnp.concatenate([x] * (width // 128), axis=1)

    def raw(at, slot, width):
        return lax.dot_general(
            qaug[at, :], jnp.concatenate([kbuf[slot, 0:width, :], kdoc[slot, 0:width, :]], axis=1),
            (((1,), (1,)), ((), ())), preferred_element_type=jnp.float32)

    def mixed(weight, slot, width):
        ones = jnp.ones((width, 128), jnp.bfloat16)
        return jnp.dot(weight, jnp.concatenate([vbuf[slot, 0:width, :], ones], axis=1),
                       preferred_element_type=jnp.float32)

    def raw_pair(at, a, b, where):
        keys = [jnp.concatenate([kbuf[x, where, :], kdoc[x, where, :]], axis=1) for x in (a, b)]
        return lax.dot_general(
            qaug[at, :], jnp.concatenate(keys, axis=0), (((1,), (1,)), ((), ())), preferred_element_type=jnp.float32)

    def mixed_pair(weight, a, b, where):
        ones = jnp.ones((rows, 128), jnp.bfloat16)
        vals = jnp.concatenate([vbuf[a, where, :], vbuf[b, where, :]], axis=0)
        return jnp.dot(weight, jnp.concatenate([vals, ones], axis=1), preferred_element_type=jnp.float32)

    def flow(count, one, two, three):
        scores, weights = {}, {}
        for u in range(count + 2):
            if u >= 2:
                three(u - 2, *weights.pop(u - 2))
            if 1 <= u <= count:
                weights[u - 1] = two(u - 1, scores.pop(u - 1))
            if u < count:
                scores[u] = one(u)

    def diagonal():
        def width(t):
            return -(-(t + 1) * tokens // 128) * 128

        def at(t):
            return pl.ds(t * tile, tile)

        def one(t):
            return raw(at(t), 8 + pos, width(t))

        def two(t, s):
            wide, done = width(t), []
            for r in range(0, tile, BAND):
                here = slice(r, r + BAND)
                x = s[here, :] * scale
                edge = by_token(128, 2)[here] - by_token(128, 0)[here] <= t * tokens - (wide - 128)
                last = jnp.where(edge, x[:, wide - 128:], -BIG)
                x = last if wide == 128 else jnp.concatenate([x[:, :wide - 128], last], axis=1)
                m = jnp.broadcast_to(jnp.max(x, axis=1, keepdims=True), (BAND, 128))
                top[pl.ds(t * tile + r, BAND), :] = m
                done.append(jnp.exp2(x - spread(m, wide)).astype(jnp.bfloat16))
            return (jnp.concatenate(done, axis=0),)

        def three(t, weight):
            acc[at(t), :] = mixed(weight, 8 + pos, width(t))

        flow(total_rows // tile, one, two, three)

    def work(first, a, b, pieces):
        def at(r, size):
            return pl.ds(pl.multiple_of(first + r, BAND), size)

        def one(u):
            r, where = pieces[u]
            return raw_pair(at(r, tile), a, b, where)

        def two(u, s):
            done, factors = [], []
            for r in range(0, tile, BAND):
                x = s[r:r + BAND, :] * scale
                here = at(pieces[u][0] + r, BAND)
                m0 = top[here, :]
                m = jnp.maximum(m0, jnp.max(x, axis=1, keepdims=True))
                top[here, :] = m
                factors.append(jnp.exp2(m0 - m))
                done.append(jnp.exp2(x - spread(m, rows)).astype(jnp.bfloat16))
            return jnp.concatenate(done, axis=0), jnp.concatenate(factors, axis=0)

        def three(u, weight, factor):
            r, where = pieces[u]
            here = at(r, tile)
            acc[here, :] = acc[here, :] * spread(factor, 2 * hdim) + mixed_pair(weight, a, b, where)

        flow(len(pieces), one, two, three)

    def unit(first, a, b, extent):
        work(first, a, b, [(r, parts[w][2]) for r in range(0, extent, tile) for w in (0, 2)])

    def sweep(a, b, h):
        where = pl.ds(pl.multiple_of(h * half_keys, half_keys), half_keys)
        work(0, a, b, [(r, where) for r in range(0, total_rows, tile)])

    def pick(if_right, if_left):
        return col * if_right + (1 - col) * if_left

    def sel(if_one, if_zero):
        return core * if_one + (1 - core) * if_zero

    core0, core1 = core == 0, core == 1
    pairs = (
        (pick(8 + pos_x, 4 + pos), sel(8 + pos_m, pick(8 + pos_d, 4 + pos_m)), right | has1 | core1),
        (pick(4 + pos, 4 + pos_x), pick(4 + pos_m, sel(4 + pos_m, 4 + pos_d)), has1),
        (pick(4 + pos_x, sel(4 + pos_d, pos)), pick(4 + pos_d, sel(pos, pos_m)), has2 | (has1 & (right | core1))),
        (pick(pos, pos_x), pick(sel(8 + pos_d, pos_m), pos_d), has2 | (right & core1)),
    )

    def local(t):
        return pl.ds(pl.multiple_of(t * tokens, tokens), tokens)

    def finish(first, t, put):
        whole = acc[pl.ds(pl.multiple_of(first + t * tile, tile), tile), :]
        norm[...] = whole[:, 0:hdim] / whole[:, hdim:]
        for g in range(group):
            put(g, norm[pl.ds(g, tokens, stride=group), :].astype(jnp.bfloat16))

    columns = pl.ds(pl.multiple_of(mine * (group * hdim), group * hdim), group * hdim)

    def outgoing(d, t):
        return pltpu.make_async_remote_copy(
            src_ref=stage.at[d - 1, local(t)],
            dst_ref=out_ref.at[local(t), columns],
            send_sem=osend_sem.at[d - 1, t],
            recv_sem=orecv_sem.at[d - 1, t],
            device_id={"head": (mine + d) % heads},
            device_id_type=MESH,
        )

    for load in loads:
        load.wait()
    diagonal()
    begin(HIGH)

    def first_in(which):
        landed(4 + pos, has1, "Z1", "X1", "D1", which=which)
        landed(8 + pos_x, right, "D0x", which=which)

    def first_over(which):
        landed(4 + pos_m, has1 & leftc & core0, which=which)
        landed(8 + pos_d, right & core0, which=which)
        landed(8 + pos_m, core1, which=which)

    @pl.loop(1, 12)
    def _(s):
        mark((8 + pos + s) % 12)

    @pl.loop(0, 4 * (me < 8).astype(jnp.int32) + 4 * (me < 4).astype(jnp.int32))
    def _(s):
        kbuf[s] = jnp.zeros((rows, hdim), jnp.bfloat16)
        vbuf[s] = jnp.zeros((rows, hdim), jnp.bfloat16)

    first_in(LOW)
    first_over(LOW)

    @pl.loop(0, 2)
    def _(h):
        @pl.when(h == 1)
        def _():
            first_in(HIGH)
            first_over(HIGH)
            landed(4 + pos_x, has1 & leftc, "D1x", which=LOW)

        @pl.when(pairs[0][2])
        def _():
            sweep(pairs[0][0], pairs[0][1], h)

    def event1():
        landed(4 + pos_x, has1 & leftc, "D1x", which=HIGH)
        landed(4 + pos_x, has1 & right, "D1x", which=LOW)
        landed(pos, has2 & right, "X2", "D2", which=LOW)
        landed(pos, has2 & right & core0, "X2", "D2", which=HIGH)
        landed(4 + pos_x, has1 & right & core0, "D1x", which=HIGH)
        landed(4 + pos_m, has1 & (right | core1))
        landed(4 + pos_d, has1 & leftc & core0)

    def event2():
        landed(pos, has2 & leftc, "D2")
        landed(pos, has2 & right & core1, "X2", "D2", which=HIGH)
        landed(4 + pos_x, has1 & right & core1, "D1x", which=HIGH)
        landed(4 + pos_d, has1 & (right | core1))
        landed(pos_m, has2 & leftc & core0)
        landed(pos_x, has2 & leftc, "D2x", which=LOW)

    def event3():
        landed(pos_x, has2 & leftc, "D2x", which=HIGH)
        landed(pos_d, has2 & leftc)
        landed(8 + pos_m, core0)
        landed(8 + pos_d, right & core1)
        landed(pos_m, has2 & (right | core1))

    others = list(range(1, heads))
    order = [(p, d) for p in ORDER for d in (others if p < 4 else [heads])]
    order = [(p % 4, d) for p, d in order]
    kinds = [p if d < heads else p + 4 for p, d in order]
    events = ((1, event1), (2, event2), (3, event3))

    def choose(index, values):
        return sum((index == i) * jnp.asarray(x, jnp.int32) for i, x in enumerate(values))

    @pl.loop(0, len(order))
    def _(u):
        for kind, event in events:
            pl.when(u == kinds.index(kind))(event)
        p = choose(u, [x for x, _ in order])
        d = choose(u, [x for _, x in order])
        first = (mine + d) % heads * span

        valid = choose(p, [x[2] for x in pairs]) == 1
        slots = choose(p, [x[0] for x in pairs]), choose(p, [x[1] for x in pairs])
        closing = (p == 3) & (d < heads)

        @pl.when(valid & jnp.logical_not(closing))
        def _():
            unit(first, *slots, span)

        @pl.when(closing)
        def _():
            @pl.loop(0, steps)
            def _(t):
                @pl.when(valid)
                def _():
                    unit(first + t * tile, *slots, tile)

                def put(g, piece):
                    stage[d - 1, local(t), g * hdim:(g + 1) * hdim] = piece

                finish(first, t, put)
                outgoing(d, t).start()

        @pl.when((p == 3) & (d == heads))
        def _():
            @pl.loop(0, steps)
            def _(t):
                def put(g, piece):
                    where = pl.ds(pl.multiple_of(mine * (group * hdim) + g * hdim, hdim), hdim)
                    out_ref[local(t), where] = piece

                finish(first, t, put)

    for d in range(1, heads):
        @pl.loop(0, steps)
        def _(t):
            outgoing(d, t).wait_send()
            source = (mine + heads - d) % heads
            cols = pl.ds(pl.multiple_of(source * (group * hdim), group * hdim), group * hdim)
            got = out_ref.at[local(t), cols]
            pltpu.make_async_copy(got, got, orecv_sem.at[d - 1, t]).wait()

    for name in moves:
        sent(name)


def on_device(mesh, queries, keys, values, doc_lengths):
    rows, group, hdim = queries.shape
    heads = mesh.shape["head"]
    n = mesh.shape["ctx"]
    bf16, f32 = jnp.bfloat16, jnp.float32
    part = rows // heads
    tile = min(MOST, part * group)
    steps = part * group // tile
    vmem = pl.BlockSpec(memory_space=pltpu.VMEM)
    anywhere = pl.BlockSpec(memory_space=pl.ANY)
    return pl.pallas_call(
        functools.partial(kernel, n, heads, tile),
        out_shape=pltpu.VMEM((part, heads * group * hdim), bf16),
        in_specs=[anywhere] * 4,
        out_specs=vmem,
        scratch_shapes=[
            pltpu.VMEM((12, rows, hdim), bf16),
            pltpu.VMEM((12, rows, hdim), bf16),
            pltpu.VMEM((12, rows, 128), bf16),
            pltpu.VMEM((rows * group, hdim + 128), bf16),
            pltpu.VMEM((rows * group, hdim + 128), f32),
            pltpu.VMEM((rows * group, 128), f32),
            pltpu.VMEM((tile, hdim), f32),
            pltpu.VMEM((heads - 1, part, group * hdim), bf16),
            pltpu.SMEM(doc_lengths.shape, jnp.int32),
            pltpu.SemaphoreType.DMA((11, 4)),
            pltpu.SemaphoreType.DMA((12, 4)),
            pltpu.SemaphoreType.DMA((heads - 1, steps)),
            pltpu.SemaphoreType.DMA((heads - 1, steps)),
            pltpu.SemaphoreType.DMA((4,)),
        ],
        compiler_params=pltpu.CompilerParams(
            collective_id=0, has_side_effects=True, vmem_limit_bytes=56 * 1024 * 1024),
    )(doc_lengths, queries.reshape(rows * group, hdim), keys.reshape(rows, hdim), values.reshape(rows, hdim))


def solution(mesh):
    placed = (P("ctx", "head", None), P("ctx", "head", None), P("ctx", "head", None), P())
    return jax.shard_map(
        functools.partial(on_device, mesh), mesh=mesh, in_specs=placed,
        out_specs=P(("ctx", "head"), None), check_vma=False
    )
```

```python
import functools
import math

import jax
import jax.numpy as jnp
from jax import lax
from jax.experimental import pallas as pl
from jax.experimental.pallas import tpu as pltpu
from jax.sharding import PartitionSpec as P

MESH = pl.DeviceIdType.MESH
BIG = 1e30
MOST = 512
BAND = 128
ORDER = (1, 2, 3, 5, 6, 7)
LOW, HIGH = (0, 1), (2, 3)
ALL = LOW + HIGH


def kernel(n, heads, tile, lens_in, q_ref, k_ref, v_ref, out_ref,
           kbuf, vbuf, kdoc, qaug, acc, top, norm, stage,
           lens_ref, send_sem, recv_sem, osend_sem, orecv_sem, load_sem):
    rows, hdim = k_ref.shape
    total_rows = q_ref.shape[0]
    group = total_rows // rows
    me = lax.axis_index("ctx")
    mine = lax.axis_index("head")
    pos = me % 4
    core = pos % 2
    col = pos // 2
    mate = me + 1 - 2 * core
    across = me + 2 - 4 * col
    pos_m = pos + 1 - 2 * core
    pos_x = pos + 2 - 4 * col
    pos_d = pos_x + pos_m - pos
    has1 = me >= 4
    has2 = me >= 8
    feeds = me + 4 < n
    right = col == 1
    leftc = col == 0

    lens_load = pltpu.make_async_copy(lens_in, lens_ref, load_sem.at[3])
    lens_load.start()
    loads = (
        pltpu.make_async_copy(k_ref, kbuf.at[8 + pos], load_sem.at[0]),
        pltpu.make_async_copy(q_ref, qaug.at[:, 0:hdim], load_sem.at[1]),
        pltpu.make_async_copy(v_ref, vbuf.at[8 + pos], load_sem.at[2]),
    )
    for load in loads:
        load.start()

    barrier = pltpu.get_barrier_semaphore()
    for peer in (mate, across):
        pl.semaphore_signal(barrier, inc=1, device_id={"ctx": peer}, device_id_type=MESH)

    @pl.when(has1)
    def _():
        pl.semaphore_signal(barrier, inc=1, device_id={"ctx": me - 4}, device_id_type=MESH)

    @pl.when(feeds)
    def _():
        pl.semaphore_signal(barrier, inc=1, device_id={"ctx": me + 4}, device_id_type=MESH)

    for d in range(1, heads):
        pl.semaphore_signal(barrier, inc=1, device_id={"head": (mine + d) % heads}, device_id_type=MESH)

    half_keys = rows // 2
    parts = [(own, buf, pl.ds(h * half_keys, half_keys)) for h in range(2) for own, buf in ((k_ref, kbuf), (v_ref, vbuf))]

    def copies(lane, slot, to_slot, target):
        return [pltpu.make_async_remote_copy(
            src_ref=own.at[where] if slot is None else buf.at[slot, where],
            dst_ref=buf.at[to_slot, where],
            send_sem=send_sem.at[lane, w],
            recv_sem=recv_sem.at[to_slot, w],
            device_id={"ctx": target},
            device_id_type=MESH,
        ) for w, (own, buf, where) in enumerate(parts)]

    moves = {
        "D0": (copies(0, None, 8 + pos, mate), core == 0),
        "X0": (copies(1, None, 8 + pos, across), leftc),
        "Z0": (copies(2, None, 4 + pos, me + 4), feeds),
        "D0x": (copies(3, 8 + pos_x, 8 + pos_x, mate), right),
        "D1": (copies(4, 4 + pos, 4 + pos, mate), has1),
        "X1": (copies(5, 4 + pos, 4 + pos, across), has1),
        "Z1": (copies(6, 4 + pos, pos, me + 4), has1 & feeds),
        "D1x": (copies(7, 4 + pos_x, 4 + pos_x, mate), has1),
        "D2": (copies(8, pos, pos, mate), has2 & (core == 1)),
        "X2": (copies(9, pos, pos, across), has2 & right),
        "D2x": (copies(10, pos_x, pos_x, mate), has2 & leftc),
    }

    def when(cond, fn):
        if cond is None:
            fn()
        else:
            pl.when(cond)(fn)

    def sent(name):
        made, cond = moves[name]

        def go():
            for copy in made:
                copy.wait_send()

        when(cond, go)

    def landed(slot, cond, *names, which=ALL):
        for w in which:
            _, buf, where = parts[w]

            def go():
                spot = buf.at[slot, where]
                pltpu.make_async_copy(spot, spot, recv_sem.at[slot, w]).wait()

            when(cond, go)
            for name in names:
                made, also = moves[name]
                when(cond if also is None else cond & also, made[w].start)

    def begin(which):
        for w in which:
            for name in ("Z0", "X0", "D0"):
                made, also = moves[name]
                when(also, made[w].start)

    lens_load.wait()

    lane = lax.broadcasted_iota(jnp.int32, (8, 128), 1)
    firsts = jnp.full((8, 128), 2**30, jnp.int32)
    ends = jnp.full((8, 128), 2**30, jnp.int32)
    run = jnp.int32(0)
    for d in range(lens_ref.shape[0]):
        firsts = jnp.where(lane == d, run, firsts)
        run = run + lens_ref[d]
        ends = jnp.where(lane == d, run, ends)
    first_row, end_row = firsts[0:1], ends[0:1]

    def member(position):
        return (position >= first_row) & (position < end_row)

    base = me * rows
    part = rows // heads
    tokens = tile // group
    steps = part // tokens
    span = part * group

    def by_token(width, dim):
        return lax.broadcasted_iota(jnp.int32, (tokens, group, width), dim).reshape(tile, width)

    @pl.loop(0, total_rows // tile)
    def _(t):
        at = pl.ds(pl.multiple_of(t * tile, tile), tile)
        qaug[at, hdim:] = jnp.where(member(base + t * tokens + by_token(128, 0)), 1.0, 0.0).astype(jnp.bfloat16)

    def mark(s):
        kpos = (me - pos - 8 + s) * rows + lax.broadcasted_iota(jnp.int32, (rows, 128), 0)
        kdoc[s] = jnp.where(member(kpos), 0.0, -BIG).astype(jnp.bfloat16)

    mark(8 + pos)
    pl.semaphore_wait(barrier, 1 + heads + has1.astype(jnp.int32) + feeds.astype(jnp.int32))
    begin(LOW)

    scale = math.log2(math.e) / hdim**0.5

    def spread(x, width):
        return jnp.concatenate([x] * (width // 128), axis=1)

    def raw(at, slot, width):
        return lax.dot_general(
            qaug[at, :], jnp.concatenate([kbuf[slot, 0:width, :], kdoc[slot, 0:width, :]], axis=1),
            (((1,), (1,)), ((), ())), preferred_element_type=jnp.float32)

    def mixed(weight, slot, width):
        ones = jnp.ones((width, 128), jnp.bfloat16)
        return jnp.dot(weight, jnp.concatenate([vbuf[slot, 0:width, :], ones], axis=1),
                       preferred_element_type=jnp.float32)

    def raw_pair(at, a, b, where):
        keys = [jnp.concatenate([kbuf[x, where, :], kdoc[x, where, :]], axis=1) for x in (a, b)]
        return lax.dot_general(
            qaug[at, :], jnp.concatenate(keys, axis=0), (((1,), (1,)), ((), ())), preferred_element_type=jnp.float32)

    def mixed_pair(weight, a, b, where):
        ones = jnp.ones((rows, 128), jnp.bfloat16)
        vals = jnp.concatenate([vbuf[a, where, :], vbuf[b, where, :]], axis=0)
        return jnp.dot(weight, jnp.concatenate([vals, ones], axis=1), preferred_element_type=jnp.float32)

    def flow(count, one, two, three):
        scores, weights = {}, {}
        for u in range(count + 2):
            if u >= 2:
                three(u - 2, *weights.pop(u - 2))
            if 1 <= u <= count:
                weights[u - 1] = two(u - 1, scores.pop(u - 1))
            if u < count:
                scores[u] = one(u)

    def diagonal():
        def width(t):
            return -(-(t + 1) * tokens // 128) * 128

        def at(t):
            return pl.ds(t * tile, tile)

        def one(t):
            return raw(at(t), 8 + pos, width(t))

        def two(t, s):
            wide, done = width(t), []
            for r in range(0, tile, BAND):
                here = slice(r, r + BAND)
                x = s[here, :] * scale
                edge = by_token(128, 2)[here] - by_token(128, 0)[here] <= t * tokens - (wide - 128)
                last = jnp.where(edge, x[:, wide - 128:], -BIG)
                x = last if wide == 128 else jnp.concatenate([x[:, :wide - 128], last], axis=1)
                m = jnp.broadcast_to(jnp.max(x, axis=1, keepdims=True), (BAND, 128))
                top[pl.ds(t * tile + r, BAND), :] = m
                done.append(jnp.exp2(x - spread(m, wide)).astype(jnp.bfloat16))
            return (jnp.concatenate(done, axis=0),)

        def three(t, weight):
            acc[at(t), :] = mixed(weight, 8 + pos, width(t))

        flow(total_rows // tile, one, two, three)

    def work(first, a, b, pieces):
        def at(r, size):
            return pl.ds(pl.multiple_of(first + r, BAND), size)

        def one(u):
            r, where = pieces[u]
            return raw_pair(at(r, tile), a, b, where)

        def two(u, s):
            done, factors = [], []
            for r in range(0, tile, BAND):
                x = s[r:r + BAND, :] * scale
                here = at(pieces[u][0] + r, BAND)
                m0 = top[here, :]
                m = jnp.maximum(m0, jnp.max(x, axis=1, keepdims=True))
                top[here, :] = m
                factors.append(jnp.exp2(m0 - m))
                done.append(jnp.exp2(x - spread(m, rows)).astype(jnp.bfloat16))
            return jnp.concatenate(done, axis=0), jnp.concatenate(factors, axis=0)

        def three(u, weight, factor):
            r, where = pieces[u]
            here = at(r, tile)
            acc[here, :] = acc[here, :] * spread(factor, 2 * hdim) + mixed_pair(weight, a, b, where)

        flow(len(pieces), one, two, three)

    def unit(first, a, b, extent):
        work(first, a, b, [(r, parts[w][2]) for r in range(0, extent, tile) for w in (0, 2)])

    def sweep(a, b, h):
        where = pl.ds(pl.multiple_of(h * half_keys, half_keys), half_keys)
        work(0, a, b, [(r, where) for r in range(0, total_rows, tile)])

    def pick(if_right, if_left):
        return col * if_right + (1 - col) * if_left

    def sel(if_one, if_zero):
        return core * if_one + (1 - core) * if_zero

    core0, core1 = core == 0, core == 1
    pairs = (
        (pick(8 + pos_x, 4 + pos), sel(8 + pos_m, pick(8 + pos_d, 4 + pos_m)), right | has1 | core1),
        (pick(4 + pos, 4 + pos_x), pick(4 + pos_m, sel(4 + pos_m, 4 + pos_d)), has1),
        (pick(4 + pos_x, sel(4 + pos_d, pos)), pick(4 + pos_d, sel(pos, pos_m)), has2 | (has1 & (right | core1))),
        (pick(pos, pos_x), pick(sel(8 + pos_d, pos_m), pos_d), has2 | (right & core1)),
    )

    def local(t):
        return pl.ds(pl.multiple_of(t * tokens, tokens), tokens)

    def finish(first, t, put):
        whole = acc[pl.ds(pl.multiple_of(first + t * tile, tile), tile), :]
        norm[...] = whole[:, 0:hdim] / whole[:, hdim:]
        for g in range(group):
            put(g, norm[pl.ds(g, tokens, stride=group), :].astype(jnp.bfloat16))

    columns = pl.ds(pl.multiple_of(mine * (group * hdim), group * hdim), group * hdim)

    def outgoing(d, t):
        return pltpu.make_async_remote_copy(
            src_ref=stage.at[d - 1, local(t)],
            dst_ref=out_ref.at[local(t), columns],
            send_sem=osend_sem.at[d - 1, t],
            recv_sem=orecv_sem.at[d - 1, t],
            device_id={"head": (mine + d) % heads},
            device_id_type=MESH,
        )

    for load in loads:
        load.wait()
    diagonal()
    begin(HIGH)

    def first_in(which):
        landed(4 + pos, has1, "Z1", "X1", "D1", which=which)
        landed(8 + pos_x, right, "D0x", which=which)

    def first_over(which):
        landed(4 + pos_m, has1 & leftc & core0, which=which)
        landed(8 + pos_d, right & core0, which=which)
        landed(8 + pos_m, core1, which=which)

    @pl.loop(1, 12)
    def _(s):
        mark((8 + pos + s) % 12)

    @pl.loop(0, 4 * (me < 8).astype(jnp.int32) + 4 * (me < 4).astype(jnp.int32))
    def _(s):
        kbuf[s] = jnp.zeros((rows, hdim), jnp.bfloat16)
        vbuf[s] = jnp.zeros((rows, hdim), jnp.bfloat16)

    first_in(LOW)
    first_over(LOW)

    @pl.loop(0, 2)
    def _(h):
        @pl.when(h == 1)
        def _():
            first_in(HIGH)
            first_over(HIGH)

        @pl.when(pairs[0][2])
        def _():
            sweep(pairs[0][0], pairs[0][1], h)

    def event1():
        landed(4 + pos_x, has1 & leftc, "D1x")
        landed(4 + pos_x, has1 & right, "D1x", which=LOW)
        landed(pos, has2 & right, "X2", "D2", which=LOW)
        landed(pos, has2 & right & core0, "X2", "D2", which=HIGH)
        landed(4 + pos_x, has1 & right & core0, "D1x", which=HIGH)
        landed(4 + pos_m, has1 & (right | core1))
        landed(4 + pos_d, has1 & leftc & core0)

    def event2():
        landed(pos, has2 & leftc, "D2")
        landed(pos, has2 & right & core1, "X2", "D2", which=HIGH)
        landed(4 + pos_x, has1 & right & core1, "D1x", which=HIGH)
        landed(4 + pos_d, has1 & (right | core1))
        landed(pos_m, has2 & leftc & core0)
        landed(pos_x, has2 & leftc, "D2x", which=LOW)

    def event3():
        landed(pos_x, has2 & leftc, "D2x", which=HIGH)
        landed(pos_d, has2 & leftc)
        landed(8 + pos_d, right & core1)
        landed(pos_m, has2 & right & core0)

    others = list(range(1, heads))
    order = [(p, d) for p in ORDER for d in (others if p < 4 else [heads])]
    order = [(p % 4, d) for p, d in order]
    kinds = [p if d < heads else p + 4 for p, d in order]
    events = ((1, event1), (2, event2), (3, event3))

    def choose(index, values):
        return sum((index == i) * jnp.asarray(x, jnp.int32) for i, x in enumerate(values))

    @pl.loop(0, len(order))
    def _(u):
        for kind, event in events:
            pl.when(u == kinds.index(kind))(event)
        p = choose(u, [x for x, _ in order])
        d = choose(u, [x for _, x in order])
        first = (mine + d) % heads * span

        valid = choose(p, [x[2] for x in pairs]) == 1
        slots = choose(p, [x[0] for x in pairs]), choose(p, [x[1] for x in pairs])
        closing = (p == 3) & (d < heads)

        @pl.when(valid & jnp.logical_not(closing))
        def _():
            unit(first, *slots, span)

        @pl.when(closing)
        def _():
            @pl.loop(0, steps)
            def _(t):
                @pl.when(valid)
                def _():
                    unit(first + t * tile, *slots, tile)

                def put(g, piece):
                    stage[d - 1, local(t), g * hdim:(g + 1) * hdim] = piece

                finish(first, t, put)
                outgoing(d, t).start()

        @pl.when((p == 3) & (d == heads))
        def _():
            @pl.loop(0, steps)
            def _(t):
                def put(g, piece):
                    where = pl.ds(pl.multiple_of(mine * (group * hdim) + g * hdim, hdim), hdim)
                    out_ref[local(t), where] = piece

                finish(first, t, put)

    for d in range(1, heads):
        @pl.loop(0, steps)
        def _(t):
            outgoing(d, t).wait_send()
            source = (mine + heads - d) % heads
            cols = pl.ds(pl.multiple_of(source * (group * hdim), group * hdim), group * hdim)
            got = out_ref.at[local(t), cols]
            pltpu.make_async_copy(got, got, orecv_sem.at[d - 1, t]).wait()

    for name in moves:
        sent(name)


def on_device(mesh, queries, keys, values, doc_lengths):
    rows, group, hdim = queries.shape
    heads = mesh.shape["head"]
    n = mesh.shape["ctx"]
    bf16, f32 = jnp.bfloat16, jnp.float32
    part = rows // heads
    tile = min(MOST, part * group)
    steps = part * group // tile
    vmem = pl.BlockSpec(memory_space=pltpu.VMEM)
    anywhere = pl.BlockSpec(memory_space=pl.ANY)
    return pl.pallas_call(
        functools.partial(kernel, n, heads, tile),
        out_shape=pltpu.VMEM((part, heads * group * hdim), bf16),
        in_specs=[anywhere] * 4,
        out_specs=vmem,
        scratch_shapes=[
            pltpu.VMEM((12, rows, hdim), bf16),
            pltpu.VMEM((12, rows, hdim), bf16),
            pltpu.VMEM((12, rows, 128), bf16),
            pltpu.VMEM((rows * group, hdim + 128), bf16),
            pltpu.VMEM((rows * group, hdim + 128), f32),
            pltpu.VMEM((rows * group, 128), f32),
            pltpu.VMEM((tile, hdim), f32),
            pltpu.VMEM((heads - 1, part, group * hdim), bf16),
            pltpu.SMEM(doc_lengths.shape, jnp.int32),
            pltpu.SemaphoreType.DMA((11, 4)),
            pltpu.SemaphoreType.DMA((12, 4)),
            pltpu.SemaphoreType.DMA((heads - 1, steps)),
            pltpu.SemaphoreType.DMA((heads - 1, steps)),
            pltpu.SemaphoreType.DMA((4,)),
        ],
        compiler_params=pltpu.CompilerParams(
            collective_id=0, has_side_effects=True, vmem_limit_bytes=56 * 1024 * 1024),
    )(doc_lengths, queries.reshape(rows * group, hdim), keys.reshape(rows, hdim), values.reshape(rows, hdim))


def solution(mesh):
    placed = (P("ctx", "head", None), P("ctx", "head", None), P("ctx", "head", None), P())
    return jax.shard_map(
        functools.partial(on_device, mesh), mesh=mesh, in_specs=placed,
        out_specs=P(("ctx", "head"), None), check_vma=False
    )
```

```python
import functools
import math

import jax
import jax.numpy as jnp
from jax import lax
from jax.experimental import pallas as pl
from jax.experimental.pallas import tpu as pltpu
from jax.sharding import PartitionSpec as P

MESH = pl.DeviceIdType.MESH
BIG = 1e30
MOST = 512
BAND = 128
ORDER = (1, 2, 3, 5, 6, 7)
FILLED = (1, 2, 5, 3, 6, 7)
LOW, HIGH = (0, 1), (2, 3)
ALL = LOW + HIGH


def kernel(n, heads, tile, lens_in, q_ref, k_ref, v_ref, out_ref,
           kbuf, vbuf, kdoc, qaug, acc, top, norm, stage,
           lens_ref, send_sem, recv_sem, osend_sem, orecv_sem, load_sem):
    rows, hdim = k_ref.shape
    total_rows = q_ref.shape[0]
    group = total_rows // rows
    me = lax.axis_index("ctx")
    mine = lax.axis_index("head")
    pos = me % 4
    core = pos % 2
    col = pos // 2
    mate = me + 1 - 2 * core
    across = me + 2 - 4 * col
    pos_m = pos + 1 - 2 * core
    pos_x = pos + 2 - 4 * col
    pos_d = pos_x + pos_m - pos
    has1 = me >= 4
    has2 = me >= 8
    feeds = me + 4 < n
    right = col == 1
    leftc = col == 0

    lens_load = pltpu.make_async_copy(lens_in, lens_ref, load_sem.at[3])
    lens_load.start()
    loads = (
        pltpu.make_async_copy(k_ref, kbuf.at[8 + pos], load_sem.at[0]),
        pltpu.make_async_copy(q_ref, qaug.at[:, 0:hdim], load_sem.at[1]),
        pltpu.make_async_copy(v_ref, vbuf.at[8 + pos], load_sem.at[2]),
    )
    for load in loads:
        load.start()

    barrier = pltpu.get_barrier_semaphore()
    for peer in (mate, across):
        pl.semaphore_signal(barrier, inc=1, device_id={"ctx": peer}, device_id_type=MESH)

    @pl.when(has1)
    def _():
        pl.semaphore_signal(barrier, inc=1, device_id={"ctx": me - 4}, device_id_type=MESH)

    @pl.when(feeds)
    def _():
        pl.semaphore_signal(barrier, inc=1, device_id={"ctx": me + 4}, device_id_type=MESH)

    for d in range(1, heads):
        pl.semaphore_signal(barrier, inc=1, device_id={"head": (mine + d) % heads}, device_id_type=MESH)

    half_keys = rows // 2
    parts = [(own, buf, pl.ds(h * half_keys, half_keys)) for h in range(2) for own, buf in ((k_ref, kbuf), (v_ref, vbuf))]

    def copies(lane, slot, to_slot, target):
        return [pltpu.make_async_remote_copy(
            src_ref=own.at[where] if slot is None else buf.at[slot, where],
            dst_ref=buf.at[to_slot, where],
            send_sem=send_sem.at[lane, w],
            recv_sem=recv_sem.at[to_slot, w],
            device_id={"ctx": target},
            device_id_type=MESH,
        ) for w, (own, buf, where) in enumerate(parts)]

    moves = {
        "D0": (copies(0, None, 8 + pos, mate), core == 0),
        "X0": (copies(1, None, 8 + pos, across), leftc),
        "Z0": (copies(2, None, 4 + pos, me + 4), feeds),
        "D0x": (copies(3, 8 + pos_x, 8 + pos_x, mate), right),
        "D1": (copies(4, 4 + pos, 4 + pos, mate), has1),
        "X1": (copies(5, 4 + pos, 4 + pos, across), has1),
        "Z1": (copies(6, 4 + pos, pos, me + 4), has1 & feeds),
        "D1x": (copies(7, 4 + pos_x, 4 + pos_x, mate), has1),
        "D2": (copies(8, pos, pos, mate), has2 & (core == 1)),
        "X2": (copies(9, pos, pos, across), has2 & right),
        "D2x": (copies(10, pos_x, pos_x, mate), has2 & leftc),
    }

    def when(cond, fn):
        if cond is None:
            fn()
        else:
            pl.when(cond)(fn)

    def sent(name):
        made, cond = moves[name]

        def go():
            for copy in made:
                copy.wait_send()

        when(cond, go)

    def landed(slot, cond, *names, which=ALL):
        for w in which:
            _, buf, where = parts[w]

            def go():
                spot = buf.at[slot, where]
                pltpu.make_async_copy(spot, spot, recv_sem.at[slot, w]).wait()

            when(cond, go)
            for name in names:
                made, also = moves[name]
                when(cond if also is None else cond & also, made[w].start)

    def begin(which):
        for w in which:
            for name in ("Z0", "X0", "D0"):
                made, also = moves[name]
                when(also, made[w].start)

    lens_load.wait()

    lane = lax.broadcasted_iota(jnp.int32, (8, 128), 1)
    firsts = jnp.full((8, 128), 2**30, jnp.int32)
    ends = jnp.full((8, 128), 2**30, jnp.int32)
    run = jnp.int32(0)
    for d in range(lens_ref.shape[0]):
        firsts = jnp.where(lane == d, run, firsts)
        run = run + lens_ref[d]
        ends = jnp.where(lane == d, run, ends)
    first_row, end_row = firsts[0:1], ends[0:1]

    def member(position):
        return (position >= first_row) & (position < end_row)

    base = me * rows
    part = rows // heads
    tokens = tile // group
    steps = part // tokens
    span = part * group

    def by_token(width, dim):
        return lax.broadcasted_iota(jnp.int32, (tokens, group, width), dim).reshape(tile, width)

    @pl.loop(0, total_rows // tile)
    def _(t):
        at = pl.ds(pl.multiple_of(t * tile, tile), tile)
        qaug[at, hdim:] = jnp.where(member(base + t * tokens + by_token(128, 0)), 1.0, 0.0).astype(jnp.bfloat16)

    def mark(s):
        kpos = (me - pos - 8 + s) * rows + lax.broadcasted_iota(jnp.int32, (rows, 128), 0)
        kdoc[s] = jnp.where(member(kpos), 0.0, -BIG).astype(jnp.bfloat16)

    mark(8 + pos)
    pl.semaphore_wait(barrier, 1 + heads + has1.astype(jnp.int32) + feeds.astype(jnp.int32))
    begin(LOW)

    scale = math.log2(math.e) / hdim**0.5

    def spread(x, width):
        return jnp.concatenate([x] * (width // 128), axis=1)

    def raw(at, slot, width):
        return lax.dot_general(
            qaug[at, :], jnp.concatenate([kbuf[slot, 0:width, :], kdoc[slot, 0:width, :]], axis=1),
            (((1,), (1,)), ((), ())), preferred_element_type=jnp.float32)

    def mixed(weight, slot, width):
        ones = jnp.ones((width, 128), jnp.bfloat16)
        return jnp.dot(weight, jnp.concatenate([vbuf[slot, 0:width, :], ones], axis=1),
                       preferred_element_type=jnp.float32)

    def raw_pair(at, a, b, where):
        keys = [jnp.concatenate([kbuf[x, where, :], kdoc[x, where, :]], axis=1) for x in (a, b)]
        return lax.dot_general(
            qaug[at, :], jnp.concatenate(keys, axis=0), (((1,), (1,)), ((), ())), preferred_element_type=jnp.float32)

    def mixed_pair(weight, a, b, where):
        ones = jnp.ones((rows, 128), jnp.bfloat16)
        vals = jnp.concatenate([vbuf[a, where, :], vbuf[b, where, :]], axis=0)
        return jnp.dot(weight, jnp.concatenate([vals, ones], axis=1), preferred_element_type=jnp.float32)

    def flow(count, one, two, three):
        scores, weights = {}, {}
        for u in range(count + 2):
            if u >= 2:
                three(u - 2, *weights.pop(u - 2))
            if 1 <= u <= count:
                weights[u - 1] = two(u - 1, scores.pop(u - 1))
            if u < count:
                scores[u] = one(u)

    def diagonal():
        def width(t):
            return -(-(t + 1) * tokens // 128) * 128

        def at(t):
            return pl.ds(t * tile, tile)

        def one(t):
            return raw(at(t), 8 + pos, width(t))

        def two(t, s):
            wide, done = width(t), []
            for r in range(0, tile, BAND):
                here = slice(r, r + BAND)
                x = s[here, :] * scale
                edge = by_token(128, 2)[here] - by_token(128, 0)[here] <= t * tokens - (wide - 128)
                last = jnp.where(edge, x[:, wide - 128:], -BIG)
                x = last if wide == 128 else jnp.concatenate([x[:, :wide - 128], last], axis=1)
                m = jnp.broadcast_to(jnp.max(x, axis=1, keepdims=True), (BAND, 128))
                top[pl.ds(t * tile + r, BAND), :] = m
                done.append(jnp.exp2(x - spread(m, wide)).astype(jnp.bfloat16))
            return (jnp.concatenate(done, axis=0),)

        def three(t, weight):
            acc[at(t), :] = mixed(weight, 8 + pos, width(t))

        flow(total_rows // tile, one, two, three)

    def work(first, a, b, pieces):
        def at(r, size):
            return pl.ds(pl.multiple_of(first + r, BAND), size)

        def one(u):
            r, where = pieces[u]
            return raw_pair(at(r, tile), a, b, where)

        def two(u, s):
            done, factors = [], []
            for r in range(0, tile, BAND):
                x = s[r:r + BAND, :] * scale
                here = at(pieces[u][0] + r, BAND)
                m0 = top[here, :]
                m = jnp.maximum(m0, jnp.max(x, axis=1, keepdims=True))
                top[here, :] = m
                factors.append(jnp.exp2(m0 - m))
                done.append(jnp.exp2(x - spread(m, rows)).astype(jnp.bfloat16))
            return jnp.concatenate(done, axis=0), jnp.concatenate(factors, axis=0)

        def three(u, weight, factor):
            r, where = pieces[u]
            here = at(r, tile)
            acc[here, :] = acc[here, :] * spread(factor, 2 * hdim) + mixed_pair(weight, a, b, where)

        flow(len(pieces), one, two, three)

    def unit(first, a, b, extent):
        work(first, a, b, [(r, parts[w][2]) for r in range(0, extent, tile) for w in (0, 2)])

    def sweep(a, b, h):
        where = pl.ds(pl.multiple_of(h * half_keys, half_keys), half_keys)
        work(0, a, b, [(r, where) for r in range(0, total_rows, tile)])

    def pick(if_right, if_left):
        return col * if_right + (1 - col) * if_left

    def sel(if_one, if_zero):
        return core * if_one + (1 - core) * if_zero

    core0, core1 = core == 0, core == 1
    pairs = (
        (pick(8 + pos_x, 4 + pos), sel(8 + pos_m, pick(8 + pos_d, 4 + pos_m)), right | has1 | core1),
        (pick(4 + pos, 4 + pos_x), pick(4 + pos_m, sel(4 + pos_m, 4 + pos_d)), has1),
        (pick(4 + pos_x, sel(4 + pos_d, pos)), pick(4 + pos_d, sel(pos, pos_m)), has2 | (has1 & (right | core1))),
        (pick(pos, pos_x), pick(sel(8 + pos_d, pos_m), pos_d), has2 | (right & core1)),
    )

    def local(t):
        return pl.ds(pl.multiple_of(t * tokens, tokens), tokens)

    def finish(first, t, put):
        whole = acc[pl.ds(pl.multiple_of(first + t * tile, tile), tile), :]
        norm[...] = whole[:, 0:hdim] / whole[:, hdim:]
        for g in range(group):
            put(g, norm[pl.ds(g, tokens, stride=group), :].astype(jnp.bfloat16))

    columns = pl.ds(pl.multiple_of(mine * (group * hdim), group * hdim), group * hdim)

    def outgoing(d, t):
        return pltpu.make_async_remote_copy(
            src_ref=stage.at[d - 1, local(t)],
            dst_ref=out_ref.at[local(t), columns],
            send_sem=osend_sem.at[d - 1, t],
            recv_sem=orecv_sem.at[d - 1, t],
            device_id={"head": (mine + d) % heads},
            device_id_type=MESH,
        )

    for load in loads:
        load.wait()
    diagonal()
    begin(HIGH)

    def first_in(which):
        landed(4 + pos, has1, "Z1", "X1", "D1", which=which)
        landed(8 + pos_x, right, "D0x", which=which)

    def first_over(which):
        landed(4 + pos_m, has1 & leftc & core0, which=which)
        landed(8 + pos_d, right & core0, which=which)
        landed(8 + pos_m, core1, which=which)

    @pl.loop(1, 12)
    def _(s):
        mark((8 + pos + s) % 12)

    @pl.loop(0, 4 * (me < 8).astype(jnp.int32) + 4 * (me < 4).astype(jnp.int32))
    def _(s):
        kbuf[s] = jnp.zeros((rows, hdim), jnp.bfloat16)
        vbuf[s] = jnp.zeros((rows, hdim), jnp.bfloat16)

    first_in(LOW)
    first_over(LOW)

    @pl.loop(0, 2)
    def _(h):
        @pl.when(h == 1)
        def _():
            first_in(HIGH)
            first_over(HIGH)

        @pl.when(pairs[0][2])
        def _():
            sweep(pairs[0][0], pairs[0][1], h)

    def event1():
        landed(4 + pos_x, has1 & leftc, "D1x")
        landed(4 + pos_x, has1 & right, "D1x", which=LOW)
        landed(pos, has2 & right, "X2", "D2", which=LOW)
        landed(pos, has2 & right & core0, "X2", "D2", which=HIGH)
        landed(4 + pos_x, has1 & right & core0, "D1x", which=HIGH)
        landed(4 + pos_m, has1 & (right | core1))
        landed(4 + pos_d, has1 & leftc & core0)

    def event2():
        landed(pos, has2 & leftc, "D2")
        landed(pos, has2 & right & core1, "X2", "D2", which=HIGH)
        landed(4 + pos_x, has1 & right & core1, "D1x", which=HIGH)
        landed(4 + pos_d, has1 & (right | core1))
        landed(pos_m, has2 & leftc & core0)
        landed(pos_x, has2 & leftc, "D2x", which=LOW)

    def event3():
        landed(pos_x, has2 & leftc, "D2x", which=HIGH)

    def event4():
        landed(pos_d, has2 & leftc)
        landed(8 + pos_d, right & core1)
        landed(pos_m, has2 & right & core0)

    others = list(range(1, heads))
    plans = [[(p % 4, d) for p in order for d in (others if p < 4 else [heads])] for order in (ORDER, FILLED)]
    kinds = [[p if d < heads else p + 4 for p, d in plan] for plan in plans]
    filled = (leftc & core1).astype(jnp.int32)
    spots = [[kind.index(p) for kind in kinds] for p in (1, 2, 3)]
    events = (
        (spots[0], event1), (spots[1], event2), ([min(spots[2])] * 2, event3), (spots[2], event4))

    def either(pair):
        return filled * pair[1] + (1 - filled) * pair[0]

    def choose(index, values):
        return sum((index == i) * jnp.asarray(x, jnp.int32) for i, x in enumerate(values))

    @pl.loop(0, len(plans[0]))
    def _(u):
        for places, event in events:
            pl.when(u == either(places))(event)
        p = either([choose(u, [x for x, _ in plan]) for plan in plans])
        d = either([choose(u, [x for _, x in plan]) for plan in plans])
        first = (mine + d) % heads * span

        valid = choose(p, [x[2] for x in pairs]) == 1
        slots = choose(p, [x[0] for x in pairs]), choose(p, [x[1] for x in pairs])
        closing = (p == 3) & (d < heads)

        @pl.when(valid & jnp.logical_not(closing))
        def _():
            unit(first, *slots, span)

        @pl.when(closing)
        def _():
            @pl.loop(0, steps)
            def _(t):
                @pl.when(valid)
                def _():
                    unit(first + t * tile, *slots, tile)

                def put(g, piece):
                    stage[d - 1, local(t), g * hdim:(g + 1) * hdim] = piece

                finish(first, t, put)
                outgoing(d, t).start()

        @pl.when((p == 3) & (d == heads))
        def _():
            @pl.loop(0, steps)
            def _(t):
                def put(g, piece):
                    where = pl.ds(pl.multiple_of(mine * (group * hdim) + g * hdim, hdim), hdim)
                    out_ref[local(t), where] = piece

                finish(first, t, put)

    for d in range(1, heads):
        @pl.loop(0, steps)
        def _(t):
            outgoing(d, t).wait_send()
            source = (mine + heads - d) % heads
            cols = pl.ds(pl.multiple_of(source * (group * hdim), group * hdim), group * hdim)
            got = out_ref.at[local(t), cols]
            pltpu.make_async_copy(got, got, orecv_sem.at[d - 1, t]).wait()

    for name in moves:
        sent(name)


def on_device(mesh, queries, keys, values, doc_lengths):
    rows, group, hdim = queries.shape
    heads = mesh.shape["head"]
    n = mesh.shape["ctx"]
    bf16, f32 = jnp.bfloat16, jnp.float32
    part = rows // heads
    tile = min(MOST, part * group)
    steps = part * group // tile
    vmem = pl.BlockSpec(memory_space=pltpu.VMEM)
    anywhere = pl.BlockSpec(memory_space=pl.ANY)
    return pl.pallas_call(
        functools.partial(kernel, n, heads, tile),
        out_shape=pltpu.VMEM((part, heads * group * hdim), bf16),
        in_specs=[anywhere] * 4,
        out_specs=vmem,
        scratch_shapes=[
            pltpu.VMEM((12, rows, hdim), bf16),
            pltpu.VMEM((12, rows, hdim), bf16),
            pltpu.VMEM((12, rows, 128), bf16),
            pltpu.VMEM((rows * group, hdim + 128), bf16),
            pltpu.VMEM((rows * group, hdim + 128), f32),
            pltpu.VMEM((rows * group, 128), f32),
            pltpu.VMEM((tile, hdim), f32),
            pltpu.VMEM((heads - 1, part, group * hdim), bf16),
            pltpu.SMEM(doc_lengths.shape, jnp.int32),
            pltpu.SemaphoreType.DMA((11, 4)),
            pltpu.SemaphoreType.DMA((12, 4)),
            pltpu.SemaphoreType.DMA((heads - 1, steps)),
            pltpu.SemaphoreType.DMA((heads - 1, steps)),
            pltpu.SemaphoreType.DMA((4,)),
        ],
        compiler_params=pltpu.CompilerParams(
            collective_id=0, has_side_effects=True, vmem_limit_bytes=56 * 1024 * 1024),
    )(doc_lengths, queries.reshape(rows * group, hdim), keys.reshape(rows, hdim), values.reshape(rows, hdim))


def solution(mesh):
    placed = (P("ctx", "head", None), P("ctx", "head", None), P("ctx", "head", None), P())
    return jax.shard_map(
        functools.partial(on_device, mesh), mesh=mesh, in_specs=placed,
        out_specs=P(("ctx", "head"), None), check_vma=False
    )
```

```python
import functools
import math

import jax
import jax.numpy as jnp
from jax import lax
from jax.experimental import pallas as pl
from jax.experimental.pallas import tpu as pltpu
from jax.sharding import PartitionSpec as P

MESH = pl.DeviceIdType.MESH
BIG = 1e30
MOST = 512
BAND = 128
ORDER = (1, 2, 3, 5, 6, 7)
FILLED = (1, 2, 5, 3, 6, 7)
LOW, HIGH = (0, 1), (2, 3)
ALL = LOW + HIGH


def kernel(n, heads, tile, lens_in, q_ref, k_ref, v_ref, out_ref,
           kbuf, vbuf, kdoc, qaug, acc, top, norm, stage,
           lens_ref, send_sem, recv_sem, osend_sem, orecv_sem, load_sem):
    rows, hdim = k_ref.shape
    total_rows = q_ref.shape[0]
    group = total_rows // rows
    me = lax.axis_index("ctx")
    mine = lax.axis_index("head")
    pos = me % 4
    core = pos % 2
    col = pos // 2
    mate = me + 1 - 2 * core
    across = me + 2 - 4 * col
    pos_m = pos + 1 - 2 * core
    pos_x = pos + 2 - 4 * col
    pos_d = pos_x + pos_m - pos
    has1 = me >= 4
    has2 = me >= 8
    feeds = me + 4 < n
    right = col == 1
    leftc = col == 0

    lens_load = pltpu.make_async_copy(lens_in, lens_ref, load_sem.at[3])
    lens_load.start()
    loads = (
        pltpu.make_async_copy(k_ref, kbuf.at[8 + pos], load_sem.at[0]),
        pltpu.make_async_copy(q_ref, qaug.at[:, 0:hdim], load_sem.at[1]),
        pltpu.make_async_copy(v_ref, vbuf.at[8 + pos], load_sem.at[2]),
    )
    for load in loads:
        load.start()

    barrier = pltpu.get_barrier_semaphore()
    for peer in (mate, across):
        pl.semaphore_signal(barrier, inc=1, device_id={"ctx": peer}, device_id_type=MESH)

    @pl.when(has1)
    def _():
        pl.semaphore_signal(barrier, inc=1, device_id={"ctx": me - 4}, device_id_type=MESH)

    @pl.when(feeds)
    def _():
        pl.semaphore_signal(barrier, inc=1, device_id={"ctx": me + 4}, device_id_type=MESH)

    for d in range(1, heads):
        pl.semaphore_signal(barrier, inc=1, device_id={"head": (mine + d) % heads}, device_id_type=MESH)

    half_keys = rows // 2
    parts = [(own, buf, pl.ds(h * half_keys, half_keys)) for h in range(2) for own, buf in ((k_ref, kbuf), (v_ref, vbuf))]

    def copies(lane, slot, to_slot, target):
        return [pltpu.make_async_remote_copy(
            src_ref=own.at[where] if slot is None else buf.at[slot, where],
            dst_ref=buf.at[to_slot, where],
            send_sem=send_sem.at[lane, w],
            recv_sem=recv_sem.at[to_slot, w],
            device_id={"ctx": target},
            device_id_type=MESH,
        ) for w, (own, buf, where) in enumerate(parts)]

    moves = {
        "D0": (copies(0, None, 8 + pos, mate), core == 0),
        "X0": (copies(1, None, 8 + pos, across), leftc),
        "Z0": (copies(2, None, 4 + pos, me + 4), feeds),
        "D0x": (copies(3, 8 + pos_x, 8 + pos_x, mate), right),
        "D1": (copies(4, 4 + pos, 4 + pos, mate), has1),
        "X1": (copies(5, 4 + pos, 4 + pos, across), has1),
        "Z1": (copies(6, 4 + pos, pos, me + 4), has1 & feeds),
        "D1x": (copies(7, 4 + pos_x, 4 + pos_x, mate), has1),
        "D2": (copies(8, pos, pos, mate), has2 & (core == 1)),
        "X2": (copies(9, pos, pos, across), has2 & right),
        "D2x": (copies(10, pos_x, pos_x, mate), has2 & leftc),
    }

    def when(cond, fn):
        if cond is None:
            fn()
        else:
            pl.when(cond)(fn)

    def sent(name):
        made, cond = moves[name]

        def go():
            for copy in made:
                copy.wait_send()

        when(cond, go)

    def landed(slot, cond, *names, which=ALL):
        for w in which:
            _, buf, where = parts[w]

            def go():
                spot = buf.at[slot, where]
                pltpu.make_async_copy(spot, spot, recv_sem.at[slot, w]).wait()

            when(cond, go)
            for name in names:
                made, also = moves[name]
                when(cond if also is None else cond & also, made[w].start)

    def begin(which):
        for w in which:
            for name in ("Z0", "X0", "D0"):
                made, also = moves[name]
                when(also, made[w].start)

    lens_load.wait()

    lane = lax.broadcasted_iota(jnp.int32, (8, 128), 1)
    firsts = jnp.full((8, 128), 2**30, jnp.int32)
    ends = jnp.full((8, 128), 2**30, jnp.int32)
    run = jnp.int32(0)
    for d in range(lens_ref.shape[0]):
        firsts = jnp.where(lane == d, run, firsts)
        run = run + lens_ref[d]
        ends = jnp.where(lane == d, run, ends)
    first_row, end_row = firsts[0:1], ends[0:1]

    def member(position):
        return (position >= first_row) & (position < end_row)

    base = me * rows
    part = rows // heads
    tokens = tile // group
    steps = part // tokens
    span = part * group

    def by_token(width, dim):
        return lax.broadcasted_iota(jnp.int32, (tokens, group, width), dim).reshape(tile, width)

    @pl.loop(0, total_rows // tile)
    def _(t):
        at = pl.ds(pl.multiple_of(t * tile, tile), tile)
        qaug[at, hdim:] = jnp.where(member(base + t * tokens + by_token(128, 0)), 1.0, 0.0).astype(jnp.bfloat16)

    def mark(s):
        kpos = (me - pos - 8 + s) * rows + lax.broadcasted_iota(jnp.int32, (rows, 128), 0)
        kdoc[s] = jnp.where(member(kpos), 0.0, -BIG).astype(jnp.bfloat16)

    mark(8 + pos)
    pl.semaphore_wait(barrier, 1 + heads + has1.astype(jnp.int32) + feeds.astype(jnp.int32))
    begin(LOW)

    scale = math.log2(math.e) / hdim**0.5

    def spread(x, width):
        return jnp.concatenate([x] * (width // 128), axis=1)

    def raw(at, slot, width):
        return lax.dot_general(
            qaug[at, :], jnp.concatenate([kbuf[slot, 0:width, :], kdoc[slot, 0:width, :]], axis=1),
            (((1,), (1,)), ((), ())), preferred_element_type=jnp.float32)

    def mixed(weight, slot, width):
        ones = jnp.ones((width, 128), jnp.bfloat16)
        return jnp.dot(weight, jnp.concatenate([vbuf[slot, 0:width, :], ones], axis=1),
                       preferred_element_type=jnp.float32)

    def raw_pair(at, a, b, where):
        keys = [jnp.concatenate([kbuf[x, where, :], kdoc[x, where, :]], axis=1) for x in (a, b)]
        return lax.dot_general(
            qaug[at, :], jnp.concatenate(keys, axis=0), (((1,), (1,)), ((), ())), preferred_element_type=jnp.float32)

    def mixed_pair(weight, a, b, where):
        ones = jnp.ones((rows, 128), jnp.bfloat16)
        vals = jnp.concatenate([vbuf[a, where, :], vbuf[b, where, :]], axis=0)
        return jnp.dot(weight, jnp.concatenate([vals, ones], axis=1), preferred_element_type=jnp.float32)

    def flow(count, one, two, three):
        scores, weights = {}, {}
        for u in range(count + 2):
            if u >= 2:
                three(u - 2, *weights.pop(u - 2))
            if 1 <= u <= count:
                weights[u - 1] = two(u - 1, scores.pop(u - 1))
            if u < count:
                scores[u] = one(u)

    def diagonal():
        def width(t):
            return -(-(t + 1) * tokens // 128) * 128

        def at(t):
            return pl.ds(t * tile, tile)

        def one(t):
            return raw(at(t), 8 + pos, width(t))

        def two(t, s):
            wide, done = width(t), []
            for r in range(0, tile, BAND):
                here = slice(r, r + BAND)
                x = s[here, :] * scale
                edge = by_token(128, 2)[here] - by_token(128, 0)[here] <= t * tokens - (wide - 128)
                last = jnp.where(edge, x[:, wide - 128:], -BIG)
                x = last if wide == 128 else jnp.concatenate([x[:, :wide - 128], last], axis=1)
                m = jnp.broadcast_to(jnp.max(x, axis=1, keepdims=True), (BAND, 128))
                top[pl.ds(t * tile + r, BAND), :] = m
                done.append(jnp.exp2(x - spread(m, wide)).astype(jnp.bfloat16))
            return (jnp.concatenate(done, axis=0),)

        def three(t, weight):
            acc[at(t), :] = mixed(weight, 8 + pos, width(t))

        flow(total_rows // tile, one, two, three)

    def work(first, a, b, pieces):
        def at(r, size):
            return pl.ds(pl.multiple_of(first + r, BAND), size)

        def one(u):
            r, where = pieces[u]
            return raw_pair(at(r, tile), a, b, where)

        def two(u, s):
            done, factors = [], []
            for r in range(0, tile, BAND):
                x = s[r:r + BAND, :] * scale
                here = at(pieces[u][0] + r, BAND)
                m0 = top[here, :]
                m = jnp.maximum(m0, jnp.max(x, axis=1, keepdims=True))
                top[here, :] = m
                factors.append(jnp.exp2(m0 - m))
                done.append(jnp.exp2(x - spread(m, rows)).astype(jnp.bfloat16))
            return jnp.concatenate(done, axis=0), jnp.concatenate(factors, axis=0)

        def three(u, weight, factor):
            r, where = pieces[u]
            here = at(r, tile)
            acc[here, :] = acc[here, :] * spread(factor, 2 * hdim) + mixed_pair(weight, a, b, where)

        flow(len(pieces), one, two, three)

    def unit(first, a, b, extent):
        work(first, a, b, [(r, parts[w][2]) for r in range(0, extent, tile) for w in (0, 2)])

    def sweep(a, b, h):
        where = pl.ds(pl.multiple_of(h * half_keys, half_keys), half_keys)
        work(0, a, b, [(r, where) for r in range(0, total_rows, tile)])

    def pick(if_right, if_left):
        return col * if_right + (1 - col) * if_left

    def sel(if_one, if_zero):
        return core * if_one + (1 - core) * if_zero

    core0, core1 = core == 0, core == 1
    pairs = (
        (pick(8 + pos_x, 4 + pos), sel(8 + pos_m, pick(8 + pos_d, 4 + pos_m)), right | has1 | core1),
        (pick(4 + pos, 4 + pos_x), pick(4 + pos_m, sel(4 + pos_m, 4 + pos_d)), has1),
        (pick(4 + pos_x, sel(4 + pos_d, pos)), pick(4 + pos_d, sel(pos, pos_m)), has2 | (has1 & (right | core1))),
        (pick(pos, pos_x), pick(sel(8 + pos_d, pos_m), pos_d), has2 | (right & core1)),
    )

    def local(t):
        return pl.ds(pl.multiple_of(t * tokens, tokens), tokens)

    def finish(first, t, put):
        whole = acc[pl.ds(pl.multiple_of(first + t * tile, tile), tile), :]
        norm[...] = whole[:, 0:hdim] / whole[:, hdim:]
        for g in range(group):
            put(g, norm[pl.ds(g, tokens, stride=group), :].astype(jnp.bfloat16))

    columns = pl.ds(pl.multiple_of(mine * (group * hdim), group * hdim), group * hdim)

    def outgoing(d, t):
        return pltpu.make_async_remote_copy(
            src_ref=stage.at[d - 1, local(t)],
            dst_ref=out_ref.at[local(t), columns],
            send_sem=osend_sem.at[d - 1, t],
            recv_sem=orecv_sem.at[d - 1, t],
            device_id={"head": (mine + d) % heads},
            device_id_type=MESH,
        )

    for load in loads:
        load.wait()
    diagonal()
    begin(HIGH)

    def first_in(which):
        landed(4 + pos, has1, "X1", "Z1", "D1", which=which)
        landed(8 + pos_x, right, "D0x", which=which)

    def first_over(which):
        landed(4 + pos_m, has1 & leftc & core0, which=which)
        landed(8 + pos_d, right & core0, which=which)
        landed(8 + pos_m, core1, which=which)

    @pl.loop(1, 12)
    def _(s):
        mark((8 + pos + s) % 12)

    @pl.loop(0, 4 * (me < 8).astype(jnp.int32) + 4 * (me < 4).astype(jnp.int32))
    def _(s):
        kbuf[s] = jnp.zeros((rows, hdim), jnp.bfloat16)
        vbuf[s] = jnp.zeros((rows, hdim), jnp.bfloat16)

    first_in(LOW)
    first_over(LOW)

    @pl.loop(0, 2)
    def _(h):
        @pl.when(h == 1)
        def _():
            first_in(HIGH)
            first_over(HIGH)
            landed(4 + pos_x, has1 & leftc & core1, "D1x", which=LOW)

        @pl.when(pairs[0][2])
        def _():
            sweep(pairs[0][0], pairs[0][1], h)

    def event1():
        landed(4 + pos_x, has1 & leftc & core0, "D1x", which=LOW)
        landed(4 + pos_x, has1 & leftc, "D1x", which=HIGH)
        landed(4 + pos_x, has1 & right, "D1x", which=LOW)
        landed(pos, has2 & right, "X2", "D2", which=LOW)
        landed(pos, has2 & right & core0, "X2", "D2", which=HIGH)
        landed(4 + pos_x, has1 & right & core0, "D1x", which=HIGH)
        landed(4 + pos_m, has1 & (right | core1))
        landed(4 + pos_d, has1 & leftc & core0)

    def event2():
        landed(pos, has2 & leftc, "D2")
        landed(pos, has2 & right & core1, "X2", "D2", which=HIGH)
        landed(4 + pos_x, has1 & right & core1, "D1x", which=HIGH)
        landed(4 + pos_d, has1 & (right | core1))
        landed(pos_m, has2 & leftc & core0)
        landed(pos_x, has2 & leftc, "D2x", which=LOW)

    def event3():
        landed(pos_x, has2 & leftc, "D2x", which=HIGH)

    def event4():
        landed(pos_d, has2 & leftc)
        landed(8 + pos_d, right & core1)
        landed(pos_m, has2 & right & core0)

    others = list(range(1, heads))
    plans = [[(p % 4, d) for p in order for d in (others if p < 4 else [heads])] for order in (ORDER, FILLED)]
    kinds = [[p if d < heads else p + 4 for p, d in plan] for plan in plans]
    filled = (leftc & core1).astype(jnp.int32)
    spots = [[kind.index(p) for kind in kinds] for p in (1, 2, 3)]
    events = (
        (spots[0], event1), (spots[1], event2), ([min(spots[2])] * 2, event3), (spots[2], event4))

    def either(pair):
        return filled * pair[1] + (1 - filled) * pair[0]

    def choose(index, values):
        return sum((index == i) * jnp.asarray(x, jnp.int32) for i, x in enumerate(values))

    @pl.loop(0, len(plans[0]))
    def _(u):
        for places, event in events:
            pl.when(u == either(places))(event)
        p = either([choose(u, [x for x, _ in plan]) for plan in plans])
        d = either([choose(u, [x for _, x in plan]) for plan in plans])
        first = (mine + d) % heads * span

        valid = choose(p, [x[2] for x in pairs]) == 1
        slots = choose(p, [x[0] for x in pairs]), choose(p, [x[1] for x in pairs])
        closing = (p == 3) & (d < heads)

        @pl.when(valid & jnp.logical_not(closing))
        def _():
            unit(first, *slots, span)

        @pl.when(closing)
        def _():
            @pl.loop(0, steps)
            def _(t):
                @pl.when(valid)
                def _():
                    unit(first + t * tile, *slots, tile)

                def put(g, piece):
                    stage[d - 1, local(t), g * hdim:(g + 1) * hdim] = piece

                finish(first, t, put)
                outgoing(d, t).start()

        @pl.when((p == 3) & (d == heads))
        def _():
            @pl.loop(0, steps)
            def _(t):
                def put(g, piece):
                    where = pl.ds(pl.multiple_of(mine * (group * hdim) + g * hdim, hdim), hdim)
                    out_ref[local(t), where] = piece

                finish(first, t, put)

    for d in range(1, heads):
        @pl.loop(0, steps)
        def _(t):
            outgoing(d, t).wait_send()
            source = (mine + heads - d) % heads
            cols = pl.ds(pl.multiple_of(source * (group * hdim), group * hdim), group * hdim)
            got = out_ref.at[local(t), cols]
            pltpu.make_async_copy(got, got, orecv_sem.at[d - 1, t]).wait()

    for name in moves:
        sent(name)


def on_device(mesh, queries, keys, values, doc_lengths):
    rows, group, hdim = queries.shape
    heads = mesh.shape["head"]
    n = mesh.shape["ctx"]
    bf16, f32 = jnp.bfloat16, jnp.float32
    part = rows // heads
    tile = min(MOST, part * group)
    steps = part * group // tile
    vmem = pl.BlockSpec(memory_space=pltpu.VMEM)
    anywhere = pl.BlockSpec(memory_space=pl.ANY)
    return pl.pallas_call(
        functools.partial(kernel, n, heads, tile),
        out_shape=pltpu.VMEM((part, heads * group * hdim), bf16),
        in_specs=[anywhere] * 4,
        out_specs=vmem,
        scratch_shapes=[
            pltpu.VMEM((12, rows, hdim), bf16),
            pltpu.VMEM((12, rows, hdim), bf16),
            pltpu.VMEM((12, rows, 128), bf16),
            pltpu.VMEM((rows * group, hdim + 128), bf16),
            pltpu.VMEM((rows * group, hdim + 128), f32),
            pltpu.VMEM((rows * group, 128), f32),
            pltpu.VMEM((tile, hdim), f32),
            pltpu.VMEM((heads - 1, part, group * hdim), bf16),
            pltpu.SMEM(doc_lengths.shape, jnp.int32),
            pltpu.SemaphoreType.DMA((11, 4)),
            pltpu.SemaphoreType.DMA((12, 4)),
            pltpu.SemaphoreType.DMA((heads - 1, steps)),
            pltpu.SemaphoreType.DMA((heads - 1, steps)),
            pltpu.SemaphoreType.DMA((4,)),
        ],
        compiler_params=pltpu.CompilerParams(
            collective_id=0, has_side_effects=True, vmem_limit_bytes=56 * 1024 * 1024),
    )(doc_lengths, queries.reshape(rows * group, hdim), keys.reshape(rows, hdim), values.reshape(rows, hdim))


def solution(mesh):
    placed = (P("ctx", "head", None), P("ctx", "head", None), P("ctx", "head", None), P())
    return jax.shard_map(
        functools.partial(on_device, mesh), mesh=mesh, in_specs=placed,
        out_specs=P(("ctx", "head"), None), check_vma=False
    )
```
